16 devices in a mesh: yz: 4 (over z, y), x: 4 (over x, core).
Axes of the slice: x: 2, y: 2, z: 2, core: 2. Of those that a mesh axis runs over, the one named last changes fastest.
Arguments:
- h: bfloat16 [128, 2048], P(None, ('x', 'yz'))
- g: bfloat16 [2, 2048], P(None, ('x', 'yz'))
- wq: bfloat16 [2, 2048, 2048], P(None, 'x', 'yz')
- wk: bfloat16 [2, 2048, 2048], P(None, 'x', 'yz')
- wv: bfloat16 [2, 2048, 2048], P(None, 'x', 'yz')
- w_in: bfloat16 [2, 2048, 8192], P(None, 'x', 'yz')
- wo: bfloat16 [2, 2048, 2048], P(None, 'yz', 'x')
- w_out: bfloat16 [2, 8192, 2048], P(None, 'yz', 'x')
- k_cache: bfloat16 [2, 128, 16, 512, 128], P(None, None, ('yz', 'x'))
- v_cache: bfloat16 [2, 128, 16, 512, 128], P(None, None, ('yz', 'x'))
- lens: int32 [128], replicated
Outputs:
- output 1: bfloat16 [128, 2048], P(None, ('x', 'yz'))
- output 2: bfloat16 [2, 128, 16, 128], P(None, None, ('yz', 'x'))
- output 3: bfloat16 [2, 128, 16, 128], P(None, None, ('yz', 'x'))
All inputs are finite; a program needn't handle non-finite values.
Results may differ from the reference program's by a relative error of at most 0.0191147.
Values are sent between devices in bfloat16 or wider.
A program may use at most 1 GiB of HBM per device.

```python
import jax
import jax.numpy as jnp
from jax import lax

E = 2048
F = 8192
H = 16
HEAD = 128
B = 128
S = 512
LAYERS = 2

EPS = 1e-6


def setup_inputs(seed: int = 0) -> dict:
    ks = jax.random.split(jax.random.PRNGKey(seed), 11)
    hd = H * HEAD
    col = 0.3 + 1.7 * jnp.arange(E, dtype=jnp.float32) / E
    h = (jax.random.normal(ks[0], (B, E), jnp.float32) * col).astype(jnp.bfloat16)
    g = (1.0 + 0.3 * jax.random.normal(ks[1], (LAYERS, E), jnp.float32)).astype(jnp.bfloat16)

    def w(k, shape, fan_in, scale=1.0):
        return (jax.random.normal(k, shape, jnp.float32) * (scale * fan_in ** -0.5)).astype(jnp.bfloat16)

    return {
        'h': h,
        'g': g,
        'wq': w(ks[2], (LAYERS, E, hd), E),
        'wk': w(ks[3], (LAYERS, E, hd), E),
        'wv': w(ks[4], (LAYERS, E, hd), E),
        'w_in': w(ks[5], (LAYERS, E, F), E),
        'wo': w(ks[6], (LAYERS, hd, E), hd, 2.0),
        'w_out': w(ks[7], (LAYERS, F, E), F),
        'k_cache': w(ks[8], (LAYERS, B, H, S, HEAD), 1, 2.0),
        'v_cache': w(ks[9], (LAYERS, B, H, S, HEAD), 1),
        'lens': jax.random.randint(ks[10], (B,), 1, S, jnp.int32),
    }


def _rope(t, pos):
    half = HEAD // 2
    inv = 10000.0 ** (-jnp.arange(half, dtype=jnp.float32) / half)
    ang = pos.astype(jnp.float32)[:, None, None] * inv
    c, s = jnp.cos(ang), jnp.sin(ang)
    tf = t.astype(jnp.float32)
    a, b = tf[..., :half], tf[..., half:]
    return jnp.concatenate([a * c - b * s, b * c + a * s], axis=-1).astype(jnp.bfloat16)


def _attend_one(args):
    q, kc, vc, k, v, ln = args
    qf = q.astype(jnp.float32)
    s = jnp.einsum('hd,hsd->hs', qf, kc.astype(jnp.float32)) * HEAD ** -0.5
    s = jnp.where(jnp.arange(S)[None, :] < ln, s, -jnp.inf)
    sn = jnp.sum(qf * k.astype(jnp.float32), axis=-1) * HEAD ** -0.5
    m = jnp.maximum(jnp.max(s, axis=-1), sn)
    p = jnp.exp(s - m[:, None])
    pn = jnp.exp(sn - m)
    den = jnp.sum(p, axis=-1) + pn
    o = jnp.einsum('hs,hsd->hd', p, vc.astype(jnp.float32)) + pn[:, None] * v.astype(jnp.float32)
    return (o / den[:, None]).astype(jnp.bfloat16)


def reference(h, g, wq, wk, wv, w_in, wo, w_out, k_cache, v_cache, lens):
    def layer(hc, xs):
        gl, wql, wkl, wvl, winl, wol, woutl, kcl, vcl = xs
        hf = hc.astype(jnp.float32)
        x = (hf * lax.rsqrt(jnp.mean(hf * hf, axis=-1, keepdims=True) + EPS) * gl.astype(jnp.float32)).astype(jnp.bfloat16)

        def proj(w):
            return jnp.dot(x, w, preferred_element_type=jnp.float32).astype(jnp.bfloat16)

        q = _rope(proj(wql).reshape(B, H, HEAD), lens)
        k = _rope(proj(wkl).reshape(B, H, HEAD), lens)
        v = proj(wvl).reshape(B, H, HEAD)
        f = jax.nn.gelu(proj(winl).astype(jnp.float32), approximate=True).astype(jnp.bfloat16)
        o = lax.map(_attend_one, (q, kcl, vcl, k, v, lens)).reshape(B, H * HEAD)
        y = (jnp.dot(o, wol, preferred_element_type=jnp.float32)
             + jnp.dot(f, woutl, preferred_element_type=jnp.float32)).astype(jnp.bfloat16)
        hn = (hf + y.astype(jnp.float32)).astype(jnp.bfloat16)
        return hn, (k, v)

    h_out, (k_new, v_new) = lax.scan(layer, h, (g, wq, wk, wv, w_in, wo, w_out, k_cache, v_cache))
    return (h_out, k_new, v_new)
```

```python
import functools

import jax
import jax.numpy as jnp
import numpy as np
from jax import lax
from jax.experimental import pallas as pl
from jax.experimental.pallas import tpu as pltpu
from jax.sharding import PartitionSpec as P

EPS = 1e-6
MESH = pl.DeviceIdType.MESH
F32 = jnp.float32
BF16 = jnp.bfloat16

L = 2
B = 128
D = 128
S = 512
NX = 4
NY = 4
E = 2048
G = 16
NG = B // G


def _dot(a, b):
    return jnp.dot(a, b, preferred_element_type=F32)


def _dot_t(a, b):
    return lax.dot_general(a, b, (((1,), (1,)), ((), ())), preferred_element_type=F32)


def _kernel(nch, h_in, g_in, wq_in, wk_in, wv_in, win_in, wo_in, wout_in, kc_in, vc_in, lens_in, inv_in,
            h_out, k_out, v_out,
            kbuf, vbuf, wq, wk, wv, win, wo, wout, gg, lrow, inv, cosb, sinb, lenb,
            hg, ssb, pf, pb, rq, sf, sb, xr, uf, ub, ur, usf, usb, ux, fb, og, zf, zb, zr,
            qv, kv, vv, hout,
            sem_in, sem_w, sem_k, sem_v, sem_o,
            s_send, s_recv, h_send, h_recv, g_send, g_recv, q_send, q_recv, qx_send, qx_recv,
            u_send, u_recv, f_send, f_recv, o_send, o_recv, y_send, y_recv):
    R = B // nch
    xi = lax.axis_index("x")
    yi = lax.axis_index("yz")
    c = lax.rem(xi, 2)
    xc = lax.div(xi, 2)
    partner = xi + 1 - 2 * c
    across = lax.rem(xi + 2, NX)
    sends = []

    def remote(src, dst, ss, rs, **dev):
        dev.setdefault("x", xi)
        dev.setdefault("yz", yi)
        cp = pltpu.make_async_remote_copy(src_ref=src, dst_ref=dst, send_sem=ss, recv_sem=rs,
                                          device_id=dev, device_id_type=MESH)
        cp.start()
        sends.append(cp)
        return cp

    def load(src, dst, sem):
        cp = pltpu.make_async_copy(src, dst, sem)
        cp.start()
        return cp

    in_h = load(h_in, hg.at[0, yi], sem_in.at[0])
    in_g = load(g_in, gg.at[yi], sem_in.at[1])
    in_l = load(lens_in, lrow, sem_in.at[2])
    in_i = load(inv_in, inv, sem_in.at[3])
    weights = (wq, wk, wv, win, wo, wout)
    sources = (wq_in, wk_in, wv_in, win_in, wo_in, wout_in)
    w_cp = {}

    def load_w(l, n):
        w_cp[l, n] = load(sources[n].at[l], weights[n].at[l], sem_w.at[l, n])

    for n in range(4):
        load_w(0, n)

    barrier = pltpu.get_barrier_semaphore()
    for dx in range(NX):
        for dy in range(NY):
            if dx or dy:
                pl.semaphore_signal(barrier, inc=1, device_id={"yz": lax.rem(yi + dy, NY), "x": lax.rem(xi + dx, NX)},
                                    device_id_type=MESH)
    pl.semaphore_wait(barrier, NX * NY - 1)

    eye = (lax.broadcasted_iota(jnp.int32, (R, B), 0) == lax.broadcasted_iota(jnp.int32, (R, B), 1))

    def send_stats(l, ch, hb):
        col = jnp.sum(hb * hb, axis=1, keepdims=True)
        row = jnp.sum(jnp.where(eye, col, 0.0), axis=0, keepdims=True)
        ssb[l, ch, 0] = row
        for dx in range(NX):
            for dy in range(NY):
                slot = dx * NY + dy
                if slot:
                    remote(ssb.at[l, ch, 0], ssb.at[l, ch, slot], s_send.at[l, ch, slot], s_recv.at[l, ch, slot],
                           x=lax.rem(xi + dx, NX), yz=lax.rem(yi + dy, NY))

    h_cp = {}

    def send_h(l, ch):
        rows = pl.ds(ch * R, R)
        h_cp[l, ch] = [remote(hg.at[l, yi, rows], hg.at[l, yi, rows], h_send.at[l, ch, d], h_recv.at[l, ch, d],
                              yz=lax.rem(yi + d, NY)) for d in (2, 1, 3)]

    in_h.wait()
    in_g.wait()
    g_cp = [remote(gg.at[yi], gg.at[yi], g_send.at[d], g_recv.at[d], yz=lax.rem(yi + d, NY)) for d in (1, 2, 3)]
    for ch in range(nch):
        hb = hg[0, yi, pl.ds(ch * R, R), :].astype(F32)
        send_stats(0, ch, hb)
        send_h(0, ch)

    def load_cache(l, grp):
        seqs = pl.ds(grp * G, G)
        pltpu.make_async_copy(kc_in.at[l, seqs], kbuf.at[seqs], sem_k.at[grp]).start()
        pltpu.make_async_copy(vc_in.at[l, seqs], vbuf.at[seqs], sem_v.at[grp]).start()

    for grp in range(NG):
        load_cache(0, grp)
    for n in (5, 4):
        load_w(0, n)
    for n in range(6):
        load_w(1, n)

    in_l.wait()
    in_i.wait()
    eye_b = (lax.broadcasted_iota(jnp.int32, (B, B), 0) == lax.broadcasted_iota(jnp.int32, (B, B), 1))
    lcol = jnp.sum(jnp.where(eye_b, lrow[...].astype(F32), 0.0), axis=1, keepdims=True)
    lenb[...] = jnp.broadcast_to(lcol, (B, D))
    ang = lcol * inv[...]
    cosb[...] = jnp.cos(ang)
    half = lax.broadcasted_iota(jnp.int32, (B, D), 1) < D // 2
    sn = jnp.sin(ang)
    sinb[...] = jnp.where(half, -sn, sn)

    waited = set()

    def need_w(l, *ns):
        for n in ns:
            if (l, n) not in waited:
                waited.add((l, n))
                w_cp[l, n].wait()

    q_cp, u_cp, x_cp, ux_cp, f_cp, o_cp, y_cp = {}, {}, {}, {}, {}, {}, {}

    def stage_in(l, ch):
        rows = pl.ds(ch * R, R)
        for cp in h_cp[l, ch]:
            cp.wait_recv()
        if l == 0 and ch == 0:
            for cp in g_cp:
                cp.wait_recv()
        for slot in range(1, NX * NY):
            pltpu.make_async_copy(ssb.at[l, ch, slot], ssb.at[l, ch, slot], s_recv.at[l, ch, slot]).wait()
        row = ssb[l, ch, 0]
        for slot in range(1, NX * NY):
            row = row + ssb[l, ch, slot]
        col = jnp.sum(jnp.where(eye, row, 0.0), axis=1, keepdims=True)
        r = lax.rsqrt(col / E + EPS)
        xs = []
        for j in range(NY):
            gj = gg[j, pl.ds(l, 1), :].astype(F32)
            xs.append((hg[l, j, rows, :].astype(F32) * r * gj).astype(BF16))
        x = jnp.concatenate(xs, axis=1)
        for t, w in enumerate((wq, wk, wv)):
            need_w(l, t)
            for n in range(2):
                acc = _dot(x, w[l, :, pl.ds(n * 256, 256)])
                for cc in range(2):
                    a = acc[:, cc * D:(cc + 1) * D]
                    pf[cc, t, n, rows, :] = a
                    pb[l, cc, t, n, rows, :] = a.astype(BF16)
            if t == 0:
                q_cp[l, ch, 0] = remote(pb.at[l, 1 - c, pl.ds(0, 1), :, rows], rq.at[l, pl.ds(0, 1), :, rows],
                                        q_send.at[l, ch, 0], q_recv.at[l, ch, 0], x=partner)
        q_cp[l, ch, 1] = remote(pb.at[l, 1 - c, pl.ds(1, 2), :, rows], rq.at[l, pl.ds(1, 2), :, rows],
                                q_send.at[l, ch, 1], q_recv.at[l, ch, 1], x=partner)
        reduce_qkv(l, ch, 0)
        need_w(l, 3)
        for n in range(8):
            acc = _dot(x, win[l, :, pl.ds(n * 256, 256)])
            cols = pl.ds((n % 4) * 256, 256)
            uf[n // 4, rows, cols] = acc
            ub[l, n // 4, rows, cols] = acc.astype(BF16)
        u_cp[l, ch] = remote(ub.at[l, 1 - c, rows], ur.at[l, rows], u_send.at[l, ch, 0], u_recv.at[l, ch, 0],
                             x=partner)
        reduce_qkv(l, ch, 1)

    def reduce_qkv(l, ch, part):
        rows = pl.ds(ch * R, R)
        ts = (0,) if part == 0 else (1, 2)
        q_cp[l, ch, part].wait_recv()
        for t in ts:
            for n in range(2):
                s = pf[c, t, n, rows, :] + rq[l, t, n, rows, :].astype(F32)
                sf[n, t, rows, :] = s
                sb[l, n, t, rows, :] = s.astype(BF16)
        span = pl.ds(ts[0], len(ts))
        x_cp[l, ch, part] = remote(sb.at[l, 1 - xc, span, rows], xr.at[l, span, rows],
                                   qx_send.at[l, ch, part], qx_recv.at[l, ch, part], x=across)

    def reduce_u(l, ch):
        rows = pl.ds(ch * R, R)
        u_cp[l, ch].wait_recv()
        us = uf[c, rows, :] + ur[l, rows, :].astype(F32)
        usf[rows, :] = us
        usb[l, rows, :] = us.astype(BF16)
        ux_cp[l, ch] = remote(usb.at[l, rows], ux.at[l, rows], u_send.at[l, ch, 1], u_recv.at[l, ch, 1], x=across)

    def rope(t, rows):
        tf = t.astype(F32)
        return (tf * cosb[rows, :] + pltpu.roll(tf, D // 2, 1) * sinb[rows, :]).astype(BF16)

    def stage_qkv(l, ch):
        rows = pl.ds(ch * R, R)
        x_cp[l, ch, 0].wait_recv()
        qv[rows, :] = rope((sf[xc, 0, rows, :] + xr[l, 0, rows, :].astype(F32)).astype(BF16), rows)
        x_cp[l, ch, 1].wait_recv()
        kv[l, rows, :] = rope((sf[xc, 1, rows, :] + xr[l, 1, rows, :].astype(F32)).astype(BF16), rows)
        vv[l, rows, :] = (sf[xc, 2, rows, :] + xr[l, 2, rows, :].astype(F32)).astype(BF16)

    rowid = lax.broadcasted_iota(jnp.int32, (G, D), 0)
    pos = lax.broadcasted_iota(jnp.int32, (G, S), 1).astype(F32)
    scale = D ** -0.5

    def attend(l, g0, g1):
        @pl.loop(g0, g1)
        def _(grp):
            base = grp * G
            rows = pl.ds(base, G)
            pltpu.make_async_copy(kc_in.at[l, rows], kbuf.at[rows], sem_k.at[grp]).wait()
            pltpu.make_async_copy(vc_in.at[l, rows], vbuf.at[rows], sem_v.at[grp]).wait()
            qf = qv[rows, :].astype(F32)
            s = jnp.zeros((G, S), F32)
            for i in range(0, G, 2):
                lhs = jnp.concatenate([jnp.where(rowid == i, qf, 0.0), jnp.where(rowid == i + 1, qf, 0.0)],
                                      axis=1).astype(BF16)
                s = s + _dot_t(lhs, jnp.concatenate([kbuf[base + i], kbuf[base + i + 1]], axis=1))
            s = jnp.where(pos < lenb[rows, :][:, :1], s * scale, -jnp.inf)
            kf = kv[l, rows, :].astype(F32)
            vf = vv[l, rows, :].astype(F32)
            s_new = jnp.sum(qf * kf, axis=1, keepdims=True) * scale
            m = jnp.maximum(jnp.max(s, axis=1, keepdims=True), s_new)
            p = jnp.exp(s - m)
            p_new = jnp.exp(s_new - m)
            den = jnp.sum(p, axis=1, keepdims=True) + p_new
            p = p.astype(BF16)
            o = p_new * vf
            for i in range(0, G, 2):
                t = _dot(p, jnp.concatenate([vbuf[base + i], vbuf[base + i + 1]], axis=1))
                o = o + jnp.where(rowid == i, t[:, :D], jnp.where(rowid == i + 1, t[:, D:], 0.0))
            og[l, xi, rows, :] = (o / den).astype(BF16)
            if l + 1 < L:
                load_cache(l + 1, grp)

    def send_o(l, ch):
        rows = pl.ds(ch * R, R)
        o_cp[l, ch] = [remote(og.at[l, xi, rows], og.at[l, xi, rows], o_send.at[l, ch, n], o_recv.at[l, ch, n], x=dst)
                       for n, dst in enumerate((across, lax.rem(partner + 2, NX), partner))]

    def stage_f(l, ch):
        rows = pl.ds(ch * R, R)
        ux_cp[l, ch].wait_recv()
        u = (usf[rows, :] + ux[l, rows, :].astype(F32)).astype(BF16)
        fb[l, c, rows, :] = jax.nn.gelu(u.astype(F32), approximate=True).astype(BF16)
        f_cp[l, ch] = remote(fb.at[l, c, rows], fb.at[l, c, rows], f_send.at[l, ch], f_recv.at[l, ch], x=partner)

    def stage_mlp(l, ch):
        rows = pl.ds(ch * R, R)
        f_cp[l, ch].wait_recv()
        need_w(l, 5)
        f = jnp.concatenate([fb[l, 0, rows, :], fb[l, 1, rows, :]], axis=1)
        for n in range(2):
            zf[pl.ds(2 * n, 1), rows, :], zf[pl.ds(2 * n + 1, 1), rows, :] = (
                a[None] for a in jnp.split(_dot(f, wout[l, :, pl.ds(n * 256, 256)]), 2, axis=1))

    def stage_out(l, ch):
        rows = pl.ds(ch * R, R)
        need_w(l, 4)
        for cp in o_cp[l, ch]:
            cp.wait_recv()
        o = jnp.concatenate([og[l, j, rows, :] for j in range(NX)], axis=1)
        for n in range(2):
            acc = _dot(o, wo[l, :, pl.ds(n * 256, 256)])
            for m in range(2):
                a = acc[:, m * D:(m + 1) * D] + zf[2 * n + m, rows, :]
                zf[2 * n + m, rows, :] = a
                zb[l, 2 * n + m, rows, :] = a.astype(BF16)
        y_cp[l, ch] = []
        for d in (2, 1, 3):
            to = lax.rem(yi + d, NY)
            y_cp[l, ch].append(remote(zb.at[l, to, rows], zr.at[l, d - 1, rows], y_send.at[l, ch, d],
                                      y_recv.at[l, ch, d], yz=to))

    out_cps = []

    def stage_h(l, ch):
        rows = pl.ds(ch * R, R)
        for cp in y_cp[l, ch]:
            cp.wait_recv()
        y = zf[yi, rows, :]
        for d in range(NY - 1):
            y = y + zr[l, d, rows, :].astype(F32)
        hn = (hg[l, yi, rows, :].astype(F32) + y.astype(BF16).astype(F32)).astype(BF16)
        if l + 1 < L:
            hg[l + 1, yi, rows, :] = hn
            send_stats(l + 1, ch, hn.astype(F32))
            send_h(l + 1, ch)
        else:
            hout[rows, :] = hn
            out_cps.append(load(hout.at[rows], h_out.at[rows], sem_o.at[0, ch]))

    gpc = NG // nch
    for l in range(L):
        for ch in range(nch):
            stage_in(l, ch)
            reduce_u(l, ch)
            stage_qkv(l, ch)
        out_cps.append(load(kv.at[l], k_out.at[l], sem_o.at[1, l]))
        out_cps.append(load(vv.at[l], v_out.at[l], sem_o.at[2, l]))
        for ch in range(nch):
            attend(l, ch * gpc, (ch + 1) * gpc)
            send_o(l, ch)
            stage_f(l, ch)
            stage_mlp(l, ch)
            stage_out(l, ch)
        for ch in range(nch):
            stage_h(l, ch)
    for cp in out_cps:
        cp.wait()
    for cp in sends:
        cp.wait_send()


def solution(mesh):
    nch = 1
    act = P(None, ('x', 'yz'))
    w_first = P(None, 'x', 'yz')
    w_second = P(None, 'yz', 'x')
    cache = P(None, None, ('yz', 'x'), None, None)
    new = P(None, None, ('yz', 'x'), None)
    inv_half = 10000.0 ** (-np.arange(D // 2, dtype=np.float64) / (D // 2))
    inv_np = np.concatenate([inv_half, inv_half]).astype(np.float32)[None]

    def body(h, g, wq, wk, wv, w_in, wo, w_out, kc, vc, lens):
        any_spec = pl.BlockSpec(memory_space=pl.ANY)
        vm = pltpu.VMEM
        dma = pltpu.SemaphoreType.DMA
        scratch = [
            vm((B, S, D), BF16), vm((B, S, D), BF16),
            vm((L, 512, 512), BF16), vm((L, 512, 512), BF16), vm((L, 512, 512), BF16), vm((L, 512, 2048), BF16),
            vm((L, 512, 512), BF16), vm((L, 2048, 512), BF16),
            vm((NY, L, D), BF16), vm((1, B), jnp.int32), vm((1, D), F32),
            vm((B, D), F32), vm((B, D), F32), vm((B, D), F32),
            vm((L, NY, B, D), BF16),
            vm((L, nch, NX * NY, 1, B), F32),
            vm((2, 3, 2, B, D), F32),
            vm((L, 2, 3, 2, B, D), BF16),
            vm((L, 3, 2, B, D), BF16),
            vm((2, 3, B, D), F32),
            vm((L, 2, 3, B, D), BF16),
            vm((L, 3, B, D), BF16),
            vm((2, B, 1024), F32),
            vm((L, 2, B, 1024), BF16),
            vm((L, B, 1024), BF16),
            vm((B, 1024), F32),
            vm((L, B, 1024), BF16),
            vm((L, B, 1024), BF16),
            vm((L, 2, B, 1024), BF16),
            vm((L, NX, B, D), BF16),
            vm((NY, B, D), F32),
            vm((L, NY, B, D), BF16),
            vm((L, NY - 1, B, D), BF16),
            vm((B, D), BF16), vm((L, B, D), BF16), vm((L, B, D), BF16), vm((B, D), BF16),
            dma((4,)), dma((L, 6)), dma((NG,)), dma((NG,)), dma((3, max(L, nch))),
            dma((L, nch, NX * NY)), dma((L, nch, NX * NY)),
            dma((L, nch, 4)), dma((L, nch, 4)), dma((4,)), dma((4,)),
            dma((L, nch, 2)), dma((L, nch, 2)), dma((L, nch, 2)), dma((L, nch, 2)),
            dma((L, nch, 2)), dma((L, nch, 2)), dma((L, nch)), dma((L, nch)),
            dma((L, nch, 3)), dma((L, nch, 3)), dma((L, nch, 4)), dma((L, nch, 4)),
        ]
        h_new, k_new, v_new = pl.pallas_call(
            functools.partial(_kernel, nch),
            out_shape=(jax.ShapeDtypeStruct((B, D), BF16), jax.ShapeDtypeStruct((L, B, D), BF16),
                       jax.ShapeDtypeStruct((L, B, D), BF16)),
            in_specs=[any_spec] * 12,
            out_specs=(any_spec,) * 3,
            scratch_shapes=scratch,
            compiler_params=pltpu.CompilerParams(collective_id=0, has_side_effects=True,
                                                 vmem_limit_bytes=67_043_328),
            name="decode_step",
        )(h, g, wq, wk, wv, w_in, wo, w_out, kc.reshape(L, B, S, D), vc.reshape(L, B, S, D),
          lens.reshape(1, B), jnp.asarray(inv_np))
        return h_new, k_new.reshape(L, B, 1, D), v_new.reshape(L, B, 1, D)

    return jax.shard_map(
        body, mesh=mesh,
        in_specs=(act, act, w_first, w_first, w_first, w_first, w_second, w_second, cache, cache, P(None)),
        out_specs=(act, new, new), check_vma=False)
```

```python
import functools

import jax
import jax.numpy as jnp
import numpy as np
from jax import lax
from jax.experimental import pallas as pl
from jax.experimental.pallas import tpu as pltpu
from jax.sharding import PartitionSpec as P

EPS = 1e-6
MESH = pl.DeviceIdType.MESH
F32 = jnp.float32
BF16 = jnp.bfloat16

L = 2
B = 128
D = 128
S = 512
NX = 4
NY = 4
E = 2048
G = 16
NG = B // G


def _dot(a, b):
    return jnp.dot(a, b, preferred_element_type=F32)


def _dot_t(a, b):
    return lax.dot_general(a, b, (((1,), (1,)), ((), ())), preferred_element_type=F32)


def _kernel(nch, h_in, g_in, wq_in, wk_in, wv_in, win_in, wo_in, wout_in, kc_in, vc_in, lens_in, inv_in,
            h_out, k_out, v_out,
            kbuf, vbuf, wq, wk, wv, win, wo, wout, gg, lrow, inv, cosb, sinb, lenb,
            hg, ssb, qf, qb, qr, pf, pb, rq, sf, sb, xr, uf, ub, ur, usf, usb, ux, fb, og, zf, zb, zr,
            qv, kv, vv, hout, sbuf, pbuf, pnew, rden,
            sem_in, sem_w, sem_k, sem_v, sem_o,
            s_send, s_recv, h_send, h_recv, g_send, g_recv, q_send, q_recv, kv_send, kv_recv, qx_send, qx_recv,
            u_send, u_recv, f_send, f_recv, o_send, o_recv, y_send, y_recv):
    R = B // nch
    xi = lax.axis_index("x")
    yi = lax.axis_index("yz")
    c = lax.rem(xi, 2)
    xc = lax.div(xi, 2)
    partner = xi + 1 - 2 * c
    across = lax.rem(xi + 2, NX)
    sends = []

    def remote(src, dst, ss, rs, **dev):
        dev.setdefault("x", xi)
        dev.setdefault("yz", yi)
        cp = pltpu.make_async_remote_copy(src_ref=src, dst_ref=dst, send_sem=ss, recv_sem=rs,
                                          device_id=dev, device_id_type=MESH)
        cp.start()
        sends.append(cp)
        return cp

    def load(src, dst, sem):
        cp = pltpu.make_async_copy(src, dst, sem)
        cp.start()
        return cp

    in_h = load(h_in, hg.at[0, yi], sem_in.at[0])
    in_g = load(g_in, gg.at[yi], sem_in.at[1])
    in_l = load(lens_in, lrow, sem_in.at[2])
    in_i = load(inv_in, inv, sem_in.at[3])
    weights = (wq, wk, wv, win, wo, wout)
    sources = (wq_in, wk_in, wv_in, win_in, wo_in, wout_in)
    w_cp = {}

    def load_w(l, n):
        w_cp[l, n] = load(sources[n].at[l], weights[n].at[l], sem_w.at[l, n])

    for n in range(4):
        load_w(0, n)

    barrier = pltpu.get_barrier_semaphore()
    for dx in range(NX):
        for dy in range(NY):
            if dx or dy:
                pl.semaphore_signal(barrier, inc=1, device_id={"yz": lax.rem(yi + dy, NY), "x": lax.rem(xi + dx, NX)},
                                    device_id_type=MESH)
    pl.semaphore_wait(barrier, NX * NY - 1)

    eye = (lax.broadcasted_iota(jnp.int32, (R, B), 0) == lax.broadcasted_iota(jnp.int32, (R, B), 1))

    def send_stats(l, ch, hb):
        col = jnp.sum(hb * hb, axis=1, keepdims=True)
        row = jnp.sum(jnp.where(eye, col, 0.0), axis=0, keepdims=True)
        ssb[l, ch, 0] = row
        for dx in range(NX):
            for dy in range(NY):
                slot = dx * NY + dy
                if slot:
                    remote(ssb.at[l, ch, 0], ssb.at[l, ch, slot], s_send.at[l, ch, slot], s_recv.at[l, ch, slot],
                           x=lax.rem(xi + dx, NX), yz=lax.rem(yi + dy, NY))

    h_cp = {}

    def send_h(l, ch):
        rows = pl.ds(ch * R, R)
        h_cp[l, ch] = [remote(hg.at[l, yi, rows], hg.at[l, yi, rows], h_send.at[l, ch, d], h_recv.at[l, ch, d],
                              yz=lax.rem(yi + d, NY)) for d in (2, 1, 3)]

    in_h.wait()
    in_g.wait()
    g_cp = [remote(gg.at[yi], gg.at[yi], g_send.at[d], g_recv.at[d], yz=lax.rem(yi + d, NY)) for d in (1, 2, 3)]
    for ch in range(nch):
        hb = hg[0, yi, pl.ds(ch * R, R), :].astype(F32)
        send_stats(0, ch, hb)
        send_h(0, ch)

    def load_cache(l, grp):
        seqs = pl.ds(grp * G, G)
        pltpu.make_async_copy(kc_in.at[l, seqs], kbuf.at[seqs], sem_k.at[grp]).start()
        pltpu.make_async_copy(vc_in.at[l, seqs], vbuf.at[seqs], sem_v.at[grp]).start()

    for grp in range(NG):
        load_cache(0, grp)
    for n in (5, 4):
        load_w(0, n)
    for n in range(6):
        load_w(1, n)

    in_l.wait()
    in_i.wait()
    eye_b = (lax.broadcasted_iota(jnp.int32, (B, B), 0) == lax.broadcasted_iota(jnp.int32, (B, B), 1))
    lcol = jnp.sum(jnp.where(eye_b, lrow[...].astype(F32), 0.0), axis=1, keepdims=True)
    lenb[...] = jnp.broadcast_to(lcol, (B, D))
    ang = lcol * inv[...]
    cosb[...] = jnp.cos(ang)
    half = lax.broadcasted_iota(jnp.int32, (B, D), 1) < D // 2
    sn = jnp.sin(ang)
    sinb[...] = jnp.where(half, -sn, sn)

    waited = set()

    def need_w(l, *ns):
        for n in ns:
            if (l, n) not in waited:
                waited.add((l, n))
                w_cp[l, n].wait()

    q_cp, kv_cp, u_cp, x_cp, ux_cp, f_cp, o_cp, y_cp = {}, {}, {}, {}, {}, {}, {}, {}
    out_cps = []

    def stage_in(l, ch):
        rows = pl.ds(ch * R, R)
        for cp in h_cp[l, ch]:
            cp.wait_recv()
        if l == 0 and ch == 0:
            for cp in g_cp:
                cp.wait_recv()
        for slot in range(1, NX * NY):
            pltpu.make_async_copy(ssb.at[l, ch, slot], ssb.at[l, ch, slot], s_recv.at[l, ch, slot]).wait()
        row = ssb[l, ch, 0]
        for slot in range(1, NX * NY):
            row = row + ssb[l, ch, slot]
        col = jnp.sum(jnp.where(eye, row, 0.0), axis=1, keepdims=True)
        r = lax.rsqrt(col / E + EPS)
        xs = []
        for j in range(NY):
            gj = gg[j, pl.ds(l, 1), :].astype(F32)
            xs.append((hg[l, j, rows, :].astype(F32) * r * gj).astype(BF16))
        x = jnp.concatenate(xs, axis=1)
        need_w(l, 0)
        for n in range(2):
            acc = _dot(x, wq[l, :, pl.ds(n * 256, 256)])
            for m in range(2):
                a = acc[:, m * D:(m + 1) * D]
                qf[2 * n + m, rows, :] = a
                qb[l, 2 * n + m, rows, :] = a.astype(BF16)
        q_cp[l, ch] = []
        for d in (2, 1, 3):
            to = lax.rem(xi + d, NX)
            q_cp[l, ch].append(remote(qb.at[l, to, rows], qr.at[l, d - 1, rows], q_send.at[l, ch, d],
                                      q_recv.at[l, ch, d], x=to))
        for t, w in enumerate((wk, wv)):
            need_w(l, t + 1)
            for n in range(2):
                acc = _dot(x, w[l, :, pl.ds(n * 256, 256)])
                for cc in range(2):
                    a = acc[:, cc * D:(cc + 1) * D]
                    pf[cc, t, n, rows, :] = a
                    pb[l, cc, t, n, rows, :] = a.astype(BF16)
        kv_cp[l, ch] = remote(pb.at[l, 1 - c, :, :, rows], rq.at[l, :, :, rows],
                              kv_send.at[l, ch], kv_recv.at[l, ch], x=partner)
        need_w(l, 3)
        for n in range(8):
            acc = _dot(x, win[l, :, pl.ds(n * 256, 256)])
            cols = pl.ds((n % 4) * 256, 256)
            uf[n // 4, rows, cols] = acc
            ub[l, n // 4, rows, cols] = acc.astype(BF16)
        u_cp[l, ch] = remote(ub.at[l, 1 - c, rows], ur.at[l, rows], u_send.at[l, ch, 0], u_recv.at[l, ch, 0],
                             x=partner)

    def reduce_kv(l, ch):
        rows = pl.ds(ch * R, R)
        kv_cp[l, ch].wait_recv()
        for t in range(2):
            for n in range(2):
                s = pf[c, t, n, rows, :] + rq[l, t, n, rows, :].astype(F32)
                sf[n, t, rows, :] = s
                sb[l, n, t, rows, :] = s.astype(BF16)
        x_cp[l, ch] = remote(sb.at[l, 1 - xc, :, rows], xr.at[l, :, rows],
                             qx_send.at[l, ch], qx_recv.at[l, ch], x=across)

    def reduce_u(l, ch, piece, pieces):
        if piece == 0:
            u_cp[l, ch].wait_recv()
            ux_cp[l, ch] = []
        size = R // pieces
        rows = pl.ds(ch * R + piece * size, size)
        us = uf[c, rows, :] + ur[l, rows, :].astype(F32)
        usf[rows, :] = us
        usb[l, rows, :] = us.astype(BF16)
        ux_cp[l, ch].append(remote(usb.at[l, rows], ux.at[l, rows], u_send.at[l, ch, 1 + piece],
                                   u_recv.at[l, ch, 1 + piece], x=across))

    def rope(t, rows):
        tf = t.astype(F32)
        return (tf * cosb[rows, :] + pltpu.roll(tf, D // 2, 1) * sinb[rows, :]).astype(BF16)

    def stage_q(l, ch):
        rows = pl.ds(ch * R, R)
        for cp in q_cp[l, ch]:
            cp.wait_recv()
        q = qf[xi, rows, :]
        for d in range(NX - 1):
            q = q + qr[l, d, rows, :].astype(F32)
        qv[rows, :] = rope(q.astype(BF16), rows)

    def stage_kv(l, ch):
        rows = pl.ds(ch * R, R)
        x_cp[l, ch].wait_recv()
        kv[l, rows, :] = rope((sf[xc, 0, rows, :] + xr[l, 0, rows, :].astype(F32)).astype(BF16), rows)
        vv[l, rows, :] = (sf[xc, 1, rows, :] + xr[l, 1, rows, :].astype(F32)).astype(BF16)
        out_cps.append(load(kv.at[l, rows], k_out.at[l, rows], sem_o.at[l, 0, ch]))
        out_cps.append(load(vv.at[l, rows], v_out.at[l, rows], sem_o.at[l, 1, ch]))

    rowid = lax.broadcasted_iota(jnp.int32, (G, D), 0)
    pos = lax.broadcasted_iota(jnp.int32, (R, S), 1).astype(F32)
    scale = D ** -0.5
    gpc = NG // nch

    def scores(l, ch):
        @pl.loop(ch * gpc, (ch + 1) * gpc)
        def _(grp):
            base = grp * G
            rows = pl.ds(base, G)
            pltpu.make_async_copy(kc_in.at[l, rows], kbuf.at[rows], sem_k.at[grp]).wait()
            q = qv[rows, :].astype(F32)
            s = jnp.zeros((G, S), F32)
            for i in range(0, G, 2):
                lhs = jnp.concatenate([jnp.where(rowid == i, q, 0.0), jnp.where(rowid == i + 1, q, 0.0)],
                                      axis=1).astype(BF16)
                s = s + _dot_t(lhs, jnp.concatenate([kbuf[base + i], kbuf[base + i + 1]], axis=1))
            sbuf[rows, :] = s
            if l + 1 < L:
                pltpu.make_async_copy(kc_in.at[l + 1, rows], kbuf.at[rows], sem_k.at[grp]).start()

    def softmax(l, ch):
        rows = pl.ds(ch * R, R)
        s = jnp.where(pos < lenb[rows, :][:, :1], sbuf[rows, :] * scale, -jnp.inf)
        s_new = jnp.sum(qv[rows, :].astype(F32) * kv[l, rows, :].astype(F32), axis=1, keepdims=True) * scale
        m = jnp.maximum(jnp.max(s, axis=1, keepdims=True), s_new)
        p = jnp.exp(s - m)
        p_new = jnp.exp(s_new - m)
        pbuf[rows, :] = p.astype(BF16)
        pnew[rows, :] = p_new * vv[l, rows, :].astype(F32)
        rden[rows, :] = jnp.broadcast_to(jnp.sum(p, axis=1, keepdims=True) + p_new, (R, D))

    def values(l, ch):
        @pl.loop(ch * gpc, (ch + 1) * gpc)
        def _(grp):
            base = grp * G
            rows = pl.ds(base, G)
            pltpu.make_async_copy(vc_in.at[l, rows], vbuf.at[rows], sem_v.at[grp]).wait()
            p = pbuf[rows, :]
            o = pnew[rows, :]
            for i in range(0, G, 2):
                t = _dot(p, jnp.concatenate([vbuf[base + i], vbuf[base + i + 1]], axis=1))
                o = o + jnp.where(rowid == i, t[:, :D], jnp.where(rowid == i + 1, t[:, D:], 0.0))
            og[l, xi, rows, :] = (o / rden[rows, :]).astype(BF16)
            if l + 1 < L:
                pltpu.make_async_copy(vc_in.at[l + 1, rows], vbuf.at[rows], sem_v.at[grp]).start()

    def send_o(l, ch):
        rows = pl.ds(ch * R, R)
        o_cp[l, ch] = [remote(og.at[l, xi, rows], og.at[l, xi, rows], o_send.at[l, ch, n], o_recv.at[l, ch, n], x=dst)
                       for n, dst in enumerate((across, lax.rem(partner + 2, NX), partner))]

    def stage_f(l, ch):
        rows = pl.ds(ch * R, R)
        for cp in ux_cp[l, ch]:
            cp.wait_recv()
        u = (usf[rows, :] + ux[l, rows, :].astype(F32)).astype(BF16)
        fb[l, c, rows, :] = jax.nn.gelu(u.astype(F32), approximate=True).astype(BF16)
        f_cp[l, ch] = remote(fb.at[l, c, rows], fb.at[l, c, rows], f_send.at[l, ch], f_recv.at[l, ch], x=partner)

    def stage_mlp(l, ch):
        rows = pl.ds(ch * R, R)
        f_cp[l, ch].wait_recv()
        need_w(l, 5)
        f = jnp.concatenate([fb[l, 0, rows, :], fb[l, 1, rows, :]], axis=1)
        for n in range(2):
            zf[pl.ds(2 * n, 1), rows, :], zf[pl.ds(2 * n + 1, 1), rows, :] = (
                a[None] for a in jnp.split(_dot(f, wout[l, :, pl.ds(n * 256, 256)]), 2, axis=1))

    def stage_out(l, ch):
        rows = pl.ds(ch * R, R)
        need_w(l, 4)
        for cp in o_cp[l, ch]:
            cp.wait_recv()
        o = jnp.concatenate([og[l, j, rows, :] for j in range(NX)], axis=1)
        for n in range(2):
            acc = _dot(o, wo[l, :, pl.ds(n * 256, 256)])
            for m in range(2):
                a = acc[:, m * D:(m + 1) * D] + zf[2 * n + m, rows, :]
                zf[2 * n + m, rows, :] = a
                zb[l, 2 * n + m, rows, :] = a.astype(BF16)
        y_cp[l, ch] = []
        for d in (2, 1, 3):
            to = lax.rem(yi + d, NY)
            y_cp[l, ch].append(remote(zb.at[l, to, rows], zr.at[l, d - 1, rows], y_send.at[l, ch, d],
                                      y_recv.at[l, ch, d], yz=to))

    def stage_h(l, ch):
        rows = pl.ds(ch * R, R)
        for cp in y_cp[l, ch]:
            cp.wait_recv()
        y = zf[yi, rows, :]
        for d in range(NY - 1):
            y = y + zr[l, d, rows, :].astype(F32)
        hn = (hg[l, yi, rows, :].astype(F32) + y.astype(BF16).astype(F32)).astype(BF16)
        if l + 1 < L:
            hg[l + 1, yi, rows, :] = hn
            send_stats(l + 1, ch, hn.astype(F32))
            send_h(l + 1, ch)
        else:
            hout[rows, :] = hn
            out_cps.append(load(hout.at[rows], h_out.at[rows], sem_o.at[l, 2, ch]))

    for l in range(L):
        stage_in(l, 0)
        reduce_kv(l, 0)
        reduce_u(l, 0, 0, 1)
        stage_in(l, 1)
        reduce_kv(l, 1)
        reduce_u(l, 1, 0, 2)
        stage_q(l, 0)
        scores(l, 0)
        stage_kv(l, 0)
        softmax(l, 0)
        values(l, 0)
        send_o(l, 0)
        reduce_u(l, 1, 1, 2)
        stage_q(l, 1)
        scores(l, 1)
        stage_kv(l, 1)
        softmax(l, 1)
        stage_f(l, 0)
        values(l, 1)
        send_o(l, 1)
        stage_mlp(l, 0)
        stage_out(l, 0)
        stage_f(l, 1)
        stage_mlp(l, 1)
        stage_out(l, 1)
        stage_h(l, 0)
        stage_h(l, 1)
    for cp in out_cps:
        cp.wait()
    for cp in sends:
        cp.wait_send()


def solution(mesh):
    nch = 2
    act = P(None, ('x', 'yz'))
    w_first = P(None, 'x', 'yz')
    w_second = P(None, 'yz', 'x')
    cache = P(None, None, ('yz', 'x'), None, None)
    new = P(None, None, ('yz', 'x'), None)
    inv_half = 10000.0 ** (-np.arange(D // 2, dtype=np.float64) / (D // 2))
    inv_np = np.concatenate([inv_half, inv_half]).astype(np.float32)[None]

    def body(h, g, wq, wk, wv, w_in, wo, w_out, kc, vc, lens):
        any_spec = pl.BlockSpec(memory_space=pl.ANY)
        vm = pltpu.VMEM
        dma = pltpu.SemaphoreType.DMA
        scratch = [
            vm((B, S, D), BF16), vm((B, S, D), BF16),
            vm((L, 512, 512), BF16), vm((L, 512, 512), BF16), vm((L, 512, 512), BF16), vm((L, 512, 2048), BF16),
            vm((L, 512, 512), BF16), vm((L, 2048, 512), BF16),
            vm((NY, L, D), BF16), vm((1, B), jnp.int32), vm((1, D), F32),
            vm((B, D), F32), vm((B, D), F32), vm((B, D), F32),
            vm((L, NY, B, D), BF16),
            vm((L, nch, NX * NY, 1, B), F32),
            vm((NX, B, D), F32),
            vm((L, NX, B, D), BF16),
            vm((L, NX - 1, B, D), BF16),
            vm((2, 2, 2, B, D), F32),
            vm((L, 2, 2, 2, B, D), BF16),
            vm((L, 2, 2, B, D), BF16),
            vm((2, 2, B, D), F32),
            vm((L, 2, 2, B, D), BF16),
            vm((L, 2, B, D), BF16),
            vm((2, B, 1024), F32),
            vm((L, 2, B, 1024), BF16),
            vm((L, B, 1024), BF16),
            vm((B, 1024), F32),
            vm((L, B, 1024), BF16),
            vm((L, B, 1024), BF16),
            vm((L, 2, B, 1024), BF16),
            vm((L, NX, B, D), BF16),
            vm((NY, B, D), F32),
            vm((L, NY, B, D), BF16),
            vm((L, NY - 1, B, D), BF16),
            vm((B, D), BF16), vm((L, B, D), BF16), vm((L, B, D), BF16), vm((B, D), BF16),
            vm((B, S), F32), vm((B, S), BF16), vm((B, D), F32), vm((B, D), F32),
            dma((4,)), dma((L, 6)), dma((NG,)), dma((NG,)), dma((L, 3, nch)),
            dma((L, nch, NX * NY)), dma((L, nch, NX * NY)),
            dma((L, nch, 4)), dma((L, nch, 4)), dma((4,)), dma((4,)),
            dma((L, nch, 4)), dma((L, nch, 4)), dma((L, nch)), dma((L, nch)), dma((L, nch)), dma((L, nch)),
            dma((L, nch, 3)), dma((L, nch, 3)), dma((L, nch)), dma((L, nch)),
            dma((L, nch, 3)), dma((L, nch, 3)), dma((L, nch, 4)), dma((L, nch, 4)),
        ]
        h_new, k_new, v_new = pl.pallas_call(
            functools.partial(_kernel, nch),
            out_shape=(jax.ShapeDtypeStruct((B, D), BF16), jax.ShapeDtypeStruct((L, B, D), BF16),
                       jax.ShapeDtypeStruct((L, B, D), BF16)),
            in_specs=[any_spec] * 12,
            out_specs=(any_spec,) * 3,
            scratch_shapes=scratch,
            compiler_params=pltpu.CompilerParams(collective_id=0, has_side_effects=True,
                                                 vmem_limit_bytes=67_043_328),
            name="decode_step",
        )(h, g, wq, wk, wv, w_in, wo, w_out, kc.reshape(L, B, S, D), vc.reshape(L, B, S, D),
          lens.reshape(1, B), jnp.asarray(inv_np))
        return h_new, k_new.reshape(L, B, 1, D), v_new.reshape(L, B, 1, D)

    return jax.shard_map(
        body, mesh=mesh,
        in_specs=(act, act, w_first, w_first, w_first, w_first, w_second, w_second, cache, cache, P(None)),
        out_specs=(act, new, new), check_vma=False)
```

```python
import functools

import jax
import jax.numpy as jnp
import numpy as np
from jax import lax
from jax.experimental import pallas as pl
from jax.experimental.pallas import tpu as pltpu
from jax.sharding import PartitionSpec as P

EPS = 1e-6
MESH = pl.DeviceIdType.MESH
F32 = jnp.float32
BF16 = jnp.bfloat16

L = 2
B = 128
D = 128
S = 512
NX = 4
NY = 4
E = 2048
G = 16
NG = B // G


def _dot(a, b):
    return jnp.dot(a, b, preferred_element_type=F32)


def _dot_t(a, b):
    return lax.dot_general(a, b, (((1,), (1,)), ((), ())), preferred_element_type=F32)


def _kernel(nch, h_in, g_in, wq_in, wk_in, wv_in, win_in, wo_in, wout_in, kc_in, vc_in, lens_in, inv_in,
            h_out, k_out, v_out,
            kbuf, vbuf, wq, wk, wv, win, wo, wout, gg, lrow, inv, cosb, sinb, lenb,
            hg, ssb, qf, qb, qr, pf, pb, rq, sf, sb, xr, uf, ub, ur, usf, usb, ux, fb, og, zf, zb, zr,
            qv, kv, vv, hout, sbuf, pbuf, pnew, rden,
            sem_in, sem_w, sem_k, sem_v, sem_o,
            s_send, s_recv, h_send, h_recv, g_send, g_recv, q_send, q_recv, kv_send, kv_recv, qx_send, qx_recv,
            u_send, u_recv, f_send, f_recv, o_send, o_recv, y_send, y_recv):
    R = B // nch
    xi = lax.axis_index("x")
    yi = lax.axis_index("yz")
    c = lax.rem(xi, 2)
    xc = lax.div(xi, 2)
    partner = xi + 1 - 2 * c
    across = lax.rem(xi + 2, NX)
    sends = []

    def remote(src, dst, ss, rs, **dev):
        dev.setdefault("x", xi)
        dev.setdefault("yz", yi)
        cp = pltpu.make_async_remote_copy(src_ref=src, dst_ref=dst, send_sem=ss, recv_sem=rs,
                                          device_id=dev, device_id_type=MESH)
        cp.start()
        sends.append(cp)
        return cp

    def load(src, dst, sem):
        cp = pltpu.make_async_copy(src, dst, sem)
        cp.start()
        return cp

    in_h = load(h_in, hg.at[0, yi], sem_in.at[0])
    in_g = load(g_in, gg.at[yi], sem_in.at[1])
    in_l = load(lens_in, lrow, sem_in.at[2])
    in_i = load(inv_in, inv, sem_in.at[3])
    weights = (wq, wk, wv, win, wo, wout)
    sources = (wq_in, wk_in, wv_in, win_in, wo_in, wout_in)
    w_cp = {}

    def load_w(l, n):
        w_cp[l, n] = load(sources[n].at[l], weights[n].at[l], sem_w.at[l, n])

    for n in range(4):
        load_w(0, n)

    barrier = pltpu.get_barrier_semaphore()
    for dx in range(NX):
        for dy in range(NY):
            if dx or dy:
                pl.semaphore_signal(barrier, inc=1, device_id={"yz": lax.rem(yi + dy, NY), "x": lax.rem(xi + dx, NX)},
                                    device_id_type=MESH)
    with jax.named_scope('barrier_wait'):
        pl.semaphore_wait(barrier, NX * NY - 1)

    eye = (lax.broadcasted_iota(jnp.int32, (R, B), 0) == lax.broadcasted_iota(jnp.int32, (R, B), 1))

    def send_stats(l, ch, hb):
        col = jnp.sum(hb * hb, axis=1, keepdims=True)
        row = jnp.sum(jnp.where(eye, col, 0.0), axis=0, keepdims=True)
        ssb[l, ch, 0] = row
        for dx in range(NX):
            for dy in range(NY):
                slot = dx * NY + dy
                if slot:
                    remote(ssb.at[l, ch, 0], ssb.at[l, ch, slot], s_send.at[l, ch, slot], s_recv.at[l, ch, slot],
                           x=lax.rem(xi + dx, NX), yz=lax.rem(yi + dy, NY))

    h_cp = {}

    def send_h(l, ch):
        rows = pl.ds(ch * R, R)
        h_cp[l, ch] = [remote(hg.at[l, yi, rows], hg.at[l, yi, rows], h_send.at[l, ch, d], h_recv.at[l, ch, d],
                              yz=lax.rem(yi + d, NY)) for d in (2, 1, 3)]

    with jax.named_scope(f"w_in"):
        in_h.wait()
        in_g.wait()
    g_cp = [remote(gg.at[yi], gg.at[yi], g_send.at[d], g_recv.at[d], yz=lax.rem(yi + d, NY)) for d in (1, 2, 3)]
    for ch in range(nch):
        hb = hg[0, yi, pl.ds(ch * R, R), :].astype(F32)
        send_stats(0, ch, hb)
        send_h(0, ch)

    def load_cache(l, grp):
        seqs = pl.ds(grp * G, G)
        pltpu.make_async_copy(kc_in.at[l, seqs], kbuf.at[seqs], sem_k.at[grp]).start()
        pltpu.make_async_copy(vc_in.at[l, seqs], vbuf.at[seqs], sem_v.at[grp]).start()

    for grp in range(NG):
        load_cache(0, grp)
    for n in (5, 4):
        load_w(0, n)
    for n in range(6):
        load_w(1, n)

    in_l.wait()
    in_i.wait()
    eye_b = (lax.broadcasted_iota(jnp.int32, (B, B), 0) == lax.broadcasted_iota(jnp.int32, (B, B), 1))
    lcol = jnp.sum(jnp.where(eye_b, lrow[...].astype(F32), 0.0), axis=1, keepdims=True)
    lenb[...] = jnp.broadcast_to(lcol, (B, D))
    ang = lcol * inv[...]
    cosb[...] = jnp.cos(ang)
    half = lax.broadcasted_iota(jnp.int32, (B, D), 1) < D // 2
    sn = jnp.sin(ang)
    sinb[...] = jnp.where(half, -sn, sn)

    waited = set()

    def need_w(l, *ns):
        for n in ns:
            if (l, n) not in waited:
                waited.add((l, n))
                with jax.named_scope(f"w_w_{l}_{n}"):
                    w_cp[l, n].wait()

    q_cp, kv_cp, u_cp, x_cp, ux_cp, f_cp, o_cp, y_cp = {}, {}, {}, {}, {}, {}, {}, {}
    out_cps = []

    def stage_in(l, ch):
        rows = pl.ds(ch * R, R)
        with jax.named_scope(f"w_h_{l}_{ch}"):
            for cp in h_cp[l, ch]:
                cp.wait_recv()
        if l == 0 and ch == 0:
            for cp in g_cp:
                cp.wait_recv()
        with jax.named_scope(f"w_s_{l}_{ch}"):
            for slot in range(1, NX * NY):
                pltpu.make_async_copy(ssb.at[l, ch, slot], ssb.at[l, ch, slot], s_recv.at[l, ch, slot]).wait()
        row = ssb[l, ch, 0]
        for slot in range(1, NX * NY):
            row = row + ssb[l, ch, slot]
        col = jnp.sum(jnp.where(eye, row, 0.0), axis=1, keepdims=True)
        r = lax.rsqrt(col / E + EPS)
        xs = []
        for j in range(NY):
            gj = gg[j, pl.ds(l, 1), :].astype(F32)
            xs.append((hg[l, j, rows, :].astype(F32) * r * gj).astype(BF16))
        x = jnp.concatenate(xs, axis=1)
        need_w(l, 0)
        for n in range(2):
            acc = _dot(x, wq[l, :, pl.ds(n * 256, 256)])
            for m in range(2):
                a = acc[:, m * D:(m + 1) * D]
                qf[2 * n + m, rows, :] = a
                qb[l, 2 * n + m, rows, :] = a.astype(BF16)
        q_cp[l, ch] = []
        for d in (2, 1, 3):
            to = lax.rem(xi + d, NX)
            q_cp[l, ch].append(remote(qb.at[l, to, rows], qr.at[l, d - 1, rows], q_send.at[l, ch, d],
                                      q_recv.at[l, ch, d], x=to))
        for t, w in enumerate((wk, wv)):
            need_w(l, t + 1)
            for n in range(2):
                acc = _dot(x, w[l, :, pl.ds(n * 256, 256)])
                for cc in range(2):
                    a = acc[:, cc * D:(cc + 1) * D]
                    pf[cc, t, n, rows, :] = a
                    pb[l, cc, t, n, rows, :] = a.astype(BF16)
        kv_cp[l, ch] = remote(pb.at[l, 1 - c, :, :, rows], rq.at[l, :, :, rows],
                              kv_send.at[l, ch], kv_recv.at[l, ch], x=partner)
        need_w(l, 3)
        for n in range(8):
            acc = _dot(x, win[l, :, pl.ds(n * 256, 256)])
            cols = pl.ds((n % 4) * 256, 256)
            uf[n // 4, rows, cols] = acc
            ub[l, n // 4, rows, cols] = acc.astype(BF16)
        u_cp[l, ch] = remote(ub.at[l, 1 - c, rows], ur.at[l, rows], u_send.at[l, ch, 0], u_recv.at[l, ch, 0],
                             x=partner)

    def reduce_kv(l, ch):
        rows = pl.ds(ch * R, R)
        with jax.named_scope(f"w_kvd2d_{l}_{ch}"):
            kv_cp[l, ch].wait_recv()
        for t in range(2):
            for n in range(2):
                s = pf[c, t, n, rows, :] + rq[l, t, n, rows, :].astype(F32)
                sf[n, t, rows, :] = s
                sb[l, n, t, rows, :] = s.astype(BF16)
        x_cp[l, ch] = remote(sb.at[l, 1 - xc, :, rows], xr.at[l, :, rows],
                             qx_send.at[l, ch], qx_recv.at[l, ch], x=across)

    def reduce_u(l, ch, piece, pieces):
        if piece == 0:
            with jax.named_scope(f"w_ud2d_{l}_{ch}"):
                u_cp[l, ch].wait_recv()
            ux_cp[l, ch] = []
        size = R // pieces
        rows = pl.ds(ch * R + piece * size, size)
        us = uf[c, rows, :] + ur[l, rows, :].astype(F32)
        usf[rows, :] = us
        usb[l, rows, :] = us.astype(BF16)
        ux_cp[l, ch].append(remote(usb.at[l, rows], ux.at[l, rows], u_send.at[l, ch, 1 + piece],
                                   u_recv.at[l, ch, 1 + piece], x=across))

    def rope(t, rows):
        tf = t.astype(F32)
        return (tf * cosb[rows, :] + pltpu.roll(tf, D // 2, 1) * sinb[rows, :]).astype(BF16)

    def stage_q(l, ch):
        rows = pl.ds(ch * R, R)
        with jax.named_scope(f"w_q_{l}_{ch}"):
            for cp in q_cp[l, ch]:
                cp.wait_recv()
        q = qf[xi, rows, :]
        for d in range(NX - 1):
            q = q + qr[l, d, rows, :].astype(F32)
        qv[rows, :] = rope(q.astype(BF16), rows)

    def stage_kv(l, ch):
        rows = pl.ds(ch * R, R)
        with jax.named_scope(f"w_kv_{l}_{ch}"):
            x_cp[l, ch].wait_recv()
        kv[l, rows, :] = rope((sf[xc, 0, rows, :] + xr[l, 0, rows, :].astype(F32)).astype(BF16), rows)
        vv[l, rows, :] = (sf[xc, 1, rows, :] + xr[l, 1, rows, :].astype(F32)).astype(BF16)
        out_cps.append(load(kv.at[l, rows], k_out.at[l, rows], sem_o.at[l, 0, ch]))
        out_cps.append(load(vv.at[l, rows], v_out.at[l, rows], sem_o.at[l, 1, ch]))

    rowid = lax.broadcasted_iota(jnp.int32, (G, D), 0)
    pos = lax.broadcasted_iota(jnp.int32, (R, S), 1).astype(F32)
    scale = D ** -0.5
    gpc = NG // nch

    def scores(l, ch):
        groups = range(ch * gpc, (ch + 1) * gpc)
        for grp in groups:
            rows = pl.ds(grp * G, G)
            pltpu.make_async_copy(kc_in.at[l, rows], kbuf.at[rows], sem_k.at[grp]).wait()
        for grp in groups:
            base = grp * G
            rows = pl.ds(base, G)
            q = qv[rows, :].astype(F32)
            s = jnp.zeros((G, S), F32)
            for i in range(0, G, 2):
                lhs = jnp.concatenate([jnp.where(rowid == i, q, 0.0), jnp.where(rowid == i + 1, q, 0.0)],
                                      axis=1).astype(BF16)
                s = s + _dot_t(lhs, jnp.concatenate([kbuf[base + i], kbuf[base + i + 1]], axis=1))
            sbuf[rows, :] = s
        if l + 1 < L:
            for grp in groups:
                rows = pl.ds(grp * G, G)
                pltpu.make_async_copy(kc_in.at[l + 1, rows], kbuf.at[rows], sem_k.at[grp]).start()

    def softmax(l, ch):
        rows = pl.ds(ch * R, R)
        s = jnp.where(pos < lenb[rows, :][:, :1], sbuf[rows, :] * scale, -jnp.inf)
        s_new = jnp.sum(qv[rows, :].astype(F32) * kv[l, rows, :].astype(F32), axis=1, keepdims=True) * scale
        m = jnp.maximum(jnp.max(s, axis=1, keepdims=True), s_new)
        p = jnp.exp(s - m)
        p_new = jnp.exp(s_new - m)
        pbuf[rows, :] = p.astype(BF16)
        pnew[rows, :] = p_new * vv[l, rows, :].astype(F32)
        rden[rows, :] = jnp.broadcast_to(jnp.sum(p, axis=1, keepdims=True) + p_new, (R, D))

    def values(l, ch):
        groups = range(ch * gpc, (ch + 1) * gpc)
        for grp in groups:
            rows = pl.ds(grp * G, G)
            pltpu.make_async_copy(vc_in.at[l, rows], vbuf.at[rows], sem_v.at[grp]).wait()
        for grp in groups:
            base = grp * G
            rows = pl.ds(base, G)
            p = pbuf[rows, :]
            o = pnew[rows, :]
            for i in range(0, G, 2):
                t = _dot(p, jnp.concatenate([vbuf[base + i], vbuf[base + i + 1]], axis=1))
                o = o + jnp.where(rowid == i, t[:, :D], jnp.where(rowid == i + 1, t[:, D:], 0.0))
            og[l, xi, rows, :] = (o / rden[rows, :]).astype(BF16)
        if l + 1 < L:
            for grp in groups:
                rows = pl.ds(grp * G, G)
                pltpu.make_async_copy(vc_in.at[l + 1, rows], vbuf.at[rows], sem_v.at[grp]).start()

    def send_o(l, ch):
        rows = pl.ds(ch * R, R)
        o_cp[l, ch] = [remote(og.at[l, xi, rows], og.at[l, xi, rows], o_send.at[l, ch, n], o_recv.at[l, ch, n], x=dst)
                       for n, dst in enumerate((across, lax.rem(partner + 2, NX), partner))]

    def stage_f(l, ch):
        rows = pl.ds(ch * R, R)
        with jax.named_scope(f"w_ux_{l}_{ch}"):
            for cp in ux_cp[l, ch]:
                cp.wait_recv()
        u = (usf[rows, :] + ux[l, rows, :].astype(F32)).astype(BF16)
        fb[l, c, rows, :] = jax.nn.gelu(u.astype(F32), approximate=True).astype(BF16)
        f_cp[l, ch] = remote(fb.at[l, c, rows], fb.at[l, c, rows], f_send.at[l, ch], f_recv.at[l, ch], x=partner)

    def stage_mlp(l, ch):
        rows = pl.ds(ch * R, R)
        with jax.named_scope(f"w_f_{l}_{ch}"):
            f_cp[l, ch].wait_recv()
        need_w(l, 5)
        f = jnp.concatenate([fb[l, 0, rows, :], fb[l, 1, rows, :]], axis=1)
        for n in range(2):
            zf[pl.ds(2 * n, 1), rows, :], zf[pl.ds(2 * n + 1, 1), rows, :] = (
                a[None] for a in jnp.split(_dot(f, wout[l, :, pl.ds(n * 256, 256)]), 2, axis=1))

    def stage_out(l, ch):
        rows = pl.ds(ch * R, R)
        need_w(l, 4)
        with jax.named_scope(f"w_o_{l}_{ch}"):
            for cp in o_cp[l, ch]:
                cp.wait_recv()
        o = jnp.concatenate([og[l, j, rows, :] for j in range(NX)], axis=1)
        for n in range(2):
            acc = _dot(o, wo[l, :, pl.ds(n * 256, 256)])
            for m in range(2):
                a = acc[:, m * D:(m + 1) * D] + zf[2 * n + m, rows, :]
                zf[2 * n + m, rows, :] = a
                zb[l, 2 * n + m, rows, :] = a.astype(BF16)
        y_cp[l, ch] = []
        for d in (2, 1, 3):
            to = lax.rem(yi + d, NY)
            y_cp[l, ch].append(remote(zb.at[l, to, rows], zr.at[l, d - 1, rows], y_send.at[l, ch, d],
                                      y_recv.at[l, ch, d], yz=to))

    def stage_h(l, ch):
        rows = pl.ds(ch * R, R)
        with jax.named_scope(f"w_y_{l}_{ch}"):
            for cp in y_cp[l, ch]:
                cp.wait_recv()
        y = zf[yi, rows, :]
        for d in range(NY - 1):
            y = y + zr[l, d, rows, :].astype(F32)
        hn = (hg[l, yi, rows, :].astype(F32) + y.astype(BF16).astype(F32)).astype(BF16)
        if l + 1 < L:
            hg[l + 1, yi, rows, :] = hn
            send_stats(l + 1, ch, hn.astype(F32))
            send_h(l + 1, ch)
        else:
            hout[rows, :] = hn
            out_cps.append(load(hout.at[rows], h_out.at[rows], sem_o.at[l, 2, ch]))

    for l in range(L):
        with jax.named_scope(f"stage_in_{l}_0_"):
            stage_in(l, 0)
        with jax.named_scope(f"reduce_kv_{l}_0_"):
            reduce_kv(l, 0)
        with jax.named_scope(f"reduce_u_{l}_0_0_1"):
            reduce_u(l, 0, 0, 1)
        with jax.named_scope(f"stage_in_{l}_1_"):
            stage_in(l, 1)
        with jax.named_scope(f"reduce_kv_{l}_1_"):
            reduce_kv(l, 1)
        with jax.named_scope(f"reduce_u_{l}_1_0_2"):
            reduce_u(l, 1, 0, 2)
        with jax.named_scope(f"stage_q_{l}_0_"):
            stage_q(l, 0)
        with jax.named_scope(f"scores_{l}_0_"):
            scores(l, 0)
        with jax.named_scope(f"stage_kv_{l}_0_"):
            stage_kv(l, 0)
        with jax.named_scope(f"softmax_{l}_0_"):
            softmax(l, 0)
        with jax.named_scope(f"values_{l}_0_"):
            values(l, 0)
        with jax.named_scope(f"send_o_{l}_0_"):
            send_o(l, 0)
        with jax.named_scope(f"reduce_u_{l}_1_1_2"):
            reduce_u(l, 1, 1, 2)
        with jax.named_scope(f"stage_q_{l}_1_"):
            stage_q(l, 1)
        with jax.named_scope(f"scores_{l}_1_"):
            scores(l, 1)
        with jax.named_scope(f"stage_kv_{l}_1_"):
            stage_kv(l, 1)
        with jax.named_scope(f"softmax_{l}_1_"):
            softmax(l, 1)
        with jax.named_scope(f"stage_f_{l}_0_"):
            stage_f(l, 0)
        with jax.named_scope(f"values_{l}_1_"):
            values(l, 1)
        with jax.named_scope(f"send_o_{l}_1_"):
            send_o(l, 1)
        with jax.named_scope(f"stage_mlp_{l}_0_"):
            stage_mlp(l, 0)
        with jax.named_scope(f"stage_out_{l}_0_"):
            stage_out(l, 0)
        with jax.named_scope(f"stage_f_{l}_1_"):
            stage_f(l, 1)
        with jax.named_scope(f"stage_mlp_{l}_1_"):
            stage_mlp(l, 1)
        with jax.named_scope(f"stage_out_{l}_1_"):
            stage_out(l, 1)
        with jax.named_scope(f"stage_h_{l}_0_"):
            stage_h(l, 0)
        with jax.named_scope(f"stage_h_{l}_1_"):
            stage_h(l, 1)
    with jax.named_scope(f"w_end"):
        for cp in out_cps:
            cp.wait()
        for cp in sends:
            cp.wait_send()


def _tail(h_in, k_in, v_in, h_out, k_out, v_out, hbuf, kbuf, vbuf, sem):
    moves = ((h_in, hbuf, h_out), (k_in, kbuf, k_out), (v_in, vbuf, v_out))
    ins = [pltpu.make_async_copy(a, b, sem.at[0, n]) for n, (a, b, _) in enumerate(moves)]
    outs = [pltpu.make_async_copy(b, o, sem.at[1, n]) for n, (_, b, o) in enumerate(moves)]
    for cp in ins:
        cp.start()
    for cp, out in zip(ins, outs):
        cp.wait()
        out.start()
    for out in outs:
        out.wait()


def solution(mesh):
    nch = 2
    act = P(None, ('x', 'yz'))
    w_first = P(None, 'x', 'yz')
    w_second = P(None, 'yz', 'x')
    cache = P(None, None, ('yz', 'x'), None, None)
    new = P(None, None, ('yz', 'x'), None)
    inv_half = 10000.0 ** (-np.arange(D // 2, dtype=np.float64) / (D // 2))
    inv_np = np.concatenate([inv_half, inv_half]).astype(np.float32)[None]

    def body(h, g, wq, wk, wv, w_in, wo, w_out, kc, vc, lens):
        any_spec = pl.BlockSpec(memory_space=pl.ANY)
        vm = pltpu.VMEM
        dma = pltpu.SemaphoreType.DMA
        scratch = [
            vm((B, S, D), BF16), vm((B, S, D), BF16),
            vm((L, 512, 512), BF16), vm((L, 512, 512), BF16), vm((L, 512, 512), BF16), vm((L, 512, 2048), BF16),
            vm((L, 512, 512), BF16), vm((L, 2048, 512), BF16),
            vm((NY, L, D), BF16), vm((1, B), jnp.int32), vm((1, D), F32),
            vm((B, D), F32), vm((B, D), F32), vm((B, D), F32),
            vm((L, NY, B, D), BF16),
            vm((L, nch, NX * NY, 1, B), F32),
            vm((NX, B, D), F32),
            vm((L, NX, B, D), BF16),
            vm((L, NX - 1, B, D), BF16),
            vm((2, 2, 2, B, D), F32),
            vm((L, 2, 2, 2, B, D), BF16),
            vm((L, 2, 2, B, D), BF16),
            vm((2, 2, B, D), F32),
            vm((L, 2, 2, B, D), BF16),
            vm((L, 2, B, D), BF16),
            vm((2, B, 1024), F32),
            vm((L, 2, B, 1024), BF16),
            vm((L, B, 1024), BF16),
            vm((B, 1024), F32),
            vm((L, B, 1024), BF16),
            vm((L, B, 1024), BF16),
            vm((L, 2, B, 1024), BF16),
            vm((L, NX, B, D), BF16),
            vm((NY, B, D), F32),
            vm((L, NY, B, D), BF16),
            vm((L, NY - 1, B, D), BF16),
            vm((B, D), BF16), vm((L, B, D), BF16), vm((L, B, D), BF16), vm((B, D), BF16),
            vm((B, S), F32), vm((B, S), BF16), vm((B, D), F32), vm((B, D), F32),
            dma((4,)), dma((L, 6)), dma((NG,)), dma((NG,)), dma((L, 3, nch)),
            dma((L, nch, NX * NY)), dma((L, nch, NX * NY)),
            dma((L, nch, 4)), dma((L, nch, 4)), dma((4,)), dma((4,)),
            dma((L, nch, 4)), dma((L, nch, 4)), dma((L, nch)), dma((L, nch)), dma((L, nch)), dma((L, nch)),
            dma((L, nch, 3)), dma((L, nch, 3)), dma((L, nch)), dma((L, nch)),
            dma((L, nch, 3)), dma((L, nch, 3)), dma((L, nch, 4)), dma((L, nch, 4)),
        ]
        h_new, k_new, v_new = pl.pallas_call(
            functools.partial(_kernel, nch),
            out_shape=(jax.ShapeDtypeStruct((B, D), BF16), jax.ShapeDtypeStruct((L, B, D), BF16),
                       jax.ShapeDtypeStruct((L, B, D), BF16)),
            in_specs=[any_spec] * 12,
            out_specs=(any_spec,) * 3,
            scratch_shapes=scratch,
            compiler_params=pltpu.CompilerParams(collective_id=0, has_side_effects=True,
                                                 vmem_limit_bytes=67_043_328),
            name="decode_step",
        )(h, g, wq, wk, wv, w_in, wo, w_out, kc.reshape(L, B, S, D), vc.reshape(L, B, S, D),
          lens.reshape(1, B), jnp.asarray(inv_np))
        shapes = ((B, D), (L, B, D), (L, B, D))
        h_new, k_new, v_new = pl.pallas_call(
            _tail,
            out_shape=tuple(jax.ShapeDtypeStruct(n, BF16) for n in shapes),
            in_specs=[any_spec] * 3,
            out_specs=(any_spec,) * 3,
            scratch_shapes=[vm(n, BF16) for n in shapes] + [dma((2, 3))],
            name="results",
        )(h_new, k_new, v_new)
        return h_new, k_new.reshape(L, B, 1, D), v_new.reshape(L, B, 1, D)

    return jax.shard_map(
        body, mesh=mesh,
        in_specs=(act, act, w_first, w_first, w_first, w_first, w_second, w_second, cache, cache, P(None)),
        out_specs=(act, new, new), check_vma=False)
```

```python
import functools

import jax
import jax.numpy as jnp
import numpy as np
from jax import lax
from jax.experimental import pallas as pl
from jax.experimental.pallas import tpu as pltpu
from jax.sharding import PartitionSpec as P

EPS = 1e-6
MESH = pl.DeviceIdType.MESH
F32 = jnp.float32
BF16 = jnp.bfloat16

L = 2
B = 128
D = 128
S = 512
NX = 4
NY = 4
E = 2048
G = 16
NG = B // G


KINDS = {k: n for n, k in enumerate(("s", "h", "q", "kv", "kvx", "u", "ux", "f", "o", "y"))}
ORDER = ("INA0 INB0 RKVA0 RUA0 QA0 QKA0 RKVB0 RUB0 KVA0 SMA0 PVA0 SOA0 FA0 QB0 QKB0 KVB0 SMB0 MLPA0 OUTA0 FB0 PVB0 SOB0 "
         "MLPB0 HA0 OUTB0 INA1 HB0 RKVA1 RUA1 QA1 QKA1 INB1 KVA1 SMA1 RKVB1 RUB1 PVA1 SOA1 FA1 QB1 QKB1 KVB1 SMB1 MLPA1 "
         "OUTA1 FB1 PVB1 SOB1 MLPB1 HA1 OUTB1 HB1")


def _dot(a, b):
    return jnp.dot(a, b, preferred_element_type=F32)


def _dot_t(a, b):
    return lax.dot_general(a, b, (((1,), (1,)), ((), ())), preferred_element_type=F32)


def _kernel(nch, h_in, g_in, wq_in, wk_in, wv_in, win_in, wo_in, wout_in, kc_in, vc_in, lens_in, inv_in,
            h_out, k_out, v_out,
            kbuf, vbuf, wqkv, win, wo, wout, gg, lrow, inv, cosb, sinb, lenb,
            hg, ssb, qf, qb, qr, pf, pb, rq, sf, sb, xr, uf, ub, ur, usf, usb, ux, fb, og, zf, zb, zr,
            qv, kv, vv, sbuf, pbuf, pnew, rden,
            sem_in, sem_w, sem_k, sem_v, g_sem, send_sem, recv_sem):
    R = B // nch
    xi = lax.axis_index("x")
    yi = lax.axis_index("yz")
    c = lax.rem(xi, 2)
    xc = lax.div(xi, 2)
    partner = xi + 1 - 2 * c
    across = lax.rem(xi + 2, NX)
    open_sends = {}

    def exchange(kind, l, ch, copies, region):
        ss, rs = send_sem.at[KINDS[kind], ch], recv_sem.at[KINDS[kind], ch]
        drain(kind, ch)
        for src, dst, dev in copies:
            pltpu.make_async_remote_copy(src_ref=src, dst_ref=dst, send_sem=ss, recv_sem=rs,
                                         device_id={"x": xi, "yz": yi, **dev}, device_id_type=MESH).start()
        open_sends[kind, ch] = region

    def drain(kind, ch):
        region = open_sends.pop((kind, ch), None)
        if region is not None:
            pltpu.make_async_copy(region, region, send_sem.at[KINDS[kind], ch]).wait()

    def arrived(kind, ch):
        region = open_sends[kind, ch]
        with jax.named_scope(f"w_{kind}_{ch}"):
            pltpu.make_async_copy(region, region, recv_sem.at[KINDS[kind], ch]).wait()

    def load(src, dst, sem):
        cp = pltpu.make_async_copy(src, dst, sem)
        cp.start()
        return cp

    in_h = load(h_in, hg.at[0, yi], sem_in.at[0])
    in_g = load(g_in, gg.at[yi], sem_in.at[1])
    in_l = load(lens_in, lrow, sem_in.at[2])
    in_i = load(inv_in, inv, sem_in.at[3])

    def load_first(l):
        for n, w in enumerate((wq_in, wk_in, wv_in)):
            load(w.at[l], wqkv.at[l, n], sem_w.at[0])
        load(win_in.at[l], win.at[l], sem_w.at[1])

    def load_second(l):
        load(wo_in.at[l], wo.at[l], sem_w.at[2])
        load(wout_in.at[l], wout.at[l], sem_w.at[3])

    def need_w(l, n):
        ref = (wqkv, win, wo, wout)[n].at[l]
        pltpu.make_async_copy(ref, ref, sem_w.at[n]).wait()

    load_first(0)

    barrier = pltpu.get_barrier_semaphore()
    for dx in range(NX):
        for dy in range(NY):
            if dx or dy:
                pl.semaphore_signal(barrier, inc=1, device_id={"yz": lax.rem(yi + dy, NY), "x": lax.rem(xi + dx, NX)},
                                    device_id_type=MESH)

    eye = (lax.broadcasted_iota(jnp.int32, (R, B), 0) == lax.broadcasted_iota(jnp.int32, (R, B), 1))

    def stats(l, ch, hb):
        col = jnp.sum(hb * hb, axis=1, keepdims=True)
        ssb[l, ch, 0] = jnp.sum(jnp.where(eye, col, 0.0), axis=0, keepdims=True)

    def send_h(l, ch):
        rows = pl.ds(ch * R, R)
        exchange("s", l, ch,
                 [(ssb.at[l, ch, 0], ssb.at[l, ch, dx * NY + dy],
                   {"x": lax.rem(xi + dx, NX), "yz": lax.rem(yi + dy, NY)})
                  for dx in range(NX) for dy in range(NY) if dx or dy],
                 ssb.at[l, ch, pl.ds(1, NX * NY - 1)])
        exchange("h", l, ch,
                 [(hg.at[l, yi, rows], hg.at[l, yi, rows], {"yz": lax.rem(yi + d, NY)}) for d in (2, 1, 3)],
                 hg.at[l, pl.ds(0, NY - 1), rows])

    in_h.wait()
    in_g.wait()
    for ch in range(nch):
        stats(0, ch, hg[0, yi, pl.ds(ch * R, R), :].astype(F32))
    with jax.named_scope('barrier_wait'):
        pl.semaphore_wait(barrier, NX * NY - 1)
    for ch in range(nch):
        send_h(0, ch)
    for d in (1, 2, 3):
        pltpu.make_async_remote_copy(src_ref=gg.at[yi], dst_ref=gg.at[yi], send_sem=g_sem.at[0], recv_sem=g_sem.at[1],
                                     device_id={"x": xi, "yz": lax.rem(yi + d, NY)}, device_id_type=MESH).start()

    def load_cache(src, buf, sem, l, ch):
        for grp in range(ch * gpc, (ch + 1) * gpc):
            seqs = pl.ds(grp * G, G)
            load(src.at[l, seqs], buf.at[seqs], sem.at[ch])

    def need_cache(buf, sem, ch):
        ref = buf.at[pl.ds(ch * R, R)]
        pltpu.make_async_copy(ref, ref, sem.at[ch]).wait()

    gpc = NG // nch
    for ch in range(nch):
        load_cache(kc_in, kbuf, sem_k, 0, ch)
        load_cache(vc_in, vbuf, sem_v, 0, ch)
    load_second(0)

    in_l.wait()
    in_i.wait()
    eye_b = (lax.broadcasted_iota(jnp.int32, (B, B), 0) == lax.broadcasted_iota(jnp.int32, (B, B), 1))
    lcol = jnp.sum(jnp.where(eye_b, lrow[...].astype(F32), 0.0), axis=1, keepdims=True)
    lenb[...] = jnp.broadcast_to(lcol, (B, D))
    ang = lcol * inv[...]
    cosb[...] = jnp.cos(ang)
    half = lax.broadcasted_iota(jnp.int32, (B, D), 1) < D // 2
    sn = jnp.sin(ang)
    sinb[...] = jnp.where(half, -sn, sn)

    def stage_in(l, ch):
        rows = pl.ds(ch * R, R)
        arrived("h", ch)
        arrived("s", ch)
        if ch == 0:
            if l == 0:
                ref = gg.at[pl.ds(0, NY - 1)]
                pltpu.make_async_copy(ref, ref, g_sem.at[1]).wait()
                pltpu.make_async_copy(ref, ref, g_sem.at[0]).wait()
            need_w(l, 0)
            need_w(l, 1)
        row = ssb[l, ch, 0]
        for slot in range(1, NX * NY):
            row = row + ssb[l, ch, slot]
        col = jnp.sum(jnp.where(eye, row, 0.0), axis=1, keepdims=True)
        r = lax.rsqrt(col / E + EPS)
        xs = []
        for j in range(NY):
            gj = gg[j, pl.ds(l, 1), :].astype(F32)
            xs.append((hg[l, j, rows, :].astype(F32) * r * gj).astype(BF16))
        x = jnp.concatenate(xs, axis=1)
        for n in range(2):
            acc = _dot(x, wqkv[l, 0, :, pl.ds(n * 256, 256)])
            for m in range(2):
                a = acc[:, m * D:(m + 1) * D]
                qf[2 * n + m, rows, :] = a
                qb[l, 2 * n + m, rows, :] = a.astype(BF16)
        tos = [lax.rem(xi + d, NX) for d in range(NX)]
        exchange("q", l, ch, [(qb.at[l, tos[d], rows], qr.at[l, d - 1, rows], {"x": tos[d]}) for d in (2, 1, 3)],
                 qr.at[l, :, rows])
        for t in range(2):
            for n in range(2):
                acc = _dot(x, wqkv[l, t + 1, :, pl.ds(n * 256, 256)])
                for cc in range(2):
                    a = acc[:, cc * D:(cc + 1) * D]
                    pf[cc, t, n, rows, :] = a
                    pb[l, cc, t, n, rows, :] = a.astype(BF16)
        exchange("kv", l, ch, [(pb.at[l, 1 - c, :, :, rows], rq.at[l, :, :, rows], {"x": partner})],
                 rq.at[l, :, :, rows])
        for n in range(8):
            acc = _dot(x, win[l, :, pl.ds(n * 256, 256)])
            cols = pl.ds((n % 4) * 256, 256)
            uf[n // 4, rows, cols] = acc
            ub[l, n // 4, rows, cols] = acc.astype(BF16)
        exchange("u", l, ch, [(ub.at[l, 1 - c, rows], ur.at[l, rows], {"x": partner})], ur.at[l, rows])
        if ch == nch - 1 and l + 1 < L:
            load_first(l + 1)

    def reduce_kv(l, ch):
        rows = pl.ds(ch * R, R)
        arrived("kv", ch)
        for t in range(2):
            for n in range(2):
                s = pf[c, t, n, rows, :] + rq[l, t, n, rows, :].astype(F32)
                sf[n, t, rows, :] = s
                sb[l, n, t, rows, :] = s.astype(BF16)
        exchange("kvx", l, ch, [(sb.at[l, 1 - xc, :, rows], xr.at[l, :, rows], {"x": across})], xr.at[l, :, rows])

    def reduce_u(l, ch):
        rows = pl.ds(ch * R, R)
        arrived("u", ch)
        us = uf[c, rows, :] + ur[l, rows, :].astype(F32)
        usf[rows, :] = us
        usb[l, rows, :] = us.astype(BF16)
        exchange("ux", l, ch, [(usb.at[l, rows], ux.at[l, rows], {"x": across})], ux.at[l, rows])

    def rope(t, rows):
        tf = t.astype(F32)
        return (tf * cosb[rows, :] + pltpu.roll(tf, D // 2, 1) * sinb[rows, :]).astype(BF16)

    def stage_q(l, ch):
        rows = pl.ds(ch * R, R)
        arrived("q", ch)
        q = qf[xi, rows, :]
        for d in range(NX - 1):
            q = q + qr[l, d, rows, :].astype(F32)
        qv[rows, :] = rope(q.astype(BF16), rows)

    def stage_kv(l, ch):
        rows = pl.ds(ch * R, R)
        arrived("kvx", ch)
        k = rope((sf[xc, 0, rows, :] + xr[l, 0, rows, :].astype(F32)).astype(BF16), rows)
        v = (sf[xc, 1, rows, :] + xr[l, 1, rows, :].astype(F32)).astype(BF16)
        kv[rows, :] = k
        vv[rows, :] = v
        k_out[l, rows, :] = k
        v_out[l, rows, :] = v

    rowid = lax.broadcasted_iota(jnp.int32, (G, D), 0)
    pos = lax.broadcasted_iota(jnp.int32, (R, S), 1).astype(F32)
    scale = D ** -0.5

    def scores(l, ch):
        groups = range(ch * gpc, (ch + 1) * gpc)
        need_cache(kbuf, sem_k, ch)
        for grp in groups:
            base = grp * G
            rows = pl.ds(base, G)
            q = qv[rows, :].astype(F32)
            s = jnp.zeros((G, S), F32)
            for i in range(0, G, 2):
                lhs = jnp.concatenate([jnp.where(rowid == i, q, 0.0), jnp.where(rowid == i + 1, q, 0.0)],
                                      axis=1).astype(BF16)
                s = s + _dot_t(lhs, jnp.concatenate([kbuf[base + i], kbuf[base + i + 1]], axis=1))
            sbuf[rows, :] = s
        if l + 1 < L:
            load_cache(kc_in, kbuf, sem_k, l + 1, ch)

    def softmax(l, ch):
        rows = pl.ds(ch * R, R)
        s = jnp.where(pos < lenb[rows, :][:, :1], sbuf[rows, :] * scale, -jnp.inf)
        s_new = jnp.sum(qv[rows, :].astype(F32) * kv[rows, :].astype(F32), axis=1, keepdims=True) * scale
        m = jnp.maximum(jnp.max(s, axis=1, keepdims=True), s_new)
        p = jnp.exp(s - m)
        p_new = jnp.exp(s_new - m)
        pbuf[rows, :] = p.astype(BF16)
        pnew[rows, :] = p_new * vv[rows, :].astype(F32)
        rden[rows, :] = jnp.broadcast_to(jnp.sum(p, axis=1, keepdims=True) + p_new, (R, D))

    def values(l, ch):
        groups = range(ch * gpc, (ch + 1) * gpc)
        need_cache(vbuf, sem_v, ch)
        for grp in groups:
            base = grp * G
            rows = pl.ds(base, G)
            p = pbuf[rows, :]
            o = pnew[rows, :]
            for i in range(0, G, 2):
                t = _dot(p, jnp.concatenate([vbuf[base + i], vbuf[base + i + 1]], axis=1))
                o = o + jnp.where(rowid == i, t[:, :D], jnp.where(rowid == i + 1, t[:, D:], 0.0))
            og[l, xi, rows, :] = (o / rden[rows, :]).astype(BF16)
        if l + 1 < L:
            load_cache(vc_in, vbuf, sem_v, l + 1, ch)

    def send_o(l, ch):
        rows = pl.ds(ch * R, R)
        exchange("o", l, ch, [(og.at[l, xi, rows], og.at[l, xi, rows], {"x": lax.rem(xi + d, NX)}) for d in (2, 1, 3)],
                 og.at[l, pl.ds(0, NX - 1), rows])

    def stage_f(l, ch):
        rows = pl.ds(ch * R, R)
        arrived("ux", ch)
        u = (usf[rows, :] + ux[l, rows, :].astype(F32)).astype(BF16)
        fb[l, c, rows, :] = jax.nn.gelu(u.astype(F32), approximate=True).astype(BF16)
        exchange("f", l, ch, [(fb.at[l, c, rows], fb.at[l, c, rows], {"x": partner})], fb.at[l, 0, rows])

    def stage_mlp(l, ch):
        rows = pl.ds(ch * R, R)
        arrived("f", ch)
        if ch == 0:
            need_w(l, 3)
        f = jnp.concatenate([fb[l, 0, rows, :], fb[l, 1, rows, :]], axis=1)
        for n in range(2):
            acc = _dot(f, wout[l, :, pl.ds(n * 256, 256)])
            zf[2 * n, rows, :] = acc[:, :D]
            zf[2 * n + 1, rows, :] = acc[:, D:]

    def stage_out(l, ch):
        rows = pl.ds(ch * R, R)
        arrived("o", ch)
        if ch == 0:
            need_w(l, 2)
        o = jnp.concatenate([og[l, j, rows, :] for j in range(NX)], axis=1)
        for n in range(2):
            acc = _dot(o, wo[l, :, pl.ds(n * 256, 256)])
            for m in range(2):
                a = acc[:, m * D:(m + 1) * D] + zf[2 * n + m, rows, :]
                zf[2 * n + m, rows, :] = a
                zb[l, 2 * n + m, rows, :] = a.astype(BF16)
        tos = [lax.rem(yi + d, NY) for d in range(NY)]
        exchange("y", l, ch, [(zb.at[l, tos[d], rows], zr.at[l, d - 1, rows], {"yz": tos[d]}) for d in (2, 1, 3)],
                 zr.at[l, :, rows])
        if ch == nch - 1 and l + 1 < L:
            load_second(l + 1)

    def stage_h(l, ch):
        rows = pl.ds(ch * R, R)
        arrived("y", ch)
        y = zf[yi, rows, :]
        for d in range(NY - 1):
            y = y + zr[l, d, rows, :].astype(F32)
        hn = (hg[l, yi, rows, :].astype(F32) + y.astype(BF16).astype(F32)).astype(BF16)
        if l + 1 < L:
            hg[l + 1, yi, rows, :] = hn
            stats(l + 1, ch, hn.astype(F32))
            send_h(l + 1, ch)
        else:
            h_out[rows, :] = hn

    stages = dict(IN=stage_in, RKV=reduce_kv, RU=reduce_u, Q=stage_q, QK=scores, KV=stage_kv, SM=softmax, PV=values,
                  SO=send_o, F=stage_f, MLP=stage_mlp, OUT=stage_out, H=stage_h)
    for step in ORDER.split():
        with jax.named_scope(step):
            stages[step[:-2]](int(step[-1]), "AB".index(step[-2]))
    for kind, ch in list(open_sends):
        drain(kind, ch)


def _tail(h_in, k_in, v_in, h_out, k_out, v_out, sem):
    cps = [pltpu.make_async_copy(a, o, sem.at[n])
           for n, (a, o) in enumerate(((k_in, k_out), (v_in, v_out), (h_in, h_out)))]
    for cp in cps:
        cp.start()
    for cp in cps:
        cp.wait()


def solution(mesh):
    nch = 2
    act = P(None, ('x', 'yz'))
    w_first = P(None, 'x', 'yz')
    w_second = P(None, 'yz', 'x')
    cache = P(None, None, ('yz', 'x'), None, None)
    new = P(None, None, ('yz', 'x'), None)
    inv_half = 10000.0 ** (-np.arange(D // 2, dtype=np.float64) / (D // 2))
    inv_np = np.concatenate([inv_half, inv_half]).astype(np.float32)[None]

    def body(h, g, wq, wk, wv, w_in, wo, w_out, kc, vc, lens):
        any_spec = pl.BlockSpec(memory_space=pl.ANY)
        vm_spec = pl.BlockSpec(memory_space=pltpu.VMEM)
        shapes = ((B, D), (L, B, D), (L, B, D))
        vm = pltpu.VMEM
        dma = pltpu.SemaphoreType.DMA
        scratch = [
            vm((B, S, D), BF16), vm((B, S, D), BF16),
            vm((L, 3, 512, 512), BF16), vm((L, 512, 2048), BF16), vm((L, 512, 512), BF16), vm((L, 2048, 512), BF16),
            vm((NY, L, D), BF16), vm((1, B), jnp.int32), vm((1, D), F32),
            vm((B, D), F32), vm((B, D), F32), vm((B, D), F32),
            vm((L, NY, B, D), BF16),
            vm((L, nch, NX * NY, 1, B), F32),
            vm((NX, B, D), F32),
            vm((L, NX, B, D), BF16),
            vm((L, NX - 1, B, D), BF16),
            vm((2, 2, 2, B, D), F32),
            vm((L, 2, 2, 2, B, D), BF16),
            vm((L, 2, 2, B, D), BF16),
            vm((2, 2, B, D), F32),
            vm((L, 2, 2, B, D), BF16),
            vm((L, 2, B, D), BF16),
            vm((2, B, 1024), F32),
            vm((L, 2, B, 1024), BF16),
            vm((L, B, 1024), BF16),
            vm((B, 1024), F32),
            vm((L, B, 1024), BF16),
            vm((L, B, 1024), BF16),
            vm((L, 2, B, 1024), BF16),
            vm((L, NX, B, D), BF16),
            vm((NY, B, D), F32),
            vm((L, NY, B, D), BF16),
            vm((L, NY - 1, B, D), BF16),
            vm((B, D), BF16), vm((B, D), BF16), vm((B, D), BF16),
            vm((B, S), F32), vm((B, S), BF16), vm((B, D), F32), vm((B, D), F32),
            dma((4,)), dma((4,)), dma((nch,)), dma((nch,)), dma((2,)),
            dma((len(KINDS), nch)), dma((len(KINDS), nch)),
        ]
        h_new, k_new, v_new = pl.pallas_call(
            functools.partial(_kernel, nch),
            out_shape=tuple(vm(n, BF16) for n in shapes),
            in_specs=[any_spec] * 12,
            out_specs=(vm_spec,) * 3,
            scratch_shapes=scratch,
            compiler_params=pltpu.CompilerParams(collective_id=0, has_side_effects=True,
                                                 vmem_limit_bytes=66_000_000),
            name="decode_step",
        )(h, g, wq, wk, wv, w_in, wo, w_out, kc.reshape(L, B, S, D), vc.reshape(L, B, S, D),
          lens.reshape(1, B), jnp.asarray(inv_np))
        h_new, k_new, v_new = pl.pallas_call(
            _tail,
            out_shape=tuple(jax.ShapeDtypeStruct(n, BF16) for n in shapes),
            in_specs=[vm_spec] * 3,
            out_specs=(any_spec,) * 3,
            scratch_shapes=[dma((3,))],
            name="results",
        )(*(pltpu.with_memory_space_constraint(a, pltpu.VMEM) for a in (h_new, k_new, v_new)))
        return h_new, k_new.reshape(L, B, 1, D), v_new.reshape(L, B, 1, D)

    return jax.shard_map(
        body, mesh=mesh,
        in_specs=(act, act, w_first, w_first, w_first, w_first, w_second, w_second, cache, cache, P(None)),
        out_specs=(act, new, new), check_vma=False)
```

```python
import functools

import jax
import jax.numpy as jnp
import numpy as np
from jax import lax
from jax.experimental import pallas as pl
from jax.experimental.pallas import tpu as pltpu
from jax.sharding import PartitionSpec as P

EPS = 1e-6
MESH = pl.DeviceIdType.MESH
F32 = jnp.float32
BF16 = jnp.bfloat16

L = 2
B = 128
D = 128
S = 512
NX = 4
NY = 4
E = 2048
G = 16
NG = B // G


KINDS = {k: n for n, k in enumerate(("s", "h", "q", "kv", "kvx", "u", "ux", "f", "o", "y"))}
ORDER = ("IN*0 XA0 RKVA0 XA0 RUA0 XA0 XA0 QA0 QKA0 QKA0 RKVB0 KVA0 SMA0 PVA0 SOA0 RUB0 QB0 QKB0 FA0 QKB0 KVB0 SMB0 MLPA0 "
         "OUTA0 PVB0 SOB0 XA1 FB0 XA1 XA1 HA0 MLPB0 OUTB0 XA1 XB1 XB1 INA1 HB0 XB1 RKVA1 RUA1 XB1 QA1 QKA1 QKA1 KVA1 SMA1 "
         "INB1 RKVB1 PVA1 SOA1 RUB1 QB1 QKB1 FA1 QKB1 KVB1 SMB1 PVB1 SOB1 MLPA1 OUTA1 FB1 MLPB1 OUTB1 HA1 HB1")


def _dot(a, b):
    return jnp.dot(a, b, preferred_element_type=F32)


def _dot_t(a, b):
    return lax.dot_general(a, b, (((1,), (1,)), ((), ())), preferred_element_type=F32)


def _kernel(nch, h_in, g_in, wq_in, wk_in, wv_in, win_in, wo_in, wout_in, kc_in, vc_in, lens_in, inv_in,
            h_out, k_out, v_out,
            kbuf, vbuf, wqkv, win, wo, wout, gg, lrow, inv, cosb, sinb, lenb,
            hg, ssb, qf, qb, qr, pf, pb, rq, sf, sb, xr, uf, ub, ur, usf, usb, ux, fb, og, zf, zb, zr,
            qv, kv, vv, sbuf, pbuf, pnew, rden,
            sem_in, sem_w, sem_k, sem_v, g_sem, send_sem, recv_sem):
    R = B // nch
    xi = lax.axis_index("x")
    yi = lax.axis_index("yz")
    c = lax.rem(xi, 2)
    xc = lax.div(xi, 2)
    partner = xi + 1 - 2 * c
    across = lax.rem(xi + 2, NX)
    open_sends = {}

    def exchange(kind, l, ch, copies, region):
        ss, rs = send_sem.at[KINDS[kind], ch], recv_sem.at[KINDS[kind], ch]
        drain(kind, ch)
        for src, dst, dev in copies:
            pltpu.make_async_remote_copy(src_ref=src, dst_ref=dst, send_sem=ss, recv_sem=rs,
                                         device_id={"x": xi, "yz": yi, **dev}, device_id_type=MESH).start()
        open_sends[kind, ch] = region

    def drain(kind, ch):
        region = open_sends.pop((kind, ch), None)
        if region is not None:
            pltpu.make_async_copy(region, region, send_sem.at[KINDS[kind], ch]).wait()

    def arrived(kind, ch):
        region = open_sends[kind, ch]
        with jax.named_scope(f"w_{kind}_{ch}"):
            pltpu.make_async_copy(region, region, recv_sem.at[KINDS[kind], ch]).wait()

    def load(src, dst, sem):
        cp = pltpu.make_async_copy(src, dst, sem)
        cp.start()
        return cp

    in_h = load(h_in, hg.at[0, yi], sem_in.at[0])
    in_g = load(g_in, gg.at[yi], sem_in.at[1])
    in_l = load(lens_in, lrow, sem_in.at[2])
    in_i = load(inv_in, inv, sem_in.at[3])

    def load_first(l):
        for n, w in enumerate((wq_in, wk_in, wv_in)):
            load(w.at[l], wqkv.at[l, n], sem_w.at[0])
        load(win_in.at[l], win.at[l], sem_w.at[1])

    def load_second(l):
        load(wo_in.at[l], wo.at[l], sem_w.at[2])
        load(wout_in.at[l], wout.at[l], sem_w.at[3])

    def need_w(l, n):
        ref = (wqkv, win, wo, wout)[n].at[l]
        pltpu.make_async_copy(ref, ref, sem_w.at[n]).wait()

    load_first(0)

    barrier = pltpu.get_barrier_semaphore()
    for dx in range(NX):
        for dy in range(NY):
            if dx or dy:
                pl.semaphore_signal(barrier, inc=1, device_id={"yz": lax.rem(yi + dy, NY), "x": lax.rem(xi + dx, NX)},
                                    device_id_type=MESH)

    eye = (lax.broadcasted_iota(jnp.int32, (R, B), 0) == lax.broadcasted_iota(jnp.int32, (R, B), 1))

    def stats(l, ch, hb):
        col = jnp.sum(hb * hb, axis=1, keepdims=True)
        ssb[l, ch, 0] = jnp.sum(jnp.where(eye, col, 0.0), axis=0, keepdims=True)

    def send_h(l, ch):
        rows = pl.ds(ch * R, R)
        exchange("s", l, ch,
                 [(ssb.at[l, ch, 0], ssb.at[l, ch, dx * NY + dy],
                   {"x": lax.rem(xi + dx, NX), "yz": lax.rem(yi + dy, NY)})
                  for dx in (2, 1, 3, 0) for dy in (3, 1, 2, 0) if dx or dy],
                 ssb.at[l, ch, pl.ds(1, NX * NY - 1)])
        exchange("h", l, ch,
                 [(hg.at[l, yi, rows], hg.at[l, yi, rows], {"yz": lax.rem(yi + d, NY)}) for d in (3, 1, 2)],
                 hg.at[l, pl.ds(0, NY - 1), rows])

    in_h.wait()
    in_g.wait()
    for ch in range(nch):
        stats(0, ch, hg[0, yi, pl.ds(ch * R, R), :].astype(F32))
    with jax.named_scope('barrier_wait'):
        pl.semaphore_wait(barrier, NX * NY - 1)
    for ch in range(nch):
        send_h(0, ch)
    for d in (1, 2, 3):
        pltpu.make_async_remote_copy(src_ref=gg.at[yi], dst_ref=gg.at[yi], send_sem=g_sem.at[0], recv_sem=g_sem.at[1],
                                     device_id={"x": xi, "yz": lax.rem(yi + d, NY)}, device_id_type=MESH).start()

    def load_cache(src, buf, sem, l, ch):
        for grp in range(ch * gpc, (ch + 1) * gpc):
            seqs = pl.ds(grp * G, G)
            load(src.at[l, seqs], buf.at[seqs], sem.at[ch])

    def need_cache(buf, sem, ch):
        ref = buf.at[pl.ds(ch * R, R)]
        pltpu.make_async_copy(ref, ref, sem.at[ch]).wait()

    gpc = NG // nch
    for ch in range(nch):
        load_cache(kc_in, kbuf, sem_k, 0, ch)
        load_cache(vc_in, vbuf, sem_v, 0, ch)
    load_second(0)

    in_l.wait()
    in_i.wait()
    eye_b = (lax.broadcasted_iota(jnp.int32, (B, B), 0) == lax.broadcasted_iota(jnp.int32, (B, B), 1))
    lcol = jnp.sum(jnp.where(eye_b, lrow[...].astype(F32), 0.0), axis=1, keepdims=True)
    lenb[...] = jnp.broadcast_to(lcol, (B, D))
    ang = lcol * inv[...]
    cosb[...] = jnp.cos(ang)
    half = lax.broadcasted_iota(jnp.int32, (B, D), 1) < D // 2
    sn = jnp.sin(ang)
    sinb[...] = jnp.where(half, -sn, sn)

    def stage_in(l, chunks):
        span = pl.ds(chunks[0] * R, R * len(chunks))
        scales = []
        for ch in chunks:
            arrived("h", ch)
            arrived("s", ch)
            row = ssb[l, ch, 0]
            for slot in range(1, NX * NY):
                row = row + ssb[l, ch, slot]
            col = jnp.sum(jnp.where(eye, row, 0.0), axis=1, keepdims=True)
            scales.append(lax.rsqrt(col / E + EPS))
        r = jnp.concatenate(scales, axis=0)
        if 0 in chunks:
            if l == 0:
                ref = gg.at[pl.ds(0, NY - 1)]
                pltpu.make_async_copy(ref, ref, g_sem.at[1]).wait()
                pltpu.make_async_copy(ref, ref, g_sem.at[0]).wait()
            need_w(l, 0)
            need_w(l, 1)
        xs = []
        for j in range(NY):
            gj = gg[j, pl.ds(l, 1), :].astype(F32)
            xs.append((hg[l, j, span, :].astype(F32) * r * gj).astype(BF16))
        x = jnp.concatenate(xs, axis=1)
        for n in range(2):
            acc = _dot(x, wqkv[l, 0, :, pl.ds(n * 256, 256)])
            for m in range(2):
                a = acc[:, m * D:(m + 1) * D]
                qf[2 * n + m, span, :] = a
                qb[l, 2 * n + m, span, :] = a.astype(BF16)
        tos = [lax.rem(xi + d, NX) for d in range(NX)]
        for ch in chunks:
            rows = pl.ds(ch * R, R)
            exchange("q", l, ch, [(qb.at[l, tos[d], rows], qr.at[l, d - 1, rows], {"x": tos[d]}) for d in (2, 1, 3)],
                     qr.at[l, :, rows])
        for t in range(2):
            for n in range(2):
                acc = _dot(x, wqkv[l, t + 1, :, pl.ds(n * 256, 256)])
                for cc in range(2):
                    a = acc[:, cc * D:(cc + 1) * D]
                    pf[cc, t, n, span, :] = a
                    pb[l, cc, t, n, span, :] = a.astype(BF16)
        for ch in chunks:
            rows = pl.ds(ch * R, R)
            exchange("kv", l, ch, [(pb.at[l, 1 - c, :, :, rows], rq.at[l, :, :, rows], {"x": partner})],
                     rq.at[l, :, :, rows])
        for n in range(8):
            acc = _dot(x, win[l, :, pl.ds(n * 256, 256)])
            cols = pl.ds((n % 4) * 256, 256)
            uf[n // 4, span, cols] = acc
            ub[l, n // 4, span, cols] = acc.astype(BF16)
        for ch in chunks:
            rows = pl.ds(ch * R, R)
            exchange("u", l, ch, [(ub.at[l, 1 - c, rows], ur.at[l, rows], {"x": partner})], ur.at[l, rows])
        if nch - 1 in chunks and l + 1 < L:
            load_first(l + 1)

    def reduce_kv(l, ch):
        rows = pl.ds(ch * R, R)
        arrived("kv", ch)
        for t in range(2):
            for n in range(2):
                s = pf[c, t, n, rows, :] + rq[l, t, n, rows, :].astype(F32)
                sf[n, t, rows, :] = s
                sb[l, n, t, rows, :] = s.astype(BF16)
        exchange("kvx", l, ch, [(sb.at[l, 1 - xc, :, rows], xr.at[l, :, rows], {"x": across})], xr.at[l, :, rows])

    def reduce_u(l, ch):
        rows = pl.ds(ch * R, R)
        arrived("u", ch)
        us = uf[c, rows, :] + ur[l, rows, :].astype(F32)
        usf[rows, :] = us
        usb[l, rows, :] = us.astype(BF16)
        exchange("ux", l, ch, [(usb.at[l, rows], ux.at[l, rows], {"x": across})], ux.at[l, rows])

    def rope(t, rows):
        tf = t.astype(F32)
        return (tf * cosb[rows, :] + pltpu.roll(tf, D // 2, 1) * sinb[rows, :]).astype(BF16)

    def stage_q(l, ch):
        rows = pl.ds(ch * R, R)
        arrived("q", ch)
        q = qf[xi, rows, :]
        for d in range(NX - 1):
            q = q + qr[l, d, rows, :].astype(F32)
        qv[rows, :] = rope(q.astype(BF16), rows)

    def stage_kv(l, ch):
        rows = pl.ds(ch * R, R)
        arrived("kvx", ch)
        k = rope((sf[xc, 0, rows, :] + xr[l, 0, rows, :].astype(F32)).astype(BF16), rows)
        v = (sf[xc, 1, rows, :] + xr[l, 1, rows, :].astype(F32)).astype(BF16)
        kv[rows, :] = k
        vv[rows, :] = v
        k_out[l, rows, :] = k
        v_out[l, rows, :] = v

    rowid = lax.broadcasted_iota(jnp.int32, (G, D), 0)
    pos = lax.broadcasted_iota(jnp.int32, (R, S), 1).astype(F32)
    scale = D ** -0.5

    ready, flipped, scored = set(), {}, {}

    def need_keys(l, ch):
        if (l, ch) not in ready:
            ready.add((l, ch))
            need_cache(kbuf, sem_k, ch)

    def transpose(l, ch):
        need_keys(l, ch)
        g = flipped.get((l, ch), 0)
        flipped[l, ch] = g + 1
        for b in range(ch * R + g * G, ch * R + (g + 1) * G):
            for j in range(S // D):
                kbuf[b, pl.ds(j * D, D), :] = kbuf[b, pl.ds(j * D, D), :].T

    def scores(l, ch):
        need_keys(l, ch)
        first = scored.get((l, ch), 0)
        scored[l, ch] = first + gpc // 2
        for g in range(first, first + gpc // 2):
            base = ch * R + g * G
            rows = pl.ds(base, G)
            q = qv[rows, :].astype(F32)
            s = jnp.zeros((G, S), F32)
            for i in range(0, G, 2):
                lhs = jnp.concatenate([jnp.where(rowid == i, q, 0.0), jnp.where(rowid == i + 1, q, 0.0)],
                                      axis=1).astype(BF16)
                if g < flipped.get((l, ch), 0):
                    keys = [jnp.concatenate([kbuf[base + i + e, pl.ds(j * D, D), :] for j in range(S // D)], axis=1)
                            for e in range(2)]
                    s = s + _dot(lhs, jnp.concatenate(keys, axis=0))
                else:
                    s = s + _dot_t(lhs, jnp.concatenate([kbuf[base + i], kbuf[base + i + 1]], axis=1))
            sbuf[rows, :] = s
        if scored[l, ch] == gpc and l + 1 < L:
            load_cache(kc_in, kbuf, sem_k, l + 1, ch)

    def softmax(l, ch):
        rows = pl.ds(ch * R, R)
        s = jnp.where(pos < lenb[rows, :][:, :1], sbuf[rows, :] * scale, -jnp.inf)
        s_new = jnp.sum(qv[rows, :].astype(F32) * kv[rows, :].astype(F32), axis=1, keepdims=True) * scale
        m = jnp.maximum(jnp.max(s, axis=1, keepdims=True), s_new)
        p = jnp.exp(s - m)
        p_new = jnp.exp(s_new - m)
        pbuf[rows, :] = p.astype(BF16)
        pnew[rows, :] = p_new * vv[rows, :].astype(F32)
        rden[rows, :] = jnp.broadcast_to(jnp.sum(p, axis=1, keepdims=True) + p_new, (R, D))

    def values(l, ch):
        groups = range(ch * gpc, (ch + 1) * gpc)
        need_cache(vbuf, sem_v, ch)
        for grp in groups:
            base = grp * G
            rows = pl.ds(base, G)
            p = pbuf[rows, :]
            o = pnew[rows, :]
            for i in range(0, G, 2):
                t = _dot(p, jnp.concatenate([vbuf[base + i], vbuf[base + i + 1]], axis=1))
                o = o + jnp.where(rowid == i, t[:, :D], jnp.where(rowid == i + 1, t[:, D:], 0.0))
            og[l, xi, rows, :] = (o / rden[rows, :]).astype(BF16)
        if l + 1 < L:
            load_cache(vc_in, vbuf, sem_v, l + 1, ch)

    def send_o(l, ch):
        rows = pl.ds(ch * R, R)
        exchange("o", l, ch, [(og.at[l, xi, rows], og.at[l, xi, rows], {"x": lax.rem(xi + d, NX)}) for d in (2, 1, 3)],
                 og.at[l, pl.ds(0, NX - 1), rows])

    def stage_f(l, ch):
        rows = pl.ds(ch * R, R)
        arrived("ux", ch)
        u = (usf[rows, :] + ux[l, rows, :].astype(F32)).astype(BF16)
        fb[l, c, rows, :] = jax.nn.gelu(u.astype(F32), approximate=True).astype(BF16)
        exchange("f", l, ch, [(fb.at[l, c, rows], fb.at[l, c, rows], {"x": partner})], fb.at[l, 0, rows])

    def stage_mlp(l, ch):
        rows = pl.ds(ch * R, R)
        arrived("f", ch)
        if ch == 0:
            need_w(l, 3)
        f = jnp.concatenate([fb[l, 0, rows, :], fb[l, 1, rows, :]], axis=1)
        for n in range(2):
            acc = _dot(f, wout[l, :, pl.ds(n * 256, 256)])
            zf[2 * n, rows, :] = acc[:, :D]
            zf[2 * n + 1, rows, :] = acc[:, D:]

    def stage_out(l, ch):
        rows = pl.ds(ch * R, R)
        arrived("o", ch)
        if ch == 0:
            need_w(l, 2)
        o = jnp.concatenate([og[l, j, rows, :] for j in range(NX)], axis=1)
        for n in range(2):
            acc = _dot(o, wo[l, :, pl.ds(n * 256, 256)])
            for m in range(2):
                a = acc[:, m * D:(m + 1) * D] + zf[2 * n + m, rows, :]
                zf[2 * n + m, rows, :] = a
                zb[l, 2 * n + m, rows, :] = a.astype(BF16)
        tos = [lax.rem(yi + d, NY) for d in range(NY)]
        exchange("y", l, ch, [(zb.at[l, tos[d], rows], zr.at[l, d - 1, rows], {"yz": tos[d]}) for d in (3, 1, 2)],
                 zr.at[l, :, rows])
        if ch == nch - 1 and l + 1 < L:
            load_second(l + 1)

    def stage_h(l, ch):
        rows = pl.ds(ch * R, R)
        arrived("y", ch)
        y = zf[yi, rows, :]
        for d in range(NY - 1):
            y = y + zr[l, d, rows, :].astype(F32)
        hn = (hg[l, yi, rows, :].astype(F32) + y.astype(BF16).astype(F32)).astype(BF16)
        if l + 1 < L:
            hg[l + 1, yi, rows, :] = hn
            stats(l + 1, ch, hn.astype(F32))
            send_h(l + 1, ch)
        else:
            h_out[rows, :] = hn

    stages = dict(IN=stage_in, RKV=reduce_kv, RU=reduce_u, Q=stage_q, QK=scores, X=transpose, KV=stage_kv, SM=softmax, PV=values,
                  SO=send_o, F=stage_f, MLP=stage_mlp, OUT=stage_out, H=stage_h)
    for step in ORDER.split():
        with jax.named_scope(step):
            chunks = range(nch) if step[-2] == "*" else ("AB".index(step[-2]),)
            stages[step[:-2]](int(step[-1]), chunks if step[:2] == "IN" else chunks[0])
    for kind, ch in list(open_sends):
        drain(kind, ch)


def _tail(h_in, k_in, v_in, h_out, k_out, v_out, sem):
    cps = [pltpu.make_async_copy(a, o, sem.at[n])
           for n, (a, o) in enumerate(((k_in, k_out), (v_in, v_out), (h_in, h_out)))]
    for cp in cps:
        cp.start()
    for cp in cps:
        cp.wait()


def solution(mesh):
    nch = 2
    act = P(None, ('x', 'yz'))
    w_first = P(None, 'x', 'yz')
    w_second = P(None, 'yz', 'x')
    cache = P(None, None, ('yz', 'x'), None, None)
    new = P(None, None, ('yz', 'x'), None)
    inv_half = 10000.0 ** (-np.arange(D // 2, dtype=np.float64) / (D // 2))
    inv_np = np.concatenate([inv_half, inv_half]).astype(np.float32)[None]

    def body(h, g, wq, wk, wv, w_in, wo, w_out, kc, vc, lens):
        any_spec = pl.BlockSpec(memory_space=pl.ANY)
        vm_spec = pl.BlockSpec(memory_space=pltpu.VMEM)
        shapes = ((B, D), (L, B, D), (L, B, D))
        vm = pltpu.VMEM
        dma = pltpu.SemaphoreType.DMA
        scratch = [
            vm((B, S, D), BF16), vm((B, S, D), BF16),
            vm((L, 3, 512, 512), BF16), vm((L, 512, 2048), BF16), vm((L, 512, 512), BF16), vm((L, 2048, 512), BF16),
            vm((NY, L, D), BF16), vm((1, B), jnp.int32), vm((1, D), F32),
            vm((B, D), F32), vm((B, D), F32), vm((B, D), F32),
            vm((L, NY, B, D), BF16),
            vm((L, nch, NX * NY, 1, B), F32),
            vm((NX, B, D), F32),
            vm((L, NX, B, D), BF16),
            vm((L, NX - 1, B, D), BF16),
            vm((2, 2, 2, B, D), F32),
            vm((L, 2, 2, 2, B, D), BF16),
            vm((L, 2, 2, B, D), BF16),
            vm((2, 2, B, D), F32),
            vm((L, 2, 2, B, D), BF16),
            vm((L, 2, B, D), BF16),
            vm((2, B, 1024), F32),
            vm((L, 2, B, 1024), BF16),
            vm((L, B, 1024), BF16),
            vm((B, 1024), F32),
            vm((L, B, 1024), BF16),
            vm((L, B, 1024), BF16),
            vm((L, 2, B, 1024), BF16),
            vm((L, NX, B, D), BF16),
            vm((NY, B, D), F32),
            vm((L, NY, B, D), BF16),
            vm((L, NY - 1, B, D), BF16),
            vm((B, D), BF16), vm((B, D), BF16), vm((B, D), BF16),
            vm((B, S), F32), vm((B, S), BF16), vm((B, D), F32), vm((B, D), F32),
            dma((4,)), dma((4,)), dma((nch,)), dma((nch,)), dma((2,)),
            dma((len(KINDS), nch)), dma((len(KINDS), nch)),
        ]
        h_new, k_new, v_new = pl.pallas_call(
            functools.partial(_kernel, nch),
            out_shape=tuple(vm(n, BF16) for n in shapes),
            in_specs=[any_spec] * 12,
            out_specs=(vm_spec,) * 3,
            scratch_shapes=scratch,
            compiler_params=pltpu.CompilerParams(collective_id=0, has_side_effects=True,
                                                 vmem_limit_bytes=66_000_000),
            name="decode_step",
        )(h, g, wq, wk, wv, w_in, wo, w_out, kc.reshape(L, B, S, D), vc.reshape(L, B, S, D),
          lens.reshape(1, B), jnp.asarray(inv_np))
        h_new, k_new, v_new = pl.pallas_call(
            _tail,
            out_shape=tuple(jax.ShapeDtypeStruct(n, BF16) for n in shapes),
            in_specs=[vm_spec] * 3,
            out_specs=(any_spec,) * 3,
            scratch_shapes=[dma((3,))],
            name="results",
        )(*(pltpu.with_memory_space_constraint(a, pltpu.VMEM) for a in (h_new, k_new, v_new)))
        return h_new, k_new.reshape(L, B, 1, D), v_new.reshape(L, B, 1, D)

    return jax.shard_map(
        body, mesh=mesh,
        in_specs=(act, act, w_first, w_first, w_first, w_first, w_second, w_second, cache, cache, P(None)),
        out_specs=(act, new, new), check_vma=False)
```

```python
import functools

import jax
import jax.numpy as jnp
import numpy as np
from jax import lax
from jax.experimental import pallas as pl
from jax.experimental.pallas import tpu as pltpu
from jax.sharding import PartitionSpec as P

EPS = 1e-6
MESH = pl.DeviceIdType.MESH
F32 = jnp.float32
BF16 = jnp.bfloat16

L = 2
B = 128
D = 128
S = 512
NX = 4
NY = 4
E = 2048
G = 16
NG = B // G


KINDS = {k: n for n, k in enumerate(("s", "h", "q", "kv", "kvx", "u", "ux", "f", "o", "y"))}
ORDER = ("IN*0 SQA0 JN*0 XA0 RKVA0 SQB0 XA0 RUA0 XA0 XA0 QA0 QKA0 QKA0 SMA0 PVA0 KVA0 SOA0 RKVB0 RUB0 QB0 QKB0 FA0 QKB0 "
         "SMB0 MLPA0 OUTA0 PVB0 KVB0 SOB0 XA1 FB0 XA1 XA1 HA0 MLPB0 OUTB0 XA1 XB1 XB1 INA1 SQA1 HB0 JNA1 XB1 RKVA1 RUA1 XB1 "
         "QA1 QKA1 QKA1 INB1 SQB1 SMA1 JNB1 PVA1 RKVB1 RUB1 KVA1 SOA1 QB1 QKB1 FA1 QKB1 SMB1 PVB1 KVB1 SOB1 MLPA1 FB1 OUTA1 "
         "MLPB1 OUTB1 HA1 HB1")


def _dot(a, b):
    return jnp.dot(a, b, preferred_element_type=F32)


def _dot_t(a, b):
    return lax.dot_general(a, b, (((1,), (1,)), ((), ())), preferred_element_type=F32)


def _kernel(nch, h_in, g_in, wq_in, wk_in, wv_in, win_in, wo_in, wout_in, kc_in, vc_in, lens_in, inv_in,
            h_out, k_out, v_out,
            kbuf, vbuf, wqkv, win, wo, wout, gg, lrow, inv, cosb, sinb, lenb,
            hg, ssb, qf, qb, qr, pf, pb, rq, sf, sb, xr, uf, ub, ur, usf, usb, ux, fb, og, zf, zb, zr,
            xbuf, qv, obuf, sbuf, pbuf, mbuf, dbuf,
            sem_in, sem_w, sem_k, sem_v, g_sem, send_sem, recv_sem):
    R = B // nch
    xi = lax.axis_index("x")
    yi = lax.axis_index("yz")
    c = lax.rem(xi, 2)
    xc = lax.div(xi, 2)
    partner = xi + 1 - 2 * c
    across = lax.rem(xi + 2, NX)
    open_sends = {}

    def exchange(kind, l, ch, copies, region):
        ss, rs = send_sem.at[KINDS[kind], ch], recv_sem.at[KINDS[kind], ch]
        drain(kind, ch)
        for src, dst, dev in copies:
            pltpu.make_async_remote_copy(src_ref=src, dst_ref=dst, send_sem=ss, recv_sem=rs,
                                         device_id={"x": xi, "yz": yi, **dev}, device_id_type=MESH).start()
        open_sends[kind, ch] = region

    def drain(kind, ch):
        region = open_sends.pop((kind, ch), None)
        if region is not None:
            pltpu.make_async_copy(region, region, send_sem.at[KINDS[kind], ch]).wait()

    def arrived(kind, ch):
        region = open_sends[kind, ch]
        with jax.named_scope(f"w_{kind}_{ch}"):
            pltpu.make_async_copy(region, region, recv_sem.at[KINDS[kind], ch]).wait()

    def load(src, dst, sem):
        cp = pltpu.make_async_copy(src, dst, sem)
        cp.start()
        return cp

    in_h = load(h_in, hg.at[0, yi], sem_in.at[0])
    in_g = load(g_in, gg.at[yi], sem_in.at[1])
    in_l = load(lens_in, lrow, sem_in.at[2])
    in_i = load(inv_in, inv, sem_in.at[3])

    def load_first(l):
        for n, w in enumerate((wq_in, wk_in, wv_in)):
            load(w.at[l], wqkv.at[l, n], sem_w.at[0])
        load(win_in.at[l], win.at[l], sem_w.at[1])

    def load_second(l):
        load(wo_in.at[l], wo.at[l], sem_w.at[2])
        load(wout_in.at[l], wout.at[l], sem_w.at[3])

    def need_w(l, n):
        ref = (wqkv, win, wo, wout)[n].at[l]
        pltpu.make_async_copy(ref, ref, sem_w.at[n]).wait()

    load_first(0)

    barrier = pltpu.get_barrier_semaphore()
    for dx in range(NX):
        for dy in range(NY):
            if dx or dy:
                pl.semaphore_signal(barrier, inc=1, device_id={"yz": lax.rem(yi + dy, NY), "x": lax.rem(xi + dx, NX)},
                                    device_id_type=MESH)

    eye = (lax.broadcasted_iota(jnp.int32, (R, B), 0) == lax.broadcasted_iota(jnp.int32, (R, B), 1))

    def stats(l, ch, hb):
        col = jnp.sum(hb * hb, axis=1, keepdims=True)
        ssb[l, ch, 0] = jnp.sum(jnp.where(eye, col, 0.0), axis=0, keepdims=True)

    def send_h(l, ch):
        rows = pl.ds(ch * R, R)
        exchange("s", l, ch,
                 [(ssb.at[l, ch, 0], ssb.at[l, ch, dx * NY + dy],
                   {"x": lax.rem(xi + dx, NX), "yz": lax.rem(yi + dy, NY)})
                  for dx in (2, 1, 3, 0) for dy in (3, 1, 2, 0) if dx or dy],
                 ssb.at[l, ch, pl.ds(1, NX * NY - 1)])
        exchange("h", l, ch,
                 [(hg.at[l, yi, rows], hg.at[l, yi, rows], {"yz": lax.rem(yi + d, NY)}) for d in (3, 1, 2)],
                 hg.at[l, pl.ds(0, NY - 1), rows])

    in_h.wait()
    in_g.wait()
    for ch in range(nch):
        stats(0, ch, hg[0, yi, pl.ds(ch * R, R), :].astype(F32))
    with jax.named_scope('barrier_wait'):
        pl.semaphore_wait(barrier, NX * NY - 1)
    for ch in range(nch):
        send_h(0, ch)
    for d in (1, 2, 3):
        pltpu.make_async_remote_copy(src_ref=gg.at[yi], dst_ref=gg.at[yi], send_sem=g_sem.at[0], recv_sem=g_sem.at[1],
                                     device_id={"x": xi, "yz": lax.rem(yi + d, NY)}, device_id_type=MESH).start()

    def load_cache(src, buf, sem, l, ch):
        for grp in range(ch * gpc, (ch + 1) * gpc):
            seqs = pl.ds(grp * G, G)
            load(src.at[l, seqs], buf.at[seqs], sem.at[ch])

    def need_cache(buf, sem, ch):
        ref = buf.at[pl.ds(ch * R, R)]
        pltpu.make_async_copy(ref, ref, sem.at[ch]).wait()

    gpc = NG // nch
    for ch in range(nch):
        load_cache(kc_in, kbuf, sem_k, 0, ch)
        load_cache(vc_in, vbuf, sem_v, 0, ch)
    load_second(0)

    in_l.wait()
    in_i.wait()
    eye_b = (lax.broadcasted_iota(jnp.int32, (B, B), 0) == lax.broadcasted_iota(jnp.int32, (B, B), 1))
    lcol = jnp.sum(jnp.where(eye_b, lrow[...].astype(F32), 0.0), axis=1, keepdims=True)
    lenb[...] = jnp.broadcast_to(lcol, (B, D))
    ang = lcol * inv[...]
    cosb[...] = jnp.cos(ang)
    half = lax.broadcasted_iota(jnp.int32, (B, D), 1) < D // 2
    sn = jnp.sin(ang)
    sinb[...] = jnp.where(half, -sn, sn)

    def stage_in(l, chunks):
        span = pl.ds(chunks[0] * R, R * len(chunks))
        scales = []
        for ch in chunks:
            arrived("h", ch)
            arrived("s", ch)
            row = ssb[l, ch, 0]
            for slot in range(1, NX * NY):
                row = row + ssb[l, ch, slot]
            col = jnp.sum(jnp.where(eye, row, 0.0), axis=1, keepdims=True)
            scales.append(lax.rsqrt(col / E + EPS))
        r = jnp.concatenate(scales, axis=0)
        if 0 in chunks:
            if l == 0:
                ref = gg.at[pl.ds(0, NY - 1)]
                pltpu.make_async_copy(ref, ref, g_sem.at[1]).wait()
                pltpu.make_async_copy(ref, ref, g_sem.at[0]).wait()
            need_w(l, 0)
            need_w(l, 1)
        xs = []
        for j in range(NY):
            gj = gg[j, pl.ds(l, 1), :].astype(F32)
            xs.append((hg[l, j, span, :].astype(F32) * r * gj).astype(BF16))
        x = jnp.concatenate(xs, axis=1)
        xbuf[span, :] = x
        for n in range(2):
            acc = _dot(x, wqkv[l, 0, :, pl.ds(n * 256, 256)])
            for m in range(2):
                a = acc[:, m * D:(m + 1) * D]
                qf[2 * n + m, span, :] = a
                qb[l, 2 * n + m, span, :] = a.astype(BF16)

    def send_q(l, ch):
        rows = pl.ds(ch * R, R)
        tos = [lax.rem(xi + d, NX) for d in range(NX)]
        exchange("q", l, ch, [(qb.at[l, tos[d], rows], qr.at[l, d - 1, rows], {"x": tos[d]}) for d in (2, 1, 3)],
                 qr.at[l, :, rows])

    def stage_in_rest(l, chunks):
        span = pl.ds(chunks[0] * R, R * len(chunks))
        x = xbuf[span, :]
        for t in range(2):
            for n in range(2):
                acc = _dot(x, wqkv[l, t + 1, :, pl.ds(n * 256, 256)])
                for cc in range(2):
                    a = acc[:, cc * D:(cc + 1) * D]
                    pf[cc, t, n, span, :] = a
                    pb[l, cc, t, n, span, :] = a.astype(BF16)
        for ch in chunks:
            rows = pl.ds(ch * R, R)
            exchange("kv", l, ch, [(pb.at[l, 1 - c, :, :, rows], rq.at[l, :, :, rows], {"x": partner})],
                     rq.at[l, :, :, rows])
        for n in range(8):
            acc = _dot(x, win[l, :, pl.ds(n * 256, 256)])
            cols = pl.ds((n % 4) * 256, 256)
            uf[n // 4, span, cols] = acc
            ub[l, n // 4, span, cols] = acc.astype(BF16)
        for ch in chunks:
            rows = pl.ds(ch * R, R)
            exchange("u", l, ch, [(ub.at[l, 1 - c, rows], ur.at[l, rows], {"x": partner})], ur.at[l, rows])
        if nch - 1 in chunks and l + 1 < L:
            load_first(l + 1)

    def reduce_kv(l, ch):
        rows = pl.ds(ch * R, R)
        arrived("kv", ch)
        for t in range(2):
            for n in range(2):
                s = pf[c, t, n, rows, :] + rq[l, t, n, rows, :].astype(F32)
                sf[n, t, rows, :] = s
                sb[l, n, t, rows, :] = s.astype(BF16)
        exchange("kvx", l, ch, [(sb.at[l, 1 - xc, :, rows], xr.at[l, :, rows], {"x": across})], xr.at[l, :, rows])

    def reduce_u(l, ch):
        rows = pl.ds(ch * R, R)
        arrived("u", ch)
        us = uf[c, rows, :] + ur[l, rows, :].astype(F32)
        usf[rows, :] = us
        usb[l, rows, :] = us.astype(BF16)
        exchange("ux", l, ch, [(usb.at[l, rows], ux.at[l, rows], {"x": across})], ux.at[l, rows])

    def rope(t, rows):
        tf = t.astype(F32)
        return (tf * cosb[rows, :] + pltpu.roll(tf, D // 2, 1) * sinb[rows, :]).astype(BF16)

    def stage_q(l, ch):
        rows = pl.ds(ch * R, R)
        arrived("q", ch)
        q = qf[xi, rows, :]
        for d in range(NX - 1):
            q = q + qr[l, d, rows, :].astype(F32)
        qv[rows, :] = rope(q.astype(BF16), rows)

    rowid = lax.broadcasted_iota(jnp.int32, (G, D), 0)
    pos = lax.broadcasted_iota(jnp.int32, (R, S), 1).astype(F32)
    scale = D ** -0.5

    ready, flipped, scored = set(), {}, {}

    def need_keys(l, ch):
        if (l, ch) not in ready:
            ready.add((l, ch))
            need_cache(kbuf, sem_k, ch)

    def transpose(l, ch):
        need_keys(l, ch)
        g = flipped.get((l, ch), 0)
        flipped[l, ch] = g + 1
        for b in range(ch * R + g * G, ch * R + (g + 1) * G):
            for j in range(S // D):
                kbuf[b, pl.ds(j * D, D), :] = kbuf[b, pl.ds(j * D, D), :].T

    def scores(l, ch):
        need_keys(l, ch)
        first = scored.get((l, ch), 0)
        scored[l, ch] = first + gpc // 2
        for g in range(first, first + gpc // 2):
            base = ch * R + g * G
            rows = pl.ds(base, G)
            q = qv[rows, :].astype(F32)
            s = jnp.zeros((G, S), F32)
            for i in range(0, G, 2):
                lhs = jnp.concatenate([jnp.where(rowid == i, q, 0.0), jnp.where(rowid == i + 1, q, 0.0)],
                                      axis=1).astype(BF16)
                if g < flipped.get((l, ch), 0):
                    keys = [jnp.concatenate([kbuf[base + i + e, pl.ds(j * D, D), :] for j in range(S // D)], axis=1)
                            for e in range(2)]
                    s = s + _dot(lhs, jnp.concatenate(keys, axis=0))
                else:
                    s = s + _dot_t(lhs, jnp.concatenate([kbuf[base + i], kbuf[base + i + 1]], axis=1))
            sbuf[rows, :] = s
        if scored[l, ch] == gpc and l + 1 < L:
            load_cache(kc_in, kbuf, sem_k, l + 1, ch)

    def softmax(l, ch):
        rows = pl.ds(ch * R, R)
        s = jnp.where(pos < lenb[rows, :][:, :1], sbuf[rows, :] * scale, -jnp.inf)
        m = jnp.max(s, axis=1, keepdims=True)
        p = jnp.exp(s - m)
        pbuf[rows, :] = p.astype(BF16)
        mbuf[rows, :] = jnp.broadcast_to(m, (R, D))
        dbuf[rows, :] = jnp.broadcast_to(jnp.sum(p, axis=1, keepdims=True), (R, D))

    def values(l, ch):
        need_cache(vbuf, sem_v, ch)
        for g in range(gpc):
            base = ch * R + g * G
            rows = pl.ds(base, G)
            p = pbuf[rows, :]
            o = jnp.zeros((G, D), F32)
            for i in range(0, G, 2):
                t = _dot(p, jnp.concatenate([vbuf[base + i], vbuf[base + i + 1]], axis=1))
                o = o + jnp.where(rowid == i, t[:, :D], jnp.where(rowid == i + 1, t[:, D:], 0.0))
            obuf[rows, :] = o
        if l + 1 < L:
            load_cache(vc_in, vbuf, sem_v, l + 1, ch)

    def stage_kv(l, ch):
        rows = pl.ds(ch * R, R)
        arrived("kvx", ch)
        k = rope((sf[xc, 0, rows, :] + xr[l, 0, rows, :].astype(F32)).astype(BF16), rows)
        v = (sf[xc, 1, rows, :] + xr[l, 1, rows, :].astype(F32)).astype(BF16)
        k_out[l, rows, :] = k
        v_out[l, rows, :] = v
        s_new = jnp.sum(qv[rows, :].astype(F32) * k.astype(F32), axis=1, keepdims=True) * scale
        m_c = mbuf[rows, :]
        m = jnp.maximum(m_c, s_new)
        a = jnp.exp(m_c - m)
        p_new = jnp.exp(s_new - m)
        o = (a * obuf[rows, :] + p_new * v.astype(F32)) / (a * dbuf[rows, :] + p_new)
        og[l, xi, rows, :] = o.astype(BF16)

    def send_o(l, ch):
        rows = pl.ds(ch * R, R)
        exchange("o", l, ch, [(og.at[l, xi, rows], og.at[l, xi, rows], {"x": lax.rem(xi + d, NX)}) for d in (2, 1, 3)],
                 og.at[l, pl.ds(0, NX - 1), rows])

    def stage_f(l, ch):
        rows = pl.ds(ch * R, R)
        arrived("ux", ch)
        u = (usf[rows, :] + ux[l, rows, :].astype(F32)).astype(BF16)
        fb[l, c, rows, :] = jax.nn.gelu(u.astype(F32), approximate=True).astype(BF16)
        exchange("f", l, ch, [(fb.at[l, c, rows], fb.at[l, c, rows], {"x": partner})], fb.at[l, 0, rows])

    def stage_mlp(l, ch):
        rows = pl.ds(ch * R, R)
        arrived("f", ch)
        if ch == 0:
            need_w(l, 3)
        f = jnp.concatenate([fb[l, 0, rows, :], fb[l, 1, rows, :]], axis=1)
        for n in range(2):
            acc = _dot(f, wout[l, :, pl.ds(n * 256, 256)])
            zf[2 * n, rows, :] = acc[:, :D]
            zf[2 * n + 1, rows, :] = acc[:, D:]

    def stage_out(l, ch):
        rows = pl.ds(ch * R, R)
        arrived("o", ch)
        if ch == 0:
            need_w(l, 2)
        o = jnp.concatenate([og[l, j, rows, :] for j in range(NX)], axis=1)
        for n in range(2):
            acc = _dot(o, wo[l, :, pl.ds(n * 256, 256)])
            for m in range(2):
                a = acc[:, m * D:(m + 1) * D] + zf[2 * n + m, rows, :]
                zf[2 * n + m, rows, :] = a
                zb[l, 2 * n + m, rows, :] = a.astype(BF16)
        tos = [lax.rem(yi + d, NY) for d in range(NY)]
        exchange("y", l, ch, [(zb.at[l, tos[d], rows], zr.at[l, d - 1, rows], {"yz": tos[d]}) for d in (3, 1, 2)],
                 zr.at[l, :, rows])
        if ch == nch - 1 and l + 1 < L:
            load_second(l + 1)

    def stage_h(l, ch):
        rows = pl.ds(ch * R, R)
        arrived("y", ch)
        y = zf[yi, rows, :]
        for d in range(NY - 1):
            y = y + zr[l, d, rows, :].astype(F32)
        hn = (hg[l, yi, rows, :].astype(F32) + y.astype(BF16).astype(F32)).astype(BF16)
        if l + 1 < L:
            hg[l + 1, yi, rows, :] = hn
            stats(l + 1, ch, hn.astype(F32))
            send_h(l + 1, ch)
        else:
            h_out[rows, :] = hn

    stages = dict(IN=stage_in, SQ=send_q, JN=stage_in_rest, RKV=reduce_kv, RU=reduce_u, Q=stage_q, QK=scores, X=transpose, KV=stage_kv, SM=softmax, PV=values,
                  SO=send_o, F=stage_f, MLP=stage_mlp, OUT=stage_out, H=stage_h)
    for step in ORDER.split():
        with jax.named_scope(step):
            chunks = range(nch) if step[-2] == "*" else ("AB".index(step[-2]),)
            stages[step[:-2]](int(step[-1]), chunks if step[:2] in ("IN", "JN") else chunks[0])
    for kind, ch in list(open_sends):
        drain(kind, ch)


def _tail(h_in, k_in, v_in, h_out, k_out, v_out, sem):
    cps = [pltpu.make_async_copy(a, o, sem.at[n])
           for n, (a, o) in enumerate(((k_in, k_out), (v_in, v_out), (h_in, h_out)))]
    for cp in cps:
        cp.start()
    for cp in cps:
        cp.wait()


def solution(mesh):
    nch = 2
    act = P(None, ('x', 'yz'))
    w_first = P(None, 'x', 'yz')
    w_second = P(None, 'yz', 'x')
    cache = P(None, None, ('yz', 'x'), None, None)
    new = P(None, None, ('yz', 'x'), None)
    inv_half = 10000.0 ** (-np.arange(D // 2, dtype=np.float64) / (D // 2))
    inv_np = np.concatenate([inv_half, inv_half]).astype(np.float32)[None]

    def body(h, g, wq, wk, wv, w_in, wo, w_out, kc, vc, lens):
        any_spec = pl.BlockSpec(memory_space=pl.ANY)
        vm_spec = pl.BlockSpec(memory_space=pltpu.VMEM)
        shapes = ((B, D), (L, B, D), (L, B, D))
        vm = pltpu.VMEM
        dma = pltpu.SemaphoreType.DMA
        scratch = [
            vm((B, S, D), BF16), vm((B, S, D), BF16),
            vm((L, 3, 512, 512), BF16), vm((L, 512, 2048), BF16), vm((L, 512, 512), BF16), vm((L, 2048, 512), BF16),
            vm((NY, L, D), BF16), vm((1, B), jnp.int32), vm((1, D), F32),
            vm((B, D), F32), vm((B, D), F32), vm((B, D), F32),
            vm((L, NY, B, D), BF16),
            vm((L, nch, NX * NY, 1, B), F32),
            vm((NX, B, D), F32),
            vm((L, NX, B, D), BF16),
            vm((L, NX - 1, B, D), BF16),
            vm((2, 2, 2, B, D), F32),
            vm((L, 2, 2, 2, B, D), BF16),
            vm((L, 2, 2, B, D), BF16),
            vm((2, 2, B, D), F32),
            vm((L, 2, 2, B, D), BF16),
            vm((L, 2, B, D), BF16),
            vm((2, B, 1024), F32),
            vm((L, 2, B, 1024), BF16),
            vm((L, B, 1024), BF16),
            vm((B, 1024), F32),
            vm((L, B, 1024), BF16),
            vm((L, B, 1024), BF16),
            vm((L, 2, B, 1024), BF16),
            vm((L, NX, B, D), BF16),
            vm((NY, B, D), F32),
            vm((L, NY, B, D), BF16),
            vm((L, NY - 1, B, D), BF16),
            vm((B, NY * D), BF16), vm((B, D), BF16), vm((B, D), F32),
            vm((B, S), F32), vm((B, S), BF16), vm((B, D), F32), vm((B, D), F32),
            dma((4,)), dma((4,)), dma((nch,)), dma((nch,)), dma((2,)),
            dma((len(KINDS), nch)), dma((len(KINDS), nch)),
        ]
        h_new, k_new, v_new = pl.pallas_call(
            functools.partial(_kernel, nch),
            out_shape=tuple(vm(n, BF16) for n in shapes),
            in_specs=[any_spec] * 12,
            out_specs=(vm_spec,) * 3,
            scratch_shapes=scratch,
            compiler_params=pltpu.CompilerParams(collective_id=0, has_side_effects=True,
                                                 vmem_limit_bytes=66_000_000),
            name="decode_step",
        )(h, g, wq, wk, wv, w_in, wo, w_out, kc.reshape(L, B, S, D), vc.reshape(L, B, S, D),
          lens.reshape(1, B), jnp.asarray(inv_np))
        h_new, k_new, v_new = pl.pallas_call(
            _tail,
            out_shape=tuple(jax.ShapeDtypeStruct(n, BF16) for n in shapes),
            in_specs=[vm_spec] * 3,
            out_specs=(any_spec,) * 3,
            scratch_shapes=[dma((3,))],
            name="results",
        )(*(pltpu.with_memory_space_constraint(a, pltpu.VMEM) for a in (h_new, k_new, v_new)))
        return h_new, k_new.reshape(L, B, 1, D), v_new.reshape(L, B, 1, D)

    return jax.shard_map(
        body, mesh=mesh,
        in_specs=(act, act, w_first, w_first, w_first, w_first, w_second, w_second, cache, cache, P(None)),
        out_specs=(act, new, new), check_vma=False)
```

```python
import functools

import jax
import jax.numpy as jnp
import numpy as np
from jax import lax
from jax.experimental import pallas as pl
from jax.experimental.pallas import tpu as pltpu
from jax.sharding import PartitionSpec as P

EPS = 1e-6
MESH = pl.DeviceIdType.MESH
F32 = jnp.float32
BF16 = jnp.bfloat16

L = 2
B = 128
D = 128
S = 512
NX = 4
NY = 4
E = 2048
G = 16
NG = B // G


KINDS = {k: n for n, k in enumerate(("s", "h", "q", "kv", "kvx", "u", "ux", "f", "o", "y"))}
ORDER = ("IN*0 SQA0 SQB0 JN*0 XA0 RKVA0 XA0 RUA0 XA0 XA0 QA0 QKA0 QKA0 RKVB0 RUB0 SMA0 PVA0 KVA0 SOA0 RUB0 QB0 QKB0 QKB0 "
         "FA0 SMB0 PVB0 KVB0 SOB0 MLPA0 OUTA0 XA1 FB0 XA1 XA1 MLPB0 XA1 OUTB0 XB1 HA0 XB1 XB1 XB1 HB0 INA1 SQA1 JNA1 RKVA1 "
         "RUA1 INB1 SQB1 RUA1 JNB1 QA1 QKA1 QKA1 RKVB1 RUB1 SMA1 PVA1 KVA1 SOA1 QB1 QKB1 QKB1 SMB1 PVB1 KVB1 SOB1 FA1 FB1 "
         "MLPA1 OUTA1 MLPB1 OUTB1 HA1 HB1").split()


def _dot(a, b):
    return jnp.dot(a, b, preferred_element_type=F32)


def _dot_t(a, b):
    return lax.dot_general(a, b, (((1,), (1,)), ((), ())), preferred_element_type=F32)


def _kernel(nch, h_in, g_in, wq_in, wk_in, wv_in, win_in, wo_in, wout_in, kc_in, vc_in, lens_in, inv_in,
            h_out, k_out, v_out,
            kbuf, vbuf, wqkv, win, wo, wout, gg, lrow, inv, cosb, sinb, lenb,
            hg, ssb, qf, qb, qr, pf, pb, rq, sf, sb, xr, uf, ub, ur, usf, usb, ux, fb, og, zf, zb, zr,
            xbuf, qv, obuf, sbuf, pbuf, mbuf, dbuf,
            sem_in, sem_w, sem_k, sem_v, g_sem, send_sem, recv_sem):
    R = B // nch
    xi = lax.axis_index("x")
    yi = lax.axis_index("yz")
    c = lax.rem(xi, 2)
    xc = lax.div(xi, 2)
    partner = xi + 1 - 2 * c
    across = lax.rem(xi + 2, NX)
    open_sends = {}

    def exchange(kind, l, ch, copies, region, first=True):
        ss, rs = send_sem.at[KINDS[kind], ch], recv_sem.at[KINDS[kind], ch]
        if first:
            drain(kind, ch)
        for src, dst, dev in copies:
            pltpu.make_async_remote_copy(src_ref=src, dst_ref=dst, send_sem=ss, recv_sem=rs,
                                         device_id={"x": xi, "yz": yi, **dev}, device_id_type=MESH).start()
        open_sends[kind, ch] = region

    def drain(kind, ch):
        region = open_sends.pop((kind, ch), None)
        if region is not None:
            pltpu.make_async_copy(region, region, send_sem.at[KINDS[kind], ch]).wait()

    def arrived(kind, ch):
        region = open_sends[kind, ch]
        with jax.named_scope(f"w_{kind}_{ch}"):
            pltpu.make_async_copy(region, region, recv_sem.at[KINDS[kind], ch]).wait()

    def load(src, dst, sem):
        cp = pltpu.make_async_copy(src, dst, sem)
        cp.start()
        return cp

    in_h = load(h_in, hg.at[0, yi], sem_in.at[0])
    in_g = load(g_in, gg.at[yi], sem_in.at[1])
    in_l = load(lens_in, lrow, sem_in.at[2])
    in_i = load(inv_in, inv, sem_in.at[3])

    def load_first(l):
        for n, w in enumerate((wq_in, wk_in, wv_in)):
            load(w.at[l], wqkv.at[l, n], sem_w.at[0])
        load(win_in.at[l], win.at[l], sem_w.at[1])

    def load_second(l):
        load(wo_in.at[l], wo.at[l], sem_w.at[2])
        load(wout_in.at[l], wout.at[l], sem_w.at[3])

    def need_w(l, n):
        ref = (wqkv, win, wo, wout)[n].at[l]
        pltpu.make_async_copy(ref, ref, sem_w.at[n]).wait()

    load_first(0)

    barrier = pltpu.get_barrier_semaphore()
    for dx in range(NX):
        for dy in range(NY):
            if dx or dy:
                pl.semaphore_signal(barrier, inc=1, device_id={"yz": lax.rem(yi + dy, NY), "x": lax.rem(xi + dx, NX)},
                                    device_id_type=MESH)

    eye = (lax.broadcasted_iota(jnp.int32, (R, B), 0) == lax.broadcasted_iota(jnp.int32, (R, B), 1))

    def stats(l, ch, hb):
        col = jnp.sum(hb * hb, axis=1, keepdims=True)
        ssb[l, ch, 0] = jnp.sum(jnp.where(eye, col, 0.0), axis=0, keepdims=True)

    def send_h(l, ch):
        rows = pl.ds(ch * R, R)
        exchange("s", l, ch,
                 [(ssb.at[l, ch, 0], ssb.at[l, ch, dx * NY + dy],
                   {"x": lax.rem(xi + dx, NX), "yz": lax.rem(yi + dy, NY)})
                  for dx in (2, 1, 3, 0) for dy in (3, 1, 2, 0) if dx or dy],
                 ssb.at[l, ch, pl.ds(1, NX * NY - 1)])
        exchange("h", l, ch,
                 [(hg.at[l, yi, rows], hg.at[l, yi, rows], {"yz": lax.rem(yi + d, NY)}) for d in (3, 1, 2)],
                 hg.at[l, pl.ds(0, NY - 1), rows])

    in_h.wait()
    in_g.wait()
    for ch in range(nch):
        stats(0, ch, hg[0, yi, pl.ds(ch * R, R), :].astype(F32))
    with jax.named_scope('barrier_wait'):
        pl.semaphore_wait(barrier, NX * NY - 1)
    for ch in range(nch):
        send_h(0, ch)
    for d in (1, 2, 3):
        pltpu.make_async_remote_copy(src_ref=gg.at[yi], dst_ref=gg.at[yi], send_sem=g_sem.at[0], recv_sem=g_sem.at[1],
                                     device_id={"x": xi, "yz": lax.rem(yi + d, NY)}, device_id_type=MESH).start()

    def load_cache(src, buf, sem, l, ch):
        for grp in range(ch * gpc, (ch + 1) * gpc):
            seqs = pl.ds(grp * G, G)
            load(src.at[l, seqs], buf.at[seqs], sem.at[ch])

    def need_cache(buf, sem, ch):
        ref = buf.at[pl.ds(ch * R, R)]
        pltpu.make_async_copy(ref, ref, sem.at[ch]).wait()

    gpc = NG // nch
    for ch in range(nch):
        load_cache(kc_in, kbuf, sem_k, 0, ch)
        load_cache(vc_in, vbuf, sem_v, 0, ch)
    load_second(0)

    in_l.wait()
    in_i.wait()
    eye_b = (lax.broadcasted_iota(jnp.int32, (B, B), 0) == lax.broadcasted_iota(jnp.int32, (B, B), 1))
    lcol = jnp.sum(jnp.where(eye_b, lrow[...].astype(F32), 0.0), axis=1, keepdims=True)
    lenb[...] = jnp.broadcast_to(lcol, (B, D))
    ang = lcol * inv[...]
    cosb[...] = jnp.cos(ang)
    half = lax.broadcasted_iota(jnp.int32, (B, D), 1) < D // 2
    sn = jnp.sin(ang)
    sinb[...] = jnp.where(half, -sn, sn)

    def stage_in(l, chunks):
        span = pl.ds(chunks[0] * R, R * len(chunks))
        scales = []
        for ch in chunks:
            arrived("h", ch)
            arrived("s", ch)
            row = ssb[l, ch, 0]
            for slot in range(1, NX * NY):
                row = row + ssb[l, ch, slot]
            col = jnp.sum(jnp.where(eye, row, 0.0), axis=1, keepdims=True)
            scales.append(lax.rsqrt(col / E + EPS))
        r = jnp.concatenate(scales, axis=0)
        if 0 in chunks:
            if l == 0:
                ref = gg.at[pl.ds(0, NY - 1)]
                pltpu.make_async_copy(ref, ref, g_sem.at[1]).wait()
                pltpu.make_async_copy(ref, ref, g_sem.at[0]).wait()
            need_w(l, 0)
            need_w(l, 1)
        xs = []
        for j in range(NY):
            gj = gg[j, pl.ds(l, 1), :].astype(F32)
            xs.append((hg[l, j, span, :].astype(F32) * r * gj).astype(BF16))
        x = jnp.concatenate(xs, axis=1)
        xbuf[span, :] = x
        for n in range(2):
            acc = _dot(x, wqkv[l, 0, :, pl.ds(n * 256, 256)])
            for m in range(2):
                a = acc[:, m * D:(m + 1) * D]
                qf[2 * n + m, span, :] = a
                qb[l, 2 * n + m, span, :] = a.astype(BF16)

    def send_q(l, ch):
        rows = pl.ds(ch * R, R)
        tos = [lax.rem(xi + d, NX) for d in range(NX)]
        exchange("q", l, ch, [(qb.at[l, tos[d], rows], qr.at[l, d - 1, rows], {"x": tos[d]}) for d in (2, 1, 3)],
                 qr.at[l, :, rows])

    def stage_in_rest(l, chunks):
        span = pl.ds(chunks[0] * R, R * len(chunks))
        x = xbuf[span, :]
        for t in range(2):
            for n in range(2):
                acc = _dot(x, wqkv[l, t + 1, :, pl.ds(n * 256, 256)])
                for cc in range(2):
                    a = acc[:, cc * D:(cc + 1) * D]
                    pf[cc, t, n, span, :] = a
                    pb[l, cc, t, n, span, :] = a.astype(BF16)
        for ch in chunks:
            rows = pl.ds(ch * R, R)
            exchange("kv", l, ch, [(pb.at[l, 1 - c, :, :, rows], rq.at[l, :, :, rows], {"x": partner})],
                     rq.at[l, :, :, rows])
        for n in range(8):
            acc = _dot(x, win[l, :, pl.ds(n * 256, 256)])
            cols = pl.ds((n % 4) * 256, 256)
            uf[n // 4, span, cols] = acc
            ub[l, n // 4, span, cols] = acc.astype(BF16)
        for ch in chunks:
            rows = pl.ds(ch * R, R)
            exchange("u", l, ch, [(ub.at[l, 1 - c, rows], ur.at[l, rows], {"x": partner})], ur.at[l, rows])
        if nch - 1 in chunks and l + 1 < L:
            load_first(l + 1)

    def reduce_kv(l, ch):
        rows = pl.ds(ch * R, R)
        arrived("kv", ch)
        for t in range(2):
            for n in range(2):
                s = pf[c, t, n, rows, :] + rq[l, t, n, rows, :].astype(F32)
                sf[n, t, rows, :] = s
                sb[l, n, t, rows, :] = s.astype(BF16)
        exchange("kvx", l, ch, [(sb.at[l, 1 - xc, :, rows], xr.at[l, :, rows], {"x": across})], xr.at[l, :, rows])

    u_done = {}

    def reduce_u(l, ch):
        pieces = ORDER.count(f"RU{'AB'[ch]}{l}")
        piece = u_done.get((l, ch), 0)
        u_done[l, ch] = piece + 1
        if piece == 0:
            arrived("u", ch)
        rows = pl.ds(ch * R + piece * (R // pieces), R // pieces)
        us = uf[c, rows, :] + ur[l, rows, :].astype(F32)
        usf[rows, :] = us
        usb[l, rows, :] = us.astype(BF16)
        exchange("ux", l, ch, [(usb.at[l, rows], ux.at[l, rows], {"x": across})], ux.at[l, pl.ds(ch * R, R)],
                 first=piece == 0)

    def rope(t, rows):
        tf = t.astype(F32)
        return (tf * cosb[rows, :] + pltpu.roll(tf, D // 2, 1) * sinb[rows, :]).astype(BF16)

    def stage_q(l, ch):
        rows = pl.ds(ch * R, R)
        arrived("q", ch)
        q = qf[xi, rows, :]
        for d in range(NX - 1):
            q = q + qr[l, d, rows, :].astype(F32)
        qv[rows, :] = rope(q.astype(BF16), rows)

    rowid = lax.broadcasted_iota(jnp.int32, (G, D), 0)
    pos = lax.broadcasted_iota(jnp.int32, (R, S), 1).astype(F32)
    scale = D ** -0.5

    ready, flipped, scored = set(), {}, {}

    def need_keys(l, ch):
        if (l, ch) not in ready:
            ready.add((l, ch))
            need_cache(kbuf, sem_k, ch)

    def transpose(l, ch):
        need_keys(l, ch)
        g = flipped.get((l, ch), 0)
        flipped[l, ch] = g + 1
        for b in range(ch * R + g * G, ch * R + (g + 1) * G):
            for j in range(S // D):
                kbuf[b, pl.ds(j * D, D), :] = kbuf[b, pl.ds(j * D, D), :].T

    def scores(l, ch):
        need_keys(l, ch)
        first = scored.get((l, ch), 0)
        scored[l, ch] = first + gpc // 2
        for g in range(first, first + gpc // 2):
            base = ch * R + g * G
            rows = pl.ds(base, G)
            q = qv[rows, :].astype(F32)
            s = jnp.zeros((G, S), F32)
            for i in range(0, G, 2):
                lhs = jnp.concatenate([jnp.where(rowid == i, q, 0.0), jnp.where(rowid == i + 1, q, 0.0)],
                                      axis=1).astype(BF16)
                if g < flipped.get((l, ch), 0):
                    keys = [jnp.concatenate([kbuf[base + i + e, pl.ds(j * D, D), :] for j in range(S // D)], axis=1)
                            for e in range(2)]
                    s = s + _dot(lhs, jnp.concatenate(keys, axis=0))
                else:
                    s = s + _dot_t(lhs, jnp.concatenate([kbuf[base + i], kbuf[base + i + 1]], axis=1))
            sbuf[rows, :] = s
        if scored[l, ch] == gpc and l + 1 < L:
            load_cache(kc_in, kbuf, sem_k, l + 1, ch)

    def softmax(l, ch):
        rows = pl.ds(ch * R, R)
        s = jnp.where(pos < lenb[rows, :][:, :1], sbuf[rows, :] * scale, -jnp.inf)
        m = jnp.max(s, axis=1, keepdims=True)
        p = jnp.exp(s - m)
        pbuf[rows, :] = p.astype(BF16)
        mbuf[rows, :] = jnp.broadcast_to(m, (R, D))
        dbuf[rows, :] = jnp.broadcast_to(jnp.sum(p, axis=1, keepdims=True), (R, D))

    def values(l, ch):
        need_cache(vbuf, sem_v, ch)
        for g in range(gpc):
            base = ch * R + g * G
            rows = pl.ds(base, G)
            p = pbuf[rows, :]
            o = jnp.zeros((G, D), F32)
            for i in range(0, G, 2):
                t = _dot(p, jnp.concatenate([vbuf[base + i], vbuf[base + i + 1]], axis=1))
                o = o + jnp.where(rowid == i, t[:, :D], jnp.where(rowid == i + 1, t[:, D:], 0.0))
            obuf[rows, :] = o
        if l + 1 < L:
            load_cache(vc_in, vbuf, sem_v, l + 1, ch)

    def stage_kv(l, ch):
        rows = pl.ds(ch * R, R)
        arrived("kvx", ch)
        k = rope((sf[xc, 0, rows, :] + xr[l, 0, rows, :].astype(F32)).astype(BF16), rows)
        v = (sf[xc, 1, rows, :] + xr[l, 1, rows, :].astype(F32)).astype(BF16)
        k_out[l, rows, :] = k
        v_out[l, rows, :] = v
        s_new = jnp.sum(qv[rows, :].astype(F32) * k.astype(F32), axis=1, keepdims=True) * scale
        m_c = mbuf[rows, :]
        m = jnp.maximum(m_c, s_new)
        a = jnp.exp(m_c - m)
        p_new = jnp.exp(s_new - m)
        o = (a * obuf[rows, :] + p_new * v.astype(F32)) / (a * dbuf[rows, :] + p_new)
        og[l, xi, rows, :] = o.astype(BF16)

    def send_o(l, ch):
        rows = pl.ds(ch * R, R)
        exchange("o", l, ch, [(og.at[l, xi, rows], og.at[l, xi, rows], {"x": lax.rem(xi + d, NX)}) for d in (2, 1, 3)],
                 og.at[l, pl.ds(0, NX - 1), rows])

    def stage_f(l, ch):
        rows = pl.ds(ch * R, R)
        arrived("ux", ch)
        u = (usf[rows, :] + ux[l, rows, :].astype(F32)).astype(BF16)
        fb[l, c, rows, :] = jax.nn.gelu(u.astype(F32), approximate=True).astype(BF16)
        exchange("f", l, ch, [(fb.at[l, c, rows], fb.at[l, c, rows], {"x": partner})], fb.at[l, 0, rows])

    def stage_mlp(l, ch):
        rows = pl.ds(ch * R, R)
        arrived("f", ch)
        if ch == 0:
            need_w(l, 3)
        f = jnp.concatenate([fb[l, 0, rows, :], fb[l, 1, rows, :]], axis=1)
        for n in range(2):
            acc = _dot(f, wout[l, :, pl.ds(n * 256, 256)])
            zf[2 * n, rows, :] = acc[:, :D]
            zf[2 * n + 1, rows, :] = acc[:, D:]

    def stage_out(l, ch):
        rows = pl.ds(ch * R, R)
        arrived("o", ch)
        if ch == 0:
            need_w(l, 2)
        o = jnp.concatenate([og[l, j, rows, :] for j in range(NX)], axis=1)
        for n in range(2):
            acc = _dot(o, wo[l, :, pl.ds(n * 256, 256)])
            for m in range(2):
                a = acc[:, m * D:(m + 1) * D] + zf[2 * n + m, rows, :]
                zf[2 * n + m, rows, :] = a
                zb[l, 2 * n + m, rows, :] = a.astype(BF16)
        tos = [lax.rem(yi + d, NY) for d in range(NY)]
        exchange("y", l, ch, [(zb.at[l, tos[d], rows], zr.at[l, d - 1, rows], {"yz": tos[d]}) for d in (3, 1, 2)],
                 zr.at[l, :, rows])
        if ch == nch - 1 and l + 1 < L:
            load_second(l + 1)

    def stage_h(l, ch):
        rows = pl.ds(ch * R, R)
        arrived("y", ch)
        y = zf[yi, rows, :]
        for d in range(NY - 1):
            y = y + zr[l, d, rows, :].astype(F32)
        hn = (hg[l, yi, rows, :].astype(F32) + y.astype(BF16).astype(F32)).astype(BF16)
        if l + 1 < L:
            hg[l + 1, yi, rows, :] = hn
            stats(l + 1, ch, hn.astype(F32))
            send_h(l + 1, ch)
        else:
            h_out[rows, :] = hn

    stages = dict(IN=stage_in, SQ=send_q, JN=stage_in_rest, RKV=reduce_kv, RU=reduce_u, Q=stage_q, QK=scores, X=transpose, KV=stage_kv, SM=softmax, PV=values,
                  SO=send_o, F=stage_f, MLP=stage_mlp, OUT=stage_out, H=stage_h)
    for step in ORDER:
        with jax.named_scope(step):
            chunks = range(nch) if step[-2] == "*" else ("AB".index(step[-2]),)
            stages[step[:-2]](int(step[-1]), chunks if step[:2] in ("IN", "JN") else chunks[0])
    for kind, ch in list(open_sends):
        drain(kind, ch)


def _tail(h_in, k_in, v_in, h_out, k_out, v_out, sem):
    cps = [pltpu.make_async_copy(a, o, sem.at[n])
           for n, (a, o) in enumerate(((k_in, k_out), (v_in, v_out), (h_in, h_out)))]
    for cp in cps:
        cp.start()
    for cp in cps:
        cp.wait()


def solution(mesh):
    nch = 2
    act = P(None, ('x', 'yz'))
    w_first = P(None, 'x', 'yz')
    w_second = P(None, 'yz', 'x')
    cache = P(None, None, ('yz', 'x'), None, None)
    new = P(None, None, ('yz', 'x'), None)
    inv_half = 10000.0 ** (-np.arange(D // 2, dtype=np.float64) / (D // 2))
    inv_np = np.concatenate([inv_half, inv_half]).astype(np.float32)[None]

    def body(h, g, wq, wk, wv, w_in, wo, w_out, kc, vc, lens):
        any_spec = pl.BlockSpec(memory_space=pl.ANY)
        vm_spec = pl.BlockSpec(memory_space=pltpu.VMEM)
        shapes = ((B, D), (L, B, D), (L, B, D))
        vm = pltpu.VMEM
        dma = pltpu.SemaphoreType.DMA
        scratch = [
            vm((B, S, D), BF16), vm((B, S, D), BF16),
            vm((L, 3, 512, 512), BF16), vm((L, 512, 2048), BF16), vm((L, 512, 512), BF16), vm((L, 2048, 512), BF16),
            vm((NY, L, D), BF16), vm((1, B), jnp.int32), vm((1, D), F32),
            vm((B, D), F32), vm((B, D), F32), vm((B, D), F32),
            vm((L, NY, B, D), BF16),
            vm((L, nch, NX * NY, 1, B), F32),
            vm((NX, B, D), F32),
            vm((L, NX, B, D), BF16),
            vm((L, NX - 1, B, D), BF16),
            vm((2, 2, 2, B, D), F32),
            vm((L, 2, 2, 2, B, D), BF16),
            vm((L, 2, 2, B, D), BF16),
            vm((2, 2, B, D), F32),
            vm((L, 2, 2, B, D), BF16),
            vm((L, 2, B, D), BF16),
            vm((2, B, 1024), F32),
            vm((L, 2, B, 1024), BF16),
            vm((L, B, 1024), BF16),
            vm((B, 1024), F32),
            vm((L, B, 1024), BF16),
            vm((L, B, 1024), BF16),
            vm((L, 2, B, 1024), BF16),
            vm((L, NX, B, D), BF16),
            vm((NY, B, D), F32),
            vm((L, NY, B, D), BF16),
            vm((L, NY - 1, B, D), BF16),
            vm((B, NY * D), BF16), vm((B, D), BF16), vm((B, D), F32),
            vm((B, S), F32), vm((B, S), BF16), vm((B, D), F32), vm((B, D), F32),
            dma((4,)), dma((4,)), dma((nch,)), dma((nch,)), dma((2,)),
            dma((len(KINDS), nch)), dma((len(KINDS), nch)),
        ]
        h_new, k_new, v_new = pl.pallas_call(
            functools.partial(_kernel, nch),
            out_shape=tuple(vm(n, BF16) for n in shapes),
            in_specs=[any_spec] * 12,
            out_specs=(vm_spec,) * 3,
            scratch_shapes=scratch,
            compiler_params=pltpu.CompilerParams(collective_id=0, has_side_effects=True,
                                                 vmem_limit_bytes=66_000_000),
            name="decode_step",
        )(h, g, wq, wk, wv, w_in, wo, w_out, kc.reshape(L, B, S, D), vc.reshape(L, B, S, D),
          lens.reshape(1, B), jnp.asarray(inv_np))
        h_new, k_new, v_new = pl.pallas_call(
            _tail,
            out_shape=tuple(jax.ShapeDtypeStruct(n, BF16) for n in shapes),
            in_specs=[vm_spec] * 3,
            out_specs=(any_spec,) * 3,
            scratch_shapes=[dma((3,))],
            name="results",
        )(*(pltpu.with_memory_space_constraint(a, pltpu.VMEM) for a in (h_new, k_new, v_new)))
        return h_new, k_new.reshape(L, B, 1, D), v_new.reshape(L, B, 1, D)

    return jax.shard_map(
        body, mesh=mesh,
        in_specs=(act, act, w_first, w_first, w_first, w_first, w_second, w_second, cache, cache, P(None)),
        out_specs=(act, new, new), check_vma=False)
```

```python
import functools

import jax
import jax.numpy as jnp
import numpy as np
from jax import lax
from jax.experimental import pallas as pl
from jax.experimental.pallas import tpu as pltpu
from jax.sharding import PartitionSpec as P

EPS = 1e-6
MESH = pl.DeviceIdType.MESH
F32 = jnp.float32
BF16 = jnp.bfloat16

L = 2
B = 128
D = 128
S = 512
NX = 4
NY = 4
E = 2048
G = 16
NG = B // G


KINDS = {k: n for n, k in enumerate(("s", "h", "q", "kv", "kvx", "u", "ux", "f", "o", "y"))}
ORDER = ("IN*0 SQA0 SQB0 JN*0 XA0 RKVA0 XA0 RUA0 XA0 XA0 QA0 QKA0 QKA0 RKVB0 RUB0 SMA0 PVA0 KVA0 SOA0 RUB0 QB0 QKB0 QKB0 "
         "FA0 SMB0 PVB0 KVB0 SOB0 MLPA0 OUTA0 XA1 FB0 XA1 XA1 MLPB0 OUTB0 XA1 HA0 XB1 LVA0 XB1 XB1 LVB0 XB1 HB0 INA1 SQA1 JNA1 "
         "RKVA1 RUA1 INB1 SQB1 RUA1 JNB1 QA1 QKA1 QKA1 RKVB1 RUB1 SMA1 PVA1 KVA1 SOA1 QB1 QKB1 QKB1 SMB1 PVB1 KVB1 SOB1 FA1 "
         "MLPA1 FB1 OUTA1 MLPB1 OUTB1 HA1 HB1").split()


def _dot(a, b):
    return jnp.dot(a, b, preferred_element_type=F32)


def _dot_t(a, b):
    return lax.dot_general(a, b, (((1,), (1,)), ((), ())), preferred_element_type=F32)


def _kernel(nch, h_in, g_in, wq_in, wk_in, wv_in, win_in, wo_in, wout_in, kc_in, vc_in, lens_in, inv_in,
            h_out, k_out, v_out,
            kbuf, vbuf, wqkv, win, wo, wout, gg, lrow, inv, cosb, sinb, lenb,
            hg, ssb, qf, qb, qr, pf, pb, rq, sf, sb, xr, uf, ub, ur, usf, usb, ux, fb, og, zf, zb, zr,
            xbuf, qv, obuf, sbuf, pbuf, mbuf, dbuf,
            sem_in, sem_w, sem_k, sem_v, g_sem, send_sem, recv_sem):
    R = B // nch
    xi = lax.axis_index("x")
    yi = lax.axis_index("yz")
    c = lax.rem(xi, 2)
    xc = lax.div(xi, 2)
    partner = xi + 1 - 2 * c
    across = lax.rem(xi + 2, NX)
    open_sends = {}

    def exchange(kind, l, ch, copies, region, first=True):
        ss, rs = send_sem.at[KINDS[kind], ch], recv_sem.at[KINDS[kind], ch]
        if first:
            drain(kind, ch)
        for src, dst, dev in copies:
            pltpu.make_async_remote_copy(src_ref=src, dst_ref=dst, send_sem=ss, recv_sem=rs,
                                         device_id={"x": xi, "yz": yi, **dev}, device_id_type=MESH).start()
        open_sends[kind, ch] = region

    def drain(kind, ch):
        region = open_sends.pop((kind, ch), None)
        if region is not None:
            pltpu.make_async_copy(region, region, send_sem.at[KINDS[kind], ch]).wait()

    def arrived(kind, ch):
        region = open_sends[kind, ch]
        with jax.named_scope(f"w_{kind}_{ch}"):
            pltpu.make_async_copy(region, region, recv_sem.at[KINDS[kind], ch]).wait()

    def load(src, dst, sem):
        cp = pltpu.make_async_copy(src, dst, sem)
        cp.start()
        return cp

    in_h = load(h_in, hg.at[0, yi], sem_in.at[0])
    in_g = load(g_in, gg.at[yi], sem_in.at[1])
    in_l = load(lens_in, lrow, sem_in.at[2])
    in_i = load(inv_in, inv, sem_in.at[3])

    def load_first(l):
        for n, w in enumerate((wq_in, wk_in, wv_in)):
            load(w.at[l], wqkv.at[l, n], sem_w.at[0])
        load(win_in.at[l], win.at[l], sem_w.at[1])

    def load_second(l):
        load(wo_in.at[l], wo.at[l], sem_w.at[2])
        load(wout_in.at[l], wout.at[l], sem_w.at[3])

    def need_w(l, n):
        ref = (wqkv, win, wo, wout)[n].at[l]
        pltpu.make_async_copy(ref, ref, sem_w.at[n]).wait()

    load_first(0)

    barrier = pltpu.get_barrier_semaphore()
    for dx in range(NX):
        for dy in range(NY):
            if dx or dy:
                pl.semaphore_signal(barrier, inc=1, device_id={"yz": lax.rem(yi + dy, NY), "x": lax.rem(xi + dx, NX)},
                                    device_id_type=MESH)

    eye = (lax.broadcasted_iota(jnp.int32, (R, B), 0) == lax.broadcasted_iota(jnp.int32, (R, B), 1))

    def stats(l, ch, hb):
        col = jnp.sum(hb * hb, axis=1, keepdims=True)
        ssb[l, ch, 0] = jnp.sum(jnp.where(eye, col, 0.0), axis=0, keepdims=True)

    def send_h(l, ch):
        rows = pl.ds(ch * R, R)
        exchange("s", l, ch,
                 [(ssb.at[l, ch, 0], ssb.at[l, ch, dx * NY + dy],
                   {"x": lax.rem(xi + dx, NX), "yz": lax.rem(yi + dy, NY)})
                  for dx in (2, 1, 3, 0) for dy in (3, 1, 2, 0) if dx or dy],
                 ssb.at[l, ch, pl.ds(1, NX * NY - 1)])
        exchange("h", l, ch,
                 [(hg.at[l, yi, rows], hg.at[l, yi, rows], {"yz": lax.rem(yi + d, NY)}) for d in (3, 1, 2)],
                 hg.at[l, pl.ds(0, NY - 1), rows])

    in_h.wait()
    in_g.wait()
    for ch in range(nch):
        stats(0, ch, hg[0, yi, pl.ds(ch * R, R), :].astype(F32))
    with jax.named_scope('barrier_wait'):
        pl.semaphore_wait(barrier, NX * NY - 1)
    for ch in range(nch):
        send_h(0, ch)
    for d in (1, 2, 3):
        pltpu.make_async_remote_copy(src_ref=gg.at[yi], dst_ref=gg.at[yi], send_sem=g_sem.at[0], recv_sem=g_sem.at[1],
                                     device_id={"x": xi, "yz": lax.rem(yi + d, NY)}, device_id_type=MESH).start()

    def load_cache(src, buf, sem, l, ch):
        for grp in range(ch * gpc, (ch + 1) * gpc):
            seqs = pl.ds(grp * G, G)
            load(src.at[l, seqs], buf.at[seqs], sem.at[ch])

    def need_cache(buf, sem, ch):
        ref = buf.at[pl.ds(ch * R, R)]
        pltpu.make_async_copy(ref, ref, sem.at[ch]).wait()

    gpc = NG // nch
    for ch in range(nch):
        load_cache(kc_in, kbuf, sem_k, 0, ch)
        load_cache(vc_in, vbuf, sem_v, 0, ch)
    load_second(0)

    in_l.wait()
    in_i.wait()
    eye_b = (lax.broadcasted_iota(jnp.int32, (B, B), 0) == lax.broadcasted_iota(jnp.int32, (B, B), 1))
    lcol = jnp.sum(jnp.where(eye_b, lrow[...].astype(F32), 0.0), axis=1, keepdims=True)
    lenb[...] = jnp.broadcast_to(lcol, (B, D))
    ang = lcol * inv[...]
    cosb[...] = jnp.cos(ang)
    half = lax.broadcasted_iota(jnp.int32, (B, D), 1) < D // 2
    sn = jnp.sin(ang)
    sinb[...] = jnp.where(half, -sn, sn)

    def stage_in(l, chunks):
        span = pl.ds(chunks[0] * R, R * len(chunks))
        scales = []
        for ch in chunks:
            arrived("h", ch)
            arrived("s", ch)
            row = ssb[l, ch, 0]
            for slot in range(1, NX * NY):
                row = row + ssb[l, ch, slot]
            col = jnp.sum(jnp.where(eye, row, 0.0), axis=1, keepdims=True)
            scales.append(lax.rsqrt(col / E + EPS))
        r = jnp.concatenate(scales, axis=0)
        if 0 in chunks:
            if l == 0:
                ref = gg.at[pl.ds(0, NY - 1)]
                pltpu.make_async_copy(ref, ref, g_sem.at[1]).wait()
                pltpu.make_async_copy(ref, ref, g_sem.at[0]).wait()
            need_w(l, 0)
            need_w(l, 1)
        xs = []
        for j in range(NY):
            gj = gg[j, pl.ds(l, 1), :].astype(F32)
            xs.append((hg[l, j, span, :].astype(F32) * r * gj).astype(BF16))
        x = jnp.concatenate(xs, axis=1)
        xbuf[span, :] = x
        for n in range(2):
            acc = _dot(x, wqkv[l, 0, :, pl.ds(n * 256, 256)])
            for m in range(2):
                a = acc[:, m * D:(m + 1) * D]
                qf[2 * n + m, span, :] = a
                qb[l, 2 * n + m, span, :] = a.astype(BF16)

    def send_q(l, ch):
        rows = pl.ds(ch * R, R)
        tos = [lax.rem(xi + d, NX) for d in range(NX)]
        exchange("q", l, ch, [(qb.at[l, tos[d], rows], qr.at[l, d - 1, rows], {"x": tos[d]}) for d in (2, 1, 3)],
                 qr.at[l, :, rows])

    def stage_in_rest(l, chunks):
        span = pl.ds(chunks[0] * R, R * len(chunks))
        x = xbuf[span, :]
        for t in range(2):
            for n in range(2):
                acc = _dot(x, wqkv[l, t + 1, :, pl.ds(n * 256, 256)])
                for cc in range(2):
                    a = acc[:, cc * D:(cc + 1) * D]
                    pf[cc, t, n, span, :] = a
                    pb[l, cc, t, n, span, :] = a.astype(BF16)
        for ch in chunks:
            rows = pl.ds(ch * R, R)
            exchange("kv", l, ch, [(pb.at[l, 1 - c, :, :, rows], rq.at[l, :, :, rows], {"x": partner})],
                     rq.at[l, :, :, rows])
        for n in range(8):
            acc = _dot(x, win[l, :, pl.ds(n * 256, 256)])
            cols = pl.ds((n % 4) * 256, 256)
            uf[n // 4, span, cols] = acc
            ub[l, n // 4, span, cols] = acc.astype(BF16)
        for ch in chunks:
            rows = pl.ds(ch * R, R)
            exchange("u", l, ch, [(ub.at[l, 1 - c, rows], ur.at[l, rows], {"x": partner})], ur.at[l, rows])
        if nch - 1 in chunks and l + 1 < L:
            load_first(l + 1)

    def reduce_kv(l, ch):
        rows = pl.ds(ch * R, R)
        arrived("kv", ch)
        for t in range(2):
            for n in range(2):
                s = pf[c, t, n, rows, :] + rq[l, t, n, rows, :].astype(F32)
                sf[n, t, rows, :] = s
                sb[l, n, t, rows, :] = s.astype(BF16)
        exchange("kvx", l, ch, [(sb.at[l, 1 - xc, :, rows], xr.at[l, :, rows], {"x": across})], xr.at[l, :, rows])

    u_done = {}

    def reduce_u(l, ch):
        pieces = ORDER.count(f"RU{'AB'[ch]}{l}")
        piece = u_done.get((l, ch), 0)
        u_done[l, ch] = piece + 1
        if piece == 0:
            arrived("u", ch)
        rows = pl.ds(ch * R + piece * (R // pieces), R // pieces)
        us = uf[c, rows, :] + ur[l, rows, :].astype(F32)
        usf[rows, :] = us
        usb[l, rows, :] = us.astype(BF16)
        exchange("ux", l, ch, [(usb.at[l, rows], ux.at[l, rows], {"x": across})], ux.at[l, pl.ds(ch * R, R)],
                 first=piece == 0)

    def rope(t, rows):
        tf = t.astype(F32)
        return (tf * cosb[rows, :] + pltpu.roll(tf, D // 2, 1) * sinb[rows, :]).astype(BF16)

    def stage_q(l, ch):
        rows = pl.ds(ch * R, R)
        arrived("q", ch)
        q = qf[xi, rows, :]
        for d in range(NX - 1):
            q = q + qr[l, d, rows, :].astype(F32)
        qv[rows, :] = rope(q.astype(BF16), rows)

    rowid = lax.broadcasted_iota(jnp.int32, (G, D), 0)
    pos = lax.broadcasted_iota(jnp.int32, (R, S), 1).astype(F32)
    scale = D ** -0.5

    ready, flipped, scored = set(), {}, {}

    def need_keys(l, ch):
        if (l, ch) not in ready:
            ready.add((l, ch))
            need_cache(kbuf, sem_k, ch)

    def transpose(l, ch):
        need_keys(l, ch)
        g = flipped.get((l, ch), 0)
        flipped[l, ch] = g + 1
        for b in range(ch * R + g * G, ch * R + (g + 1) * G):
            for j in range(S // D):
                kbuf[b, pl.ds(j * D, D), :] = kbuf[b, pl.ds(j * D, D), :].T

    def scores(l, ch):
        need_keys(l, ch)
        first = scored.get((l, ch), 0)
        scored[l, ch] = first + gpc // 2
        for g in range(first, first + gpc // 2):
            base = ch * R + g * G
            rows = pl.ds(base, G)
            q = qv[rows, :].astype(F32)
            s = jnp.zeros((G, S), F32)
            for i in range(0, G, 2):
                lhs = jnp.concatenate([jnp.where(rowid == i, q, 0.0), jnp.where(rowid == i + 1, q, 0.0)],
                                      axis=1).astype(BF16)
                if g < flipped.get((l, ch), 0):
                    keys = [jnp.concatenate([kbuf[base + i + e, pl.ds(j * D, D), :] for j in range(S // D)], axis=1)
                            for e in range(2)]
                    s = s + _dot(lhs, jnp.concatenate(keys, axis=0))
                else:
                    s = s + _dot_t(lhs, jnp.concatenate([kbuf[base + i], kbuf[base + i + 1]], axis=1))
            sbuf[rows, :] = s
        if scored[l, ch] == gpc and l + 1 < L:
            load_cache(kc_in, kbuf, sem_k, l + 1, ch)

    def softmax(l, ch):
        rows = pl.ds(ch * R, R)
        s = jnp.where(pos < lenb[rows, :][:, :1], sbuf[rows, :] * scale, -jnp.inf)
        m = jnp.max(s, axis=1, keepdims=True)
        p = jnp.exp(s - m)
        pbuf[rows, :] = p.astype(BF16)
        mbuf[rows, :] = jnp.broadcast_to(m, (R, D))
        dbuf[rows, :] = jnp.broadcast_to(jnp.sum(p, axis=1, keepdims=True), (R, D))

    def values(l, ch):
        need_cache(vbuf, sem_v, ch)
        for g in range(gpc):
            base = ch * R + g * G
            rows = pl.ds(base, G)
            p = pbuf[rows, :]
            o = jnp.zeros((G, D), F32)
            for i in range(0, G, 2):
                t = _dot(p, jnp.concatenate([vbuf[base + i], vbuf[base + i + 1]], axis=1))
                o = o + jnp.where(rowid == i, t[:, :D], jnp.where(rowid == i + 1, t[:, D:], 0.0))
            obuf[rows, :] = o

    def load_values(l, ch):
        load_cache(vc_in, vbuf, sem_v, l + 1, ch)

    def stage_kv(l, ch):
        rows = pl.ds(ch * R, R)
        arrived("kvx", ch)
        k = rope((sf[xc, 0, rows, :] + xr[l, 0, rows, :].astype(F32)).astype(BF16), rows)
        v = (sf[xc, 1, rows, :] + xr[l, 1, rows, :].astype(F32)).astype(BF16)
        k_out[l, rows, :] = k
        v_out[l, rows, :] = v
        s_new = jnp.sum(qv[rows, :].astype(F32) * k.astype(F32), axis=1, keepdims=True) * scale
        m_c = mbuf[rows, :]
        m = jnp.maximum(m_c, s_new)
        a = jnp.exp(m_c - m)
        p_new = jnp.exp(s_new - m)
        o = (a * obuf[rows, :] + p_new * v.astype(F32)) / (a * dbuf[rows, :] + p_new)
        og[l, xi, rows, :] = o.astype(BF16)

    def send_o(l, ch):
        rows = pl.ds(ch * R, R)
        exchange("o", l, ch, [(og.at[l, xi, rows], og.at[l, xi, rows], {"x": lax.rem(xi + d, NX)}) for d in (2, 1, 3)],
                 og.at[l, pl.ds(0, NX - 1), rows])

    def stage_f(l, ch):
        rows = pl.ds(ch * R, R)
        arrived("ux", ch)
        u = (usf[rows, :] + ux[l, rows, :].astype(F32)).astype(BF16)
        fb[l, c, rows, :] = jax.nn.gelu(u.astype(F32), approximate=True).astype(BF16)
        exchange("f", l, ch, [(fb.at[l, c, rows], fb.at[l, c, rows], {"x": partner})], fb.at[l, 0, rows])

    def stage_mlp(l, ch):
        rows = pl.ds(ch * R, R)
        arrived("f", ch)
        if ch == 0:
            need_w(l, 3)
        f = jnp.concatenate([fb[l, 0, rows, :], fb[l, 1, rows, :]], axis=1)
        for n in range(2):
            acc = _dot(f, wout[l, :, pl.ds(n * 256, 256)])
            zf[2 * n, rows, :] = acc[:, :D]
            zf[2 * n + 1, rows, :] = acc[:, D:]

    def stage_out(l, ch):
        rows = pl.ds(ch * R, R)
        arrived("o", ch)
        if ch == 0:
            need_w(l, 2)
        o = jnp.concatenate([og[l, j, rows, :] for j in range(NX)], axis=1)
        for n in range(2):
            acc = _dot(o, wo[l, :, pl.ds(n * 256, 256)])
            for m in range(2):
                a = acc[:, m * D:(m + 1) * D] + zf[2 * n + m, rows, :]
                zf[2 * n + m, rows, :] = a
                zb[l, 2 * n + m, rows, :] = a.astype(BF16)
        tos = [lax.rem(yi + d, NY) for d in range(NY)]
        exchange("y", l, ch, [(zb.at[l, tos[d], rows], zr.at[l, d - 1, rows], {"yz": tos[d]}) for d in (3, 1, 2)],
                 zr.at[l, :, rows])
        if ch == nch - 1 and l + 1 < L:
            load_second(l + 1)

    def stage_h(l, ch):
        rows = pl.ds(ch * R, R)
        arrived("y", ch)
        y = zf[yi, rows, :]
        for d in range(NY - 1):
            y = y + zr[l, d, rows, :].astype(F32)
        hn = (hg[l, yi, rows, :].astype(F32) + y.astype(BF16).astype(F32)).astype(BF16)
        if l + 1 < L:
            hg[l + 1, yi, rows, :] = hn
            stats(l + 1, ch, hn.astype(F32))
            send_h(l + 1, ch)
        else:
            h_out[rows, :] = hn

    stages = dict(IN=stage_in, SQ=send_q, JN=stage_in_rest, RKV=reduce_kv, RU=reduce_u, Q=stage_q, QK=scores, X=transpose, KV=stage_kv, SM=softmax, PV=values, LV=load_values,
                  SO=send_o, F=stage_f, MLP=stage_mlp, OUT=stage_out, H=stage_h)
    for step in ORDER:
        with jax.named_scope(step):
            chunks = range(nch) if step[-2] == "*" else ("AB".index(step[-2]),)
            stages[step[:-2]](int(step[-1]), chunks if step[:2] in ("IN", "JN") else chunks[0])
    for kind, ch in list(open_sends):
        drain(kind, ch)


def _tail(h_in, k_in, v_in, h_out, k_out, v_out, sem):
    cps = [pltpu.make_async_copy(a, o, sem.at[n])
           for n, (a, o) in enumerate(((k_in, k_out), (v_in, v_out), (h_in, h_out)))]
    for cp in cps:
        cp.start()
    for cp in cps:
        cp.wait()


def solution(mesh):
    nch = 2
    act = P(None, ('x', 'yz'))
    w_first = P(None, 'x', 'yz')
    w_second = P(None, 'yz', 'x')
    cache = P(None, None, ('yz', 'x'), None, None)
    new = P(None, None, ('yz', 'x'), None)
    inv_half = 10000.0 ** (-np.arange(D // 2, dtype=np.float64) / (D // 2))
    inv_np = np.concatenate([inv_half, inv_half]).astype(np.float32)[None]

    def body(h, g, wq, wk, wv, w_in, wo, w_out, kc, vc, lens):
        any_spec = pl.BlockSpec(memory_space=pl.ANY)
        vm_spec = pl.BlockSpec(memory_space=pltpu.VMEM)
        shapes = ((B, D), (L, B, D), (L, B, D))
        vm = pltpu.VMEM
        dma = pltpu.SemaphoreType.DMA
        scratch = [
            vm((B, S, D), BF16), vm((B, S, D), BF16),
            vm((L, 3, 512, 512), BF16), vm((L, 512, 2048), BF16), vm((L, 512, 512), BF16), vm((L, 2048, 512), BF16),
            vm((NY, L, D), BF16), vm((1, B), jnp.int32), vm((1, D), F32),
            vm((B, D), F32), vm((B, D), F32), vm((B, D), F32),
            vm((L, NY, B, D), BF16),
            vm((L, nch, NX * NY, 1, B), F32),
            vm((NX, B, D), F32),
            vm((L, NX, B, D), BF16),
            vm((L, NX - 1, B, D), BF16),
            vm((2, 2, 2, B, D), F32),
            vm((L, 2, 2, 2, B, D), BF16),
            vm((L, 2, 2, B, D), BF16),
            vm((2, 2, B, D), F32),
            vm((L, 2, 2, B, D), BF16),
            vm((L, 2, B, D), BF16),
            vm((2, B, 1024), F32),
            vm((L, 2, B, 1024), BF16),
            vm((L, B, 1024), BF16),
            vm((B, 1024), F32),
            vm((L, B, 1024), BF16),
            vm((L, B, 1024), BF16),
            vm((L, 2, B, 1024), BF16),
            vm((L, NX, B, D), BF16),
            vm((NY, B, D), F32),
            vm((L, NY, B, D), BF16),
            vm((L, NY - 1, B, D), BF16),
            vm((B, NY * D), BF16), vm((B, D), BF16), vm((B, D), F32),
            vm((B, S), F32), vm((B, S), BF16), vm((B, D), F32), vm((B, D), F32),
            dma((4,)), dma((4,)), dma((nch,)), dma((nch,)), dma((2,)),
            dma((len(KINDS), nch)), dma((len(KINDS), nch)),
        ]
        h_new, k_new, v_new = pl.pallas_call(
            functools.partial(_kernel, nch),
            out_shape=tuple(vm(n, BF16) for n in shapes),
            in_specs=[any_spec] * 12,
            out_specs=(vm_spec,) * 3,
            scratch_shapes=scratch,
            compiler_params=pltpu.CompilerParams(collective_id=0, has_side_effects=True,
                                                 vmem_limit_bytes=66_000_000),
            name="decode_step",
        )(h, g, wq, wk, wv, w_in, wo, w_out, kc.reshape(L, B, S, D), vc.reshape(L, B, S, D),
          lens.reshape(1, B), jnp.asarray(inv_np))
        h_new, k_new, v_new = pl.pallas_call(
            _tail,
            out_shape=tuple(jax.ShapeDtypeStruct(n, BF16) for n in shapes),
            in_specs=[vm_spec] * 3,
            out_specs=(any_spec,) * 3,
            scratch_shapes=[dma((3,))],
            name="results",
        )(*(pltpu.with_memory_space_constraint(a, pltpu.VMEM) for a in (h_new, k_new, v_new)))
        return h_new, k_new.reshape(L, B, 1, D), v_new.reshape(L, B, 1, D)

    return jax.shard_map(
        body, mesh=mesh,
        in_specs=(act, act, w_first, w_first, w_first, w_first, w_second, w_second, cache, cache, P(None)),
        out_specs=(act, new, new), check_vma=False)
```

```python
import functools

import jax
import jax.numpy as jnp
import numpy as np
from jax import lax
from jax.experimental import pallas as pl
from jax.experimental.pallas import tpu as pltpu
from jax.sharding import PartitionSpec as P

EPS = 1e-6
MESH = pl.DeviceIdType.MESH
F32 = jnp.float32
BF16 = jnp.bfloat16

L = 2
B = 128
D = 128
S = 512
NX = 4
NY = 4
E = 2048
G = 16
NG = B // G


KINDS = {k: n for n, k in enumerate(("s", "h", "q", "kv", "kvx", "u", "ux", "f", "o", "y"))}
ORDER = ("XA0 XA0 IN*0 SQA0 SQB0 JN*0 XA0 RKVA0 XA0 RUA0 XB0 XB0 QA0 QKA0 QKA0 RKVB0 RUB0 SMA0 PVA0 KVA0 SOA0 RUB0 QB0 QKB0 QKB0 "
         "FA0 SMB0 PVB0 KVB0 SOB0 MLPA0 OUTA0 XA1 FB0 XA1 XA1 MLPB0 OUTB0 XA1 HA0 XB1 LVA0 XB1 XB1 LVB0 XB1 HB0 INA1 SQA1 JNA1 "
         "RKVA1 RUA1 INB1 SQB1 RUA1 JNB1 QA1 QKA1 QKA1 RKVB1 RUB1 SMA1 PVA1 KVA1 SOA1 QB1 QKB1 QKB1 SMB1 PVB1 KVB1 SOB1 FA1 "
         "MLPA1 FB1 OUTA1 MLPB1 OUTB1 HA1 HB1").split()


def _dot(a, b):
    return jnp.dot(a, b, preferred_element_type=F32)


def _dot_t(a, b):
    return lax.dot_general(a, b, (((1,), (1,)), ((), ())), preferred_element_type=F32)


def _kernel(nch, h_in, g_in, wq_in, wk_in, wv_in, win_in, wo_in, wout_in, kc_in, vc_in, lens_in, inv_in,
            h_out, k_out, v_out,
            kbuf, vbuf, wqkv, win, wo, wout, gg, lrow, inv, cosb, sinb, lenb,
            hg, ssb, qf, qb, qr, pf, pb, rq, sf, sb, xr, uf, ub, ur, usf, usb, ux, fb, og, zf, zb, zr,
            xbuf, qv, obuf, sbuf, pbuf, mbuf, dbuf,
            sem_in, sem_w, sem_k, sem_v, g_sem, send_sem, recv_sem):
    R = B // nch
    xi = lax.axis_index("x")
    yi = lax.axis_index("yz")
    c = lax.rem(xi, 2)
    xc = lax.div(xi, 2)
    partner = xi + 1 - 2 * c
    across = lax.rem(xi + 2, NX)
    open_sends = {}

    def exchange(kind, l, ch, copies, region, first=True):
        ss, rs = send_sem.at[KINDS[kind], ch], recv_sem.at[KINDS[kind], ch]
        if first:
            drain(kind, ch)
        for src, dst, dev in copies:
            pltpu.make_async_remote_copy(src_ref=src, dst_ref=dst, send_sem=ss, recv_sem=rs,
                                         device_id={"x": xi, "yz": yi, **dev}, device_id_type=MESH).start()
        open_sends[kind, ch] = region

    def drain(kind, ch):
        region = open_sends.pop((kind, ch), None)
        if region is not None:
            pltpu.make_async_copy(region, region, send_sem.at[KINDS[kind], ch]).wait()

    def arrived(kind, ch):
        region = open_sends[kind, ch]
        with jax.named_scope(f"w_{kind}_{ch}"):
            pltpu.make_async_copy(region, region, recv_sem.at[KINDS[kind], ch]).wait()

    def load(src, dst, sem):
        cp = pltpu.make_async_copy(src, dst, sem)
        cp.start()
        return cp

    in_h = load(h_in, hg.at[0, yi], sem_in.at[0])
    in_g = load(g_in, gg.at[yi], sem_in.at[1])
    in_l = load(lens_in, lrow, sem_in.at[2])
    in_i = load(inv_in, inv, sem_in.at[3])

    def load_first(l):
        for n, w in enumerate((wq_in, wk_in, wv_in)):
            load(w.at[l], wqkv.at[l, n], sem_w.at[0])
        load(win_in.at[l], win.at[l], sem_w.at[1])

    def load_second(l):
        load(wo_in.at[l], wo.at[l], sem_w.at[2])
        load(wout_in.at[l], wout.at[l], sem_w.at[3])

    def need_w(l, n):
        ref = (wqkv, win, wo, wout)[n].at[l]
        pltpu.make_async_copy(ref, ref, sem_w.at[n]).wait()

    gpc = NG // nch

    def load_cache(src, buf, sem, l, ch):
        for grp in range(ch * gpc, (ch + 1) * gpc):
            seqs = pl.ds(grp * G, G)
            load(src.at[l, seqs], buf.at[seqs], sem.at[ch])

    def need_cache(buf, sem, ch):
        ref = buf.at[pl.ds(ch * R, R)]
        pltpu.make_async_copy(ref, ref, sem.at[ch]).wait()

    load_cache(kc_in, kbuf, sem_k, 0, 0)
    load_first(0)

    barrier = pltpu.get_barrier_semaphore()
    for dx in range(NX):
        for dy in range(NY):
            if dx or dy:
                pl.semaphore_signal(barrier, inc=1, device_id={"yz": lax.rem(yi + dy, NY), "x": lax.rem(xi + dx, NX)},
                                    device_id_type=MESH)

    eye = (lax.broadcasted_iota(jnp.int32, (R, B), 0) == lax.broadcasted_iota(jnp.int32, (R, B), 1))

    def stats(l, ch, hb):
        col = jnp.sum(hb * hb, axis=1, keepdims=True)
        ssb[l, ch, 0] = jnp.sum(jnp.where(eye, col, 0.0), axis=0, keepdims=True)

    def send_h(l, ch):
        rows = pl.ds(ch * R, R)
        exchange("s", l, ch,
                 [(ssb.at[l, ch, 0], ssb.at[l, ch, dx * NY + dy],
                   {"x": lax.rem(xi + dx, NX), "yz": lax.rem(yi + dy, NY)})
                  for dx in (2, 1, 3, 0) for dy in (3, 1, 2, 0) if dx or dy],
                 ssb.at[l, ch, pl.ds(1, NX * NY - 1)])
        exchange("h", l, ch,
                 [(hg.at[l, yi, rows], hg.at[l, yi, rows], {"yz": lax.rem(yi + d, NY)}) for d in (3, 1, 2)],
                 hg.at[l, pl.ds(0, NY - 1), rows])

    in_h.wait()
    in_g.wait()
    for ch in range(nch):
        stats(0, ch, hg[0, yi, pl.ds(ch * R, R), :].astype(F32))
    with jax.named_scope('barrier_wait'):
        pl.semaphore_wait(barrier, NX * NY - 1)
    for ch in range(nch):
        send_h(0, ch)
    for d in (1, 2, 3):
        pltpu.make_async_remote_copy(src_ref=gg.at[yi], dst_ref=gg.at[yi], send_sem=g_sem.at[0], recv_sem=g_sem.at[1],
                                     device_id={"x": xi, "yz": lax.rem(yi + d, NY)}, device_id_type=MESH).start()

    for ch in range(1, nch):
        load_cache(kc_in, kbuf, sem_k, 0, ch)
    for ch in range(nch):
        load_cache(vc_in, vbuf, sem_v, 0, ch)
    load_second(0)

    in_l.wait()
    in_i.wait()
    eye_b = (lax.broadcasted_iota(jnp.int32, (B, B), 0) == lax.broadcasted_iota(jnp.int32, (B, B), 1))
    lcol = jnp.sum(jnp.where(eye_b, lrow[...].astype(F32), 0.0), axis=1, keepdims=True)
    lenb[...] = jnp.broadcast_to(lcol, (B, D))
    ang = lcol * inv[...]
    cosb[...] = jnp.cos(ang)
    half = lax.broadcasted_iota(jnp.int32, (B, D), 1) < D // 2
    sn = jnp.sin(ang)
    sinb[...] = jnp.where(half, -sn, sn)

    def stage_in(l, chunks):
        span = pl.ds(chunks[0] * R, R * len(chunks))
        scales = []
        for ch in chunks:
            arrived("h", ch)
            arrived("s", ch)
            row = ssb[l, ch, 0]
            for slot in range(1, NX * NY):
                row = row + ssb[l, ch, slot]
            col = jnp.sum(jnp.where(eye, row, 0.0), axis=1, keepdims=True)
            scales.append(lax.rsqrt(col / E + EPS))
        r = jnp.concatenate(scales, axis=0)
        if 0 in chunks:
            if l == 0:
                ref = gg.at[pl.ds(0, NY - 1)]
                pltpu.make_async_copy(ref, ref, g_sem.at[1]).wait()
                pltpu.make_async_copy(ref, ref, g_sem.at[0]).wait()
            need_w(l, 0)
            need_w(l, 1)
        xs = []
        for j in range(NY):
            gj = gg[j, pl.ds(l, 1), :].astype(F32)
            xs.append((hg[l, j, span, :].astype(F32) * r * gj).astype(BF16))
        x = jnp.concatenate(xs, axis=1)
        xbuf[span, :] = x
        for n in range(2):
            acc = _dot(x, wqkv[l, 0, :, pl.ds(n * 256, 256)])
            for m in range(2):
                a = acc[:, m * D:(m + 1) * D]
                qf[2 * n + m, span, :] = a
                qb[l, 2 * n + m, span, :] = a.astype(BF16)

    def send_q(l, ch):
        rows = pl.ds(ch * R, R)
        tos = [lax.rem(xi + d, NX) for d in range(NX)]
        exchange("q", l, ch, [(qb.at[l, tos[d], rows], qr.at[l, d - 1, rows], {"x": tos[d]}) for d in (2, 1, 3)],
                 qr.at[l, :, rows])

    def stage_in_rest(l, chunks):
        span = pl.ds(chunks[0] * R, R * len(chunks))
        x = xbuf[span, :]
        for t in range(2):
            for n in range(2):
                acc = _dot(x, wqkv[l, t + 1, :, pl.ds(n * 256, 256)])
                for cc in range(2):
                    a = acc[:, cc * D:(cc + 1) * D]
                    pf[cc, t, n, span, :] = a
                    pb[l, cc, t, n, span, :] = a.astype(BF16)
        for ch in chunks:
            rows = pl.ds(ch * R, R)
            exchange("kv", l, ch, [(pb.at[l, 1 - c, :, :, rows], rq.at[l, :, :, rows], {"x": partner})],
                     rq.at[l, :, :, rows])
        for n in range(8):
            acc = _dot(x, win[l, :, pl.ds(n * 256, 256)])
            cols = pl.ds((n % 4) * 256, 256)
            uf[n // 4, span, cols] = acc
            ub[l, n // 4, span, cols] = acc.astype(BF16)
        for ch in chunks:
            rows = pl.ds(ch * R, R)
            exchange("u", l, ch, [(ub.at[l, 1 - c, rows], ur.at[l, rows], {"x": partner})], ur.at[l, rows])
        if nch - 1 in chunks and l + 1 < L:
            load_first(l + 1)

    def reduce_kv(l, ch):
        rows = pl.ds(ch * R, R)
        arrived("kv", ch)
        for t in range(2):
            for n in range(2):
                s = pf[c, t, n, rows, :] + rq[l, t, n, rows, :].astype(F32)
                sf[n, t, rows, :] = s
                sb[l, n, t, rows, :] = s.astype(BF16)
        exchange("kvx", l, ch, [(sb.at[l, 1 - xc, :, rows], xr.at[l, :, rows], {"x": across})], xr.at[l, :, rows])

    u_done = {}

    def reduce_u(l, ch):
        pieces = ORDER.count(f"RU{'AB'[ch]}{l}")
        piece = u_done.get((l, ch), 0)
        u_done[l, ch] = piece + 1
        if piece == 0:
            arrived("u", ch)
        rows = pl.ds(ch * R + piece * (R // pieces), R // pieces)
        us = uf[c, rows, :] + ur[l, rows, :].astype(F32)
        usf[rows, :] = us
        usb[l, rows, :] = us.astype(BF16)
        exchange("ux", l, ch, [(usb.at[l, rows], ux.at[l, rows], {"x": across})], ux.at[l, pl.ds(ch * R, R)],
                 first=piece == 0)

    def rope(t, rows):
        tf = t.astype(F32)
        return (tf * cosb[rows, :] + pltpu.roll(tf, D // 2, 1) * sinb[rows, :]).astype(BF16)

    def stage_q(l, ch):
        rows = pl.ds(ch * R, R)
        arrived("q", ch)
        q = qf[xi, rows, :]
        for d in range(NX - 1):
            q = q + qr[l, d, rows, :].astype(F32)
        qv[rows, :] = rope(q.astype(BF16), rows)

    rowid = lax.broadcasted_iota(jnp.int32, (G, D), 0)
    pos = lax.broadcasted_iota(jnp.int32, (R, S), 1).astype(F32)
    scale = D ** -0.5

    ready, flipped, scored = set(), {}, {}

    def need_keys(l, ch):
        if (l, ch) not in ready:
            ready.add((l, ch))
            need_cache(kbuf, sem_k, ch)

    def transpose(l, ch):
        need_keys(l, ch)
        g = flipped.get((l, ch), 0)
        flipped[l, ch] = g + 1
        for b in range(ch * R + g * G, ch * R + (g + 1) * G):
            for j in range(S // D):
                kbuf[b, pl.ds(j * D, D), :] = kbuf[b, pl.ds(j * D, D), :].T

    def scores(l, ch):
        need_keys(l, ch)
        first = scored.get((l, ch), 0)
        scored[l, ch] = first + gpc // 2
        for g in range(first, first + gpc // 2):
            base = ch * R + g * G
            rows = pl.ds(base, G)
            q = qv[rows, :].astype(F32)
            s = jnp.zeros((G, S), F32)
            for i in range(0, G, 2):
                lhs = jnp.concatenate([jnp.where(rowid == i, q, 0.0), jnp.where(rowid == i + 1, q, 0.0)],
                                      axis=1).astype(BF16)
                if g < flipped.get((l, ch), 0):
                    keys = [jnp.concatenate([kbuf[base + i + e, pl.ds(j * D, D), :] for j in range(S // D)], axis=1)
                            for e in range(2)]
                    s = s + _dot(lhs, jnp.concatenate(keys, axis=0))
                else:
                    s = s + _dot_t(lhs, jnp.concatenate([kbuf[base + i], kbuf[base + i + 1]], axis=1))
            sbuf[rows, :] = s
        if scored[l, ch] == gpc and l + 1 < L:
            load_cache(kc_in, kbuf, sem_k, l + 1, ch)

    def softmax(l, ch):
        rows = pl.ds(ch * R, R)
        s = jnp.where(pos < lenb[rows, :][:, :1], sbuf[rows, :] * scale, -jnp.inf)
        m = jnp.max(s, axis=1, keepdims=True)
        p = jnp.exp(s - m)
        pbuf[rows, :] = p.astype(BF16)
        mbuf[rows, :] = jnp.broadcast_to(m, (R, D))
        dbuf[rows, :] = jnp.broadcast_to(jnp.sum(p, axis=1, keepdims=True), (R, D))

    def values(l, ch):
        need_cache(vbuf, sem_v, ch)
        for g in range(gpc):
            base = ch * R + g * G
            rows = pl.ds(base, G)
            p = pbuf[rows, :]
            o = jnp.zeros((G, D), F32)
            for i in range(0, G, 2):
                t = _dot(p, jnp.concatenate([vbuf[base + i], vbuf[base + i + 1]], axis=1))
                o = o + jnp.where(rowid == i, t[:, :D], jnp.where(rowid == i + 1, t[:, D:], 0.0))
            obuf[rows, :] = o

    def load_values(l, ch):
        load_cache(vc_in, vbuf, sem_v, l + 1, ch)

    def stage_kv(l, ch):
        rows = pl.ds(ch * R, R)
        arrived("kvx", ch)
        k = rope((sf[xc, 0, rows, :] + xr[l, 0, rows, :].astype(F32)).astype(BF16), rows)
        v = (sf[xc, 1, rows, :] + xr[l, 1, rows, :].astype(F32)).astype(BF16)
        k_out[l, rows, :] = k
        v_out[l, rows, :] = v
        s_new = jnp.sum(qv[rows, :].astype(F32) * k.astype(F32), axis=1, keepdims=True) * scale
        m_c = mbuf[rows, :]
        m = jnp.maximum(m_c, s_new)
        a = jnp.exp(m_c - m)
        p_new = jnp.exp(s_new - m)
        o = (a * obuf[rows, :] + p_new * v.astype(F32)) / (a * dbuf[rows, :] + p_new)
        og[l, xi, rows, :] = o.astype(BF16)

    def send_o(l, ch):
        rows = pl.ds(ch * R, R)
        exchange("o", l, ch, [(og.at[l, xi, rows], og.at[l, xi, rows], {"x": lax.rem(xi + d, NX)}) for d in (2, 1, 3)],
                 og.at[l, pl.ds(0, NX - 1), rows])

    def stage_f(l, ch):
        rows = pl.ds(ch * R, R)
        arrived("ux", ch)
        u = (usf[rows, :] + ux[l, rows, :].astype(F32)).astype(BF16)
        fb[l, c, rows, :] = jax.nn.gelu(u.astype(F32), approximate=True).astype(BF16)
        exchange("f", l, ch, [(fb.at[l, c, rows], fb.at[l, c, rows], {"x": partner})], fb.at[l, 0, rows])

    def stage_mlp(l, ch):
        rows = pl.ds(ch * R, R)
        arrived("f", ch)
        if ch == 0:
            need_w(l, 3)
        f = jnp.concatenate([fb[l, 0, rows, :], fb[l, 1, rows, :]], axis=1)
        for n in range(2):
            acc = _dot(f, wout[l, :, pl.ds(n * 256, 256)])
            zf[2 * n, rows, :] = acc[:, :D]
            zf[2 * n + 1, rows, :] = acc[:, D:]

    def stage_out(l, ch):
        rows = pl.ds(ch * R, R)
        arrived("o", ch)
        if ch == 0:
            need_w(l, 2)
        o = jnp.concatenate([og[l, j, rows, :] for j in range(NX)], axis=1)
        for n in range(2):
            acc = _dot(o, wo[l, :, pl.ds(n * 256, 256)])
            for m in range(2):
                a = acc[:, m * D:(m + 1) * D] + zf[2 * n + m, rows, :]
                zf[2 * n + m, rows, :] = a
                zb[l, 2 * n + m, rows, :] = a.astype(BF16)
        tos = [lax.rem(yi + d, NY) for d in range(NY)]
        exchange("y", l, ch, [(zb.at[l, tos[d], rows], zr.at[l, d - 1, rows], {"yz": tos[d]}) for d in (3, 1, 2)],
                 zr.at[l, :, rows])
        if ch == nch - 1 and l + 1 < L:
            load_second(l + 1)

    def stage_h(l, ch):
        rows = pl.ds(ch * R, R)
        arrived("y", ch)
        y = zf[yi, rows, :]
        for d in range(NY - 1):
            y = y + zr[l, d, rows, :].astype(F32)
        hn = (hg[l, yi, rows, :].astype(F32) + y.astype(BF16).astype(F32)).astype(BF16)
        if l + 1 < L:
            hg[l + 1, yi, rows, :] = hn
            stats(l + 1, ch, hn.astype(F32))
            send_h(l + 1, ch)
        else:
            h_out[rows, :] = hn

    stages = dict(IN=stage_in, SQ=send_q, JN=stage_in_rest, RKV=reduce_kv, RU=reduce_u, Q=stage_q, QK=scores, X=transpose, KV=stage_kv, SM=softmax, PV=values, LV=load_values,
                  SO=send_o, F=stage_f, MLP=stage_mlp, OUT=stage_out, H=stage_h)
    for step in ORDER:
        with jax.named_scope(step):
            chunks = range(nch) if step[-2] == "*" else ("AB".index(step[-2]),)
            stages[step[:-2]](int(step[-1]), chunks if step[:2] in ("IN", "JN") else chunks[0])
    for kind, ch in list(open_sends):
        drain(kind, ch)


def _tail(h_in, k_in, v_in, h_out, k_out, v_out, sem):
    cps = [pltpu.make_async_copy(a, o, sem.at[n])
           for n, (a, o) in enumerate(((k_in, k_out), (v_in, v_out), (h_in, h_out)))]
    for cp in cps:
        cp.start()
    for cp in cps:
        cp.wait()


def solution(mesh):
    nch = 2
    act = P(None, ('x', 'yz'))
    w_first = P(None, 'x', 'yz')
    w_second = P(None, 'yz', 'x')
    cache = P(None, None, ('yz', 'x'), None, None)
    new = P(None, None, ('yz', 'x'), None)
    inv_half = 10000.0 ** (-np.arange(D // 2, dtype=np.float64) / (D // 2))
    inv_np = np.concatenate([inv_half, inv_half]).astype(np.float32)[None]

    def body(h, g, wq, wk, wv, w_in, wo, w_out, kc, vc, lens):
        any_spec = pl.BlockSpec(memory_space=pl.ANY)
        vm_spec = pl.BlockSpec(memory_space=pltpu.VMEM)
        shapes = ((B, D), (L, B, D), (L, B, D))
        vm = pltpu.VMEM
        dma = pltpu.SemaphoreType.DMA
        scratch = [
            vm((B, S, D), BF16), vm((B, S, D), BF16),
            vm((L, 3, 512, 512), BF16), vm((L, 512, 2048), BF16), vm((L, 512, 512), BF16), vm((L, 2048, 512), BF16),
            vm((NY, L, D), BF16), vm((1, B), jnp.int32), vm((1, D), F32),
            vm((B, D), F32), vm((B, D), F32), vm((B, D), F32),
            vm((L, NY, B, D), BF16),
            vm((L, nch, NX * NY, 1, B), F32),
            vm((NX, B, D), F32),
            vm((L, NX, B, D), BF16),
            vm((L, NX - 1, B, D), BF16),
            vm((2, 2, 2, B, D), F32),
            vm((L, 2, 2, 2, B, D), BF16),
            vm((L, 2, 2, B, D), BF16),
            vm((2, 2, B, D), F32),
            vm((L, 2, 2, B, D), BF16),
            vm((L, 2, B, D), BF16),
            vm((2, B, 1024), F32),
            vm((L, 2, B, 1024), BF16),
            vm((L, B, 1024), BF16),
            vm((B, 1024), F32),
            vm((L, B, 1024), BF16),
            vm((L, B, 1024), BF16),
            vm((L, 2, B, 1024), BF16),
            vm((L, NX, B, D), BF16),
            vm((NY, B, D), F32),
            vm((L, NY, B, D), BF16),
            vm((L, NY - 1, B, D), BF16),
            vm((B, NY * D), BF16), vm((B, D), BF16), vm((B, D), F32),
            vm((B, S), F32), vm((B, S), BF16), vm((B, D), F32), vm((B, D), F32),
            dma((4,)), dma((4,)), dma((nch,)), dma((nch,)), dma((2,)),
            dma((len(KINDS), nch)), dma((len(KINDS), nch)),
        ]
        h_new, k_new, v_new = pl.pallas_call(
            functools.partial(_kernel, nch),
            out_shape=tuple(vm(n, BF16) for n in shapes),
            in_specs=[any_spec] * 12,
            out_specs=(vm_spec,) * 3,
            scratch_shapes=scratch,
            compiler_params=pltpu.CompilerParams(collective_id=0, has_side_effects=True,
                                                 vmem_limit_bytes=66_000_000),
            name="decode_step",
        )(h, g, wq, wk, wv, w_in, wo, w_out, kc.reshape(L, B, S, D), vc.reshape(L, B, S, D),
          lens.reshape(1, B), jnp.asarray(inv_np))
        h_new, k_new, v_new = pl.pallas_call(
            _tail,
            out_shape=tuple(jax.ShapeDtypeStruct(n, BF16) for n in shapes),
            in_specs=[vm_spec] * 3,
            out_specs=(any_spec,) * 3,
            scratch_shapes=[dma((3,))],
            name="results",
        )(*(pltpu.with_memory_space_constraint(a, pltpu.VMEM) for a in (h_new, k_new, v_new)))
        return h_new, k_new.reshape(L, B, 1, D), v_new.reshape(L, B, 1, D)

    return jax.shard_map(
        body, mesh=mesh,
        in_specs=(act, act, w_first, w_first, w_first, w_first, w_second, w_second, cache, cache, P(None)),
        out_specs=(act, new, new), check_vma=False)
```

```python
import functools

import jax
import jax.numpy as jnp
import numpy as np
from jax import lax
from jax.experimental import pallas as pl
from jax.experimental.pallas import tpu as pltpu
from jax.sharding import PartitionSpec as P

EPS = 1e-6
MESH = pl.DeviceIdType.MESH
F32 = jnp.float32
BF16 = jnp.bfloat16

L = 2
B = 128
D = 128
S = 512
NX = 4
NY = 4
E = 2048
G = 16
NG = B // G


KINDS = {k: n for n, k in enumerate(("s", "h", "q", "kv", "kvx", "u", "ux", "f", "o", "y"))}
ORDER = ("IN*0 SQA0 SQB0 JN*0 XA0 RKVA0 XA0 RUA0 XA0 XA0 QA0 QKA0 QKA0 RKVB0 RUB0 SMA0 PVA0 KVA0 SOA0 RUB0 QB0 QKB0 QKB0 "
         "FA0 SMB0 PVB0 KVB0 SOB0 MLPA0 OUTA0 XA1 FB0 XA1 XA1 MLPB0 OUTB0 XA1 HA0 XB1 LVA0 XB1 XB1 LVB0 XB1 HB0 INA1 SQA1 JNA1 "
         "RKVA1 RUA1 INB1 SQB1 RUA1 JNB1 QA1 QKA1 QKA1 RKVB1 RUB1 SMA1 PVA1 KVA1 SOA1 QB1 QKB1 QKB1 SMB1 PVB1 KVB1 SOB1 FA1 "
         "MLPA1 FB1 OUTA1 MLPB1 OUTB1 HA1 HB1").split()


def _dot(a, b):
    return jnp.dot(a, b, preferred_element_type=F32)


def _dot_t(a, b):
    return lax.dot_general(a, b, (((1,), (1,)), ((), ())), preferred_element_type=F32)


def _kernel(nch, h_in, g_in, wq_in, wk_in, wv_in, win_in, wo_in, wout_in, kc_in, vc_in, lens_in, inv_in,
            h_out, k_out, v_out,
            kbuf, vbuf, wqkv, win, wo, wout, gg, lrow, inv, cosb, sinb, lenb,
            hg, ssb, qf, qb, qr, pf, pb, rq, sf, sb, xr, uf, ub, ur, usf, usb, ux, fb, og, zf, zb, zr,
            xbuf, qv, obuf, sbuf, pbuf, mbuf, dbuf,
            sem_in, sem_w, sem_k, sem_v, g_sem, send_sem, recv_sem):
    R = B // nch
    xi = lax.axis_index("x")
    yi = lax.axis_index("yz")
    c = lax.rem(xi, 2)
    xc = lax.div(xi, 2)
    partner = xi + 1 - 2 * c
    across = lax.rem(xi + 2, NX)
    open_sends = {}

    def exchange(kind, l, ch, copies, region, first=True):
        ss, rs = send_sem.at[KINDS[kind], ch], recv_sem.at[KINDS[kind], ch]
        if first:
            drain(kind, ch)
        for src, dst, dev in copies:
            pltpu.make_async_remote_copy(src_ref=src, dst_ref=dst, send_sem=ss, recv_sem=rs,
                                         device_id={"x": xi, "yz": yi, **dev}, device_id_type=MESH).start()
        open_sends[kind, ch] = region

    def drain(kind, ch):
        region = open_sends.pop((kind, ch), None)
        if region is not None:
            pltpu.make_async_copy(region, region, send_sem.at[KINDS[kind], ch]).wait()

    def arrived(kind, ch):
        region = open_sends[kind, ch]
        with jax.named_scope(f"w_{kind}_{ch}"):
            pltpu.make_async_copy(region, region, recv_sem.at[KINDS[kind], ch]).wait()

    def load(src, dst, sem):
        cp = pltpu.make_async_copy(src, dst, sem)
        cp.start()
        return cp

    in_h = load(h_in, hg.at[0, yi], sem_in.at[0])
    in_g = load(g_in, gg.at[yi], sem_in.at[1])
    in_l = load(lens_in, lrow, sem_in.at[2])
    in_i = load(inv_in, inv, sem_in.at[3])

    def load_first(l):
        for n, w in enumerate((wq_in, wk_in, wv_in)):
            load(w.at[l], wqkv.at[l, n], sem_w.at[0])
        load(win_in.at[l], win.at[l], sem_w.at[1])

    def load_second(l):
        load(wo_in.at[l], wo.at[l], sem_w.at[2])
        load(wout_in.at[l], wout.at[l], sem_w.at[3])

    def need_w(l, n):
        ref = (wqkv, win, wo, wout)[n].at[l]
        pltpu.make_async_copy(ref, ref, sem_w.at[n]).wait()

    load_first(0)

    barrier = pltpu.get_barrier_semaphore()
    for dx in range(NX):
        for dy in range(NY):
            if dx or dy:
                pl.semaphore_signal(barrier, inc=1, device_id={"yz": lax.rem(yi + dy, NY), "x": lax.rem(xi + dx, NX)},
                                    device_id_type=MESH)

    eye = (lax.broadcasted_iota(jnp.int32, (R, B), 0) == lax.broadcasted_iota(jnp.int32, (R, B), 1))

    def stats(l, ch, hb):
        col = jnp.sum(hb * hb, axis=1, keepdims=True)
        ssb[l, ch, 0] = jnp.sum(jnp.where(eye, col, 0.0), axis=0, keepdims=True)

    def send_h(l, ch):
        rows = pl.ds(ch * R, R)
        exchange("s", l, ch,
                 [(ssb.at[l, ch, 0], ssb.at[l, ch, dx * NY + dy],
                   {"x": lax.rem(xi + dx, NX), "yz": lax.rem(yi + dy, NY)})
                  for dx in (2, 1, 3, 0) for dy in (3, 1, 2, 0) if dx or dy],
                 ssb.at[l, ch, pl.ds(1, NX * NY - 1)])
        exchange("h", l, ch,
                 [(hg.at[l, yi, rows], hg.at[l, yi, rows], {"yz": lax.rem(yi + d, NY)}) for d in (3, 1, 2)],
                 hg.at[l, pl.ds(0, NY - 1), rows])

    in_h.wait()
    in_g.wait()
    for ch in range(nch):
        stats(0, ch, hg[0, yi, pl.ds(ch * R, R), :].astype(F32))
    with jax.named_scope('barrier_wait'):
        pl.semaphore_wait(barrier, NX * NY - 1)
    for ch in range(nch):
        send_h(0, ch)
    for d in (1, 2, 3):
        pltpu.make_async_remote_copy(src_ref=gg.at[yi], dst_ref=gg.at[yi], send_sem=g_sem.at[0], recv_sem=g_sem.at[1],
                                     device_id={"x": xi, "yz": lax.rem(yi + d, NY)}, device_id_type=MESH).start()

    def load_cache(src, buf, sem, l, ch):
        for grp in range(ch * gpc, (ch + 1) * gpc):
            seqs = pl.ds(grp * G, G)
            load(src.at[l, seqs], buf.at[seqs], sem.at[ch])

    def need_cache(buf, sem, ch):
        ref = buf.at[pl.ds(ch * R, R)]
        pltpu.make_async_copy(ref, ref, sem.at[ch]).wait()

    gpc = NG // nch
    for ch in range(nch):
        load_cache(kc_in, kbuf, sem_k, 0, ch)
        load_cache(vc_in, vbuf, sem_v, 0, ch)
    load_second(0)

    in_l.wait()
    in_i.wait()
    eye_b = (lax.broadcasted_iota(jnp.int32, (B, B), 0) == lax.broadcasted_iota(jnp.int32, (B, B), 1))
    lcol = jnp.sum(jnp.where(eye_b, lrow[...].astype(F32), 0.0), axis=1, keepdims=True)
    lenb[...] = jnp.broadcast_to(lcol, (B, D))
    ang = lcol * inv[...]
    cosb[...] = jnp.cos(ang)
    half = lax.broadcasted_iota(jnp.int32, (B, D), 1) < D // 2
    sn = jnp.sin(ang)
    sinb[...] = jnp.where(half, -sn, sn)

    def stage_in(l, chunks):
        span = pl.ds(chunks[0] * R, R * len(chunks))
        scales = []
        for ch in chunks:
            arrived("h", ch)
            arrived("s", ch)
            row = ssb[l, ch, 0]
            for slot in range(1, NX * NY):
                row = row + ssb[l, ch, slot]
            col = jnp.sum(jnp.where(eye, row, 0.0), axis=1, keepdims=True)
            scales.append(lax.rsqrt(col / E + EPS))
        r = jnp.concatenate(scales, axis=0)
        if 0 in chunks:
            if l == 0:
                ref = gg.at[pl.ds(0, NY - 1)]
                pltpu.make_async_copy(ref, ref, g_sem.at[1]).wait()
                pltpu.make_async_copy(ref, ref, g_sem.at[0]).wait()
            need_w(l, 0)
            need_w(l, 1)
        xs = []
        for j in range(NY):
            gj = gg[j, pl.ds(l, 1), :].astype(F32)
            xs.append((hg[l, j, span, :].astype(F32) * r * gj).astype(BF16))
        x = jnp.concatenate(xs, axis=1)
        xbuf[span, :] = x
        for n in range(2):
            acc = _dot(x, wqkv[l, 0, :, pl.ds(n * 256, 256)])
            for m in range(2):
                a = acc[:, m * D:(m + 1) * D]
                qf[2 * n + m, span, :] = a
                qb[l, 2 * n + m, span, :] = a.astype(BF16)

    def send_q(l, ch):
        rows = pl.ds(ch * R, R)
        tos = [lax.rem(xi + d, NX) for d in range(NX)]
        exchange("q", l, ch, [(qb.at[l, tos[d], rows], qr.at[l, d - 1, rows], {"x": tos[d]}) for d in (2, 1, 3)],
                 qr.at[l, :, rows])

    def stage_in_rest(l, chunks):
        span = pl.ds(chunks[0] * R, R * len(chunks))
        x = xbuf[span, :]
        for t in range(2):
            for n in range(2):
                acc = _dot(x, wqkv[l, t + 1, :, pl.ds(n * 256, 256)])
                for cc in range(2):
                    a = acc[:, cc * D:(cc + 1) * D]
                    pf[cc, t, n, span, :] = a
                    pb[l, cc, t, n, span, :] = a.astype(BF16)
        for ch in chunks:
            rows = pl.ds(ch * R, R)
            exchange("kv", l, ch, [(pb.at[l, 1 - c, :, :, rows], rq.at[l, :, :, rows], {"x": partner})],
                     rq.at[l, :, :, rows])
        for n in range(4):
            acc = _dot(x, win[l, :, pl.ds(pl.multiple_of((1 - c) * 1024 + n * 256, 256), 256)])
            ub[l, span, pl.ds(n * 256, 256)] = acc.astype(BF16)
        for ch in chunks:
            rows = pl.ds(ch * R, R)
            exchange("u", l, ch, [(ub.at[l, rows], ur.at[l, rows], {"x": partner})], ur.at[l, rows])
        for n in range(4):
            uf[span, pl.ds(n * 256, 256)] = _dot(x, win[l, :, pl.ds(pl.multiple_of(c * 1024 + n * 256, 256), 256)])
        if nch - 1 in chunks and l + 1 < L:
            load_first(l + 1)

    def reduce_kv(l, ch):
        rows = pl.ds(ch * R, R)
        arrived("kv", ch)
        for t in range(2):
            for n in range(2):
                s = pf[c, t, n, rows, :] + rq[l, t, n, rows, :].astype(F32)
                sf[n, t, rows, :] = s
                sb[l, n, t, rows, :] = s.astype(BF16)
        exchange("kvx", l, ch, [(sb.at[l, 1 - xc, :, rows], xr.at[l, :, rows], {"x": across})], xr.at[l, :, rows])

    u_done = {}

    def reduce_u(l, ch):
        pieces = ORDER.count(f"RU{'AB'[ch]}{l}")
        piece = u_done.get((l, ch), 0)
        u_done[l, ch] = piece + 1
        if piece == 0:
            arrived("u", ch)
        rows = pl.ds(ch * R + piece * (R // pieces), R // pieces)
        us = uf[rows, :] + ur[l, rows, :].astype(F32)
        usf[rows, :] = us
        usb[l, rows, :] = us.astype(BF16)
        exchange("ux", l, ch, [(usb.at[l, rows], ux.at[l, rows], {"x": across})], ux.at[l, pl.ds(ch * R, R)],
                 first=piece == 0)

    def rope(t, rows):
        tf = t.astype(F32)
        return (tf * cosb[rows, :] + pltpu.roll(tf, D // 2, 1) * sinb[rows, :]).astype(BF16)

    def stage_q(l, ch):
        rows = pl.ds(ch * R, R)
        arrived("q", ch)
        q = qf[xi, rows, :]
        for d in range(NX - 1):
            q = q + qr[l, d, rows, :].astype(F32)
        qv[rows, :] = rope(q.astype(BF16), rows)

    rowid = lax.broadcasted_iota(jnp.int32, (G, D), 0)
    pos = lax.broadcasted_iota(jnp.int32, (R, S), 1).astype(F32)
    scale = D ** -0.5

    ready, flipped, scored = set(), {}, {}

    def need_keys(l, ch):
        if (l, ch) not in ready:
            ready.add((l, ch))
            need_cache(kbuf, sem_k, ch)

    def transpose(l, ch):
        need_keys(l, ch)
        g = flipped.get((l, ch), 0)
        flipped[l, ch] = g + 1
        for b in range(ch * R + g * G, ch * R + (g + 1) * G):
            for j in range(S // D):
                kbuf[b, pl.ds(j * D, D), :] = kbuf[b, pl.ds(j * D, D), :].T

    def scores(l, ch):
        need_keys(l, ch)
        first = scored.get((l, ch), 0)
        scored[l, ch] = first + gpc // 2
        for g in range(first, first + gpc // 2):
            base = ch * R + g * G
            rows = pl.ds(base, G)
            q = qv[rows, :].astype(F32)
            s = jnp.zeros((G, S), F32)
            for i in range(0, G, 2):
                lhs = jnp.concatenate([jnp.where(rowid == i, q, 0.0), jnp.where(rowid == i + 1, q, 0.0)],
                                      axis=1).astype(BF16)
                if g < flipped.get((l, ch), 0):
                    keys = [jnp.concatenate([kbuf[base + i + e, pl.ds(j * D, D), :] for j in range(S // D)], axis=1)
                            for e in range(2)]
                    s = s + _dot(lhs, jnp.concatenate(keys, axis=0))
                else:
                    s = s + _dot_t(lhs, jnp.concatenate([kbuf[base + i], kbuf[base + i + 1]], axis=1))
            sbuf[rows, :] = s
        if scored[l, ch] == gpc and l + 1 < L:
            load_cache(kc_in, kbuf, sem_k, l + 1, ch)

    def softmax(l, ch):
        rows = pl.ds(ch * R, R)
        s = jnp.where(pos < lenb[rows, :][:, :1], sbuf[rows, :] * scale, -jnp.inf)
        m = jnp.max(s, axis=1, keepdims=True)
        p = jnp.exp(s - m)
        pbuf[rows, :] = p.astype(BF16)
        mbuf[rows, :] = jnp.broadcast_to(m, (R, D))
        dbuf[rows, :] = jnp.broadcast_to(jnp.sum(p, axis=1, keepdims=True), (R, D))

    def values(l, ch):
        need_cache(vbuf, sem_v, ch)
        for g in range(gpc):
            base = ch * R + g * G
            rows = pl.ds(base, G)
            p = pbuf[rows, :]
            o = jnp.zeros((G, D), F32)
            for i in range(0, G, 2):
                t = _dot(p, jnp.concatenate([vbuf[base + i], vbuf[base + i + 1]], axis=1))
                o = o + jnp.where(rowid == i, t[:, :D], jnp.where(rowid == i + 1, t[:, D:], 0.0))
            obuf[rows, :] = o

    def load_values(l, ch):
        load_cache(vc_in, vbuf, sem_v, l + 1, ch)

    def stage_kv(l, ch):
        rows = pl.ds(ch * R, R)
        arrived("kvx", ch)
        k = rope((sf[xc, 0, rows, :] + xr[l, 0, rows, :].astype(F32)).astype(BF16), rows)
        v = (sf[xc, 1, rows, :] + xr[l, 1, rows, :].astype(F32)).astype(BF16)
        k_out[l, rows, :] = k
        v_out[l, rows, :] = v
        s_new = jnp.sum(qv[rows, :].astype(F32) * k.astype(F32), axis=1, keepdims=True) * scale
        m_c = mbuf[rows, :]
        m = jnp.maximum(m_c, s_new)
        a = jnp.exp(m_c - m)
        p_new = jnp.exp(s_new - m)
        o = (a * obuf[rows, :] + p_new * v.astype(F32)) / (a * dbuf[rows, :] + p_new)
        og[l, xi, rows, :] = o.astype(BF16)

    def send_o(l, ch):
        rows = pl.ds(ch * R, R)
        exchange("o", l, ch, [(og.at[l, xi, rows], og.at[l, xi, rows], {"x": lax.rem(xi + d, NX)}) for d in (2, 1, 3)],
                 og.at[l, pl.ds(0, NX - 1), rows])

    def stage_f(l, ch):
        rows = pl.ds(ch * R, R)
        arrived("ux", ch)
        u = (usf[rows, :] + ux[l, rows, :].astype(F32)).astype(BF16)
        fb[l, c, rows, :] = jax.nn.gelu(u.astype(F32), approximate=True).astype(BF16)
        exchange("f", l, ch, [(fb.at[l, c, rows], fb.at[l, c, rows], {"x": partner})], fb.at[l, 0, rows])

    def stage_mlp(l, ch):
        rows = pl.ds(ch * R, R)
        arrived("f", ch)
        if ch == 0:
            need_w(l, 3)
        f = jnp.concatenate([fb[l, 0, rows, :], fb[l, 1, rows, :]], axis=1)
        for n in range(2):
            acc = _dot(f, wout[l, :, pl.ds(n * 256, 256)])
            zf[2 * n, rows, :] = acc[:, :D]
            zf[2 * n + 1, rows, :] = acc[:, D:]

    def stage_out(l, ch):
        rows = pl.ds(ch * R, R)
        arrived("o", ch)
        if ch == 0:
            need_w(l, 2)
        o = jnp.concatenate([og[l, j, rows, :] for j in range(NX)], axis=1)
        for n in range(2):
            acc = _dot(o, wo[l, :, pl.ds(n * 256, 256)])
            for m in range(2):
                a = acc[:, m * D:(m + 1) * D] + zf[2 * n + m, rows, :]
                zf[2 * n + m, rows, :] = a
                zb[l, 2 * n + m, rows, :] = a.astype(BF16)
        tos = [lax.rem(yi + d, NY) for d in range(NY)]
        exchange("y", l, ch, [(zb.at[l, tos[d], rows], zr.at[l, d - 1, rows], {"yz": tos[d]}) for d in (3, 1, 2)],
                 zr.at[l, :, rows])
        if ch == nch - 1 and l + 1 < L:
            load_second(l + 1)

    def stage_h(l, ch):
        rows = pl.ds(ch * R, R)
        arrived("y", ch)
        y = zf[yi, rows, :]
        for d in range(NY - 1):
            y = y + zr[l, d, rows, :].astype(F32)
        hn = (hg[l, yi, rows, :].astype(F32) + y.astype(BF16).astype(F32)).astype(BF16)
        if l + 1 < L:
            hg[l + 1, yi, rows, :] = hn
            stats(l + 1, ch, hn.astype(F32))
            send_h(l + 1, ch)
        else:
            h_out[rows, :] = hn

    stages = dict(IN=stage_in, SQ=send_q, JN=stage_in_rest, RKV=reduce_kv, RU=reduce_u, Q=stage_q, QK=scores, X=transpose, KV=stage_kv, SM=softmax, PV=values, LV=load_values,
                  SO=send_o, F=stage_f, MLP=stage_mlp, OUT=stage_out, H=stage_h)
    for step in ORDER:
        with jax.named_scope(step):
            chunks = range(nch) if step[-2] == "*" else ("AB".index(step[-2]),)
            stages[step[:-2]](int(step[-1]), chunks if step[:2] in ("IN", "JN") else chunks[0])
    for kind, ch in list(open_sends):
        drain(kind, ch)


def _tail(h_in, k_in, v_in, h_out, k_out, v_out, sem):
    cps = [pltpu.make_async_copy(a, o, sem.at[n])
           for n, (a, o) in enumerate(((k_in, k_out), (v_in, v_out), (h_in, h_out)))]
    for cp in cps:
        cp.start()
    for cp in cps:
        cp.wait()


def solution(mesh):
    nch = 2
    act = P(None, ('x', 'yz'))
    w_first = P(None, 'x', 'yz')
    w_second = P(None, 'yz', 'x')
    cache = P(None, None, ('yz', 'x'), None, None)
    new = P(None, None, ('yz', 'x'), None)
    inv_half = 10000.0 ** (-np.arange(D // 2, dtype=np.float64) / (D // 2))
    inv_np = np.concatenate([inv_half, inv_half]).astype(np.float32)[None]

    def body(h, g, wq, wk, wv, w_in, wo, w_out, kc, vc, lens):
        any_spec = pl.BlockSpec(memory_space=pl.ANY)
        vm_spec = pl.BlockSpec(memory_space=pltpu.VMEM)
        shapes = ((B, D), (L, B, D), (L, B, D))
        vm = pltpu.VMEM
        dma = pltpu.SemaphoreType.DMA
        scratch = [
            vm((B, S, D), BF16), vm((B, S, D), BF16),
            vm((L, 3, 512, 512), BF16), vm((L, 512, 2048), BF16), vm((L, 512, 512), BF16), vm((L, 2048, 512), BF16),
            vm((NY, L, D), BF16), vm((1, B), jnp.int32), vm((1, D), F32),
            vm((B, D), F32), vm((B, D), F32), vm((B, D), F32),
            vm((L, NY, B, D), BF16),
            vm((L, nch, NX * NY, 1, B), F32),
            vm((NX, B, D), F32),
            vm((L, NX, B, D), BF16),
            vm((L, NX - 1, B, D), BF16),
            vm((2, 2, 2, B, D), F32),
            vm((L, 2, 2, 2, B, D), BF16),
            vm((L, 2, 2, B, D), BF16),
            vm((2, 2, B, D), F32),
            vm((L, 2, 2, B, D), BF16),
            vm((L, 2, B, D), BF16),
            vm((B, 1024), F32),
            vm((L, B, 1024), BF16),
            vm((L, B, 1024), BF16),
            vm((B, 1024), F32),
            vm((L, B, 1024), BF16),
            vm((L, B, 1024), BF16),
            vm((L, 2, B, 1024), BF16),
            vm((L, NX, B, D), BF16),
            vm((NY, B, D), F32),
            vm((L, NY, B, D), BF16),
            vm((L, NY - 1, B, D), BF16),
            vm((B, NY * D), BF16), vm((B, D), BF16), vm((B, D), F32),
            vm((B, S), F32), vm((B, S), BF16), vm((B, D), F32), vm((B, D), F32),
            dma((4,)), dma((4,)), dma((nch,)), dma((nch,)), dma((2,)),
            dma((len(KINDS), nch)), dma((len(KINDS), nch)),
        ]
        h_new, k_new, v_new = pl.pallas_call(
            functools.partial(_kernel, nch),
            out_shape=tuple(vm(n, BF16) for n in shapes),
            in_specs=[any_spec] * 12,
            out_specs=(vm_spec,) * 3,
            scratch_shapes=scratch,
            compiler_params=pltpu.CompilerParams(collective_id=0, has_side_effects=True,
                                                 vmem_limit_bytes=66_000_000),
            name="decode_step",
        )(h, g, wq, wk, wv, w_in, wo, w_out, kc.reshape(L, B, S, D), vc.reshape(L, B, S, D),
          lens.reshape(1, B), jnp.asarray(inv_np))
        h_new, k_new, v_new = pl.pallas_call(
            _tail,
            out_shape=tuple(jax.ShapeDtypeStruct(n, BF16) for n in shapes),
            in_specs=[vm_spec] * 3,
            out_specs=(any_spec,) * 3,
            scratch_shapes=[dma((3,))],
            name="results",
        )(*(pltpu.with_memory_space_constraint(a, pltpu.VMEM) for a in (h_new, k_new, v_new)))
        return h_new, k_new.reshape(L, B, 1, D), v_new.reshape(L, B, 1, D)

    return jax.shard_map(
        body, mesh=mesh,
        in_specs=(act, act, w_first, w_first, w_first, w_first, w_second, w_second, cache, cache, P(None)),
        out_specs=(act, new, new), check_vma=False)
```

```python
import functools

import jax
import jax.numpy as jnp
import numpy as np
from jax import lax
from jax.experimental import pallas as pl
from jax.experimental.pallas import tpu as pltpu
from jax.sharding import PartitionSpec as P

EPS = 1e-6
MESH = pl.DeviceIdType.MESH
F32 = jnp.float32
BF16 = jnp.bfloat16

L = 2
B = 128
D = 128
S = 512
NX = 4
NY = 4
E = 2048
G = 16
NG = B // G


KINDS = {k: n for n, k in enumerate(("s", "h", "q", "kv", "kvx", "u", "ux", "f", "o", "y"))}
SENDS = {"s": 0, "h": 1, "q": 0, "kv": 1, "kvx": 1, "u": 2, "ux": 2, "f": 1, "o": 0, "y": 0}
ORDER = ("IN*0 SQA0 SQB0 JN*0 XA0 RKVA0 XA0 RUA0 XA0 XA0 QA0 QKA0 QKA0 RKVB0 RUB0 SMA0 PVA0 KVA0 SOA0 RUB0 QB0 QKB0 QKB0 "
         "FA0 SMB0 PVB0 KVB0 SOB0 MLPA0 OUTA0 XA1 FB0 XA1 XA1 MLPB0 OUTB0 XA1 HA0 XB1 LVA0 XB1 XB1 LVB0 XB1 HB0 INA1 SQA1 JNA1 "
         "RKVA1 RUA1 INB1 SQB1 RUA1 JNB1 QA1 QKA1 QKA1 RKVB1 RUB1 SMA1 PVA1 KVA1 SOA1 QB1 QKB1 QKB1 SMB1 PVB1 KVB1 SOB1 FA1 "
         "MLPA1 FB1 OUTA1 MLPB1 OUTB1 HA1 HB1").split()


def _dot(a, b):
    return jnp.dot(a, b, preferred_element_type=F32)


def _dot_t(a, b):
    return lax.dot_general(a, b, (((1,), (1,)), ((), ())), preferred_element_type=F32)


def _kernel(nch, h_in, g_in, wq_in, wk_in, wv_in, win_in, wo_in, wout_in, kc_in, vc_in, lens_in, inv_in,
            h_out, k_out, v_out,
            kbuf, vbuf, wqkv, win, wo, wout, gg, lrow, inv, cosb, sinb, lenb,
            hg, ssb, qf, qb, qr, pf, pb, rq, sf, sb, xr, uf, ub, ur, usf, usb, ux, fb, og, zf, zb, zr,
            xbuf, qv, obuf, sbuf, pbuf, mbuf, dbuf,
            sem_in, sem_w, sem_k, sem_v, g_sem, send_sem, recv_sem):
    R = B // nch
    xi = lax.axis_index("x")
    yi = lax.axis_index("yz")
    c = lax.rem(xi, 2)
    xc = lax.div(xi, 2)
    partner = xi + 1 - 2 * c
    across = lax.rem(xi + 2, NX)
    open_sends, regions = {}, {}

    def exchange(kind, l, ch, copies, region, first=True):
        ss, rs = send_sem.at[SENDS[kind], ch], recv_sem.at[KINDS[kind], ch]
        if first:
            drain(SENDS[kind], ch)
        for src, dst, dev in copies:
            pltpu.make_async_remote_copy(src_ref=src, dst_ref=dst, send_sem=ss, recv_sem=rs,
                                         device_id={"x": xi, "yz": yi, **dev}, device_id_type=MESH).start()
        open_sends[SENDS[kind], ch] = regions[kind, ch] = region

    def drain(n, ch):
        region = open_sends.pop((n, ch), None)
        if region is not None:
            pltpu.make_async_copy(region, region, send_sem.at[n, ch]).wait()

    def arrived(kind, ch):
        region = regions[kind, ch]
        with jax.named_scope(f"w_{kind}_{ch}"):
            pltpu.make_async_copy(region, region, recv_sem.at[KINDS[kind], ch]).wait()

    def load(src, dst, sem):
        cp = pltpu.make_async_copy(src, dst, sem)
        cp.start()
        return cp

    in_h = load(h_in, hg.at[0, yi], sem_in.at[0])
    in_g = load(g_in, gg.at[yi], sem_in.at[1])
    in_l = load(lens_in, lrow, sem_in.at[2])
    in_i = load(inv_in, inv, sem_in.at[3])

    def load_first(l):
        for n, w in enumerate((wq_in, wk_in, wv_in)):
            load(w.at[l], wqkv.at[l, n], sem_w.at[0])
        load(win_in.at[l], win.at[l], sem_w.at[1])

    def load_second(l):
        load(wo_in.at[l], wo.at[l], sem_w.at[2])
        load(wout_in.at[l], wout.at[l], sem_w.at[3])

    def need_w(l, n):
        ref = (wqkv, win, wo, wout)[n].at[l]
        pltpu.make_async_copy(ref, ref, sem_w.at[n]).wait()

    load_first(0)

    barrier = pltpu.get_barrier_semaphore()
    for dx in range(NX):
        for dy in range(NY):
            if dx or dy:
                pl.semaphore_signal(barrier, inc=1, device_id={"yz": lax.rem(yi + dy, NY), "x": lax.rem(xi + dx, NX)},
                                    device_id_type=MESH)

    eye = (lax.broadcasted_iota(jnp.int32, (R, B), 0) == lax.broadcasted_iota(jnp.int32, (R, B), 1))

    def stats(l, ch, hb):
        col = jnp.sum(hb * hb, axis=1, keepdims=True)
        ssb[l, 0, ch] = jnp.sum(jnp.where(eye, col, 0.0), axis=0, keepdims=True)

    def send_h(l, ch, rows, chs):
        exchange("s", l, ch,
                 [(ssb.at[l, 0, chs], ssb.at[l, dx * NY + dy, chs],
                   {"x": lax.rem(xi + dx, NX), "yz": lax.rem(yi + dy, NY)})
                  for dx in (2, 1, 3, 0) for dy in (3, 1, 2, 0) if dx or dy],
                 ssb.at[l, pl.ds(1, NX * NY - 1), chs])
        exchange("h", l, ch,
                 [(hg.at[l, yi, rows], hg.at[l, yi, rows], {"yz": lax.rem(yi + d, NY)}) for d in (3, 1, 2)],
                 hg.at[l, pl.ds(0, NY - 1), rows])

    in_h.wait()
    in_g.wait()
    for ch in range(nch):
        stats(0, ch, hg[0, yi, pl.ds(ch * R, R), :].astype(F32))
    with jax.named_scope('barrier_wait'):
        pl.semaphore_wait(barrier, NX * NY - 1)
    send_h(0, 0, pl.ds(0, B), pl.ds(0, nch))
    for d in (1, 2, 3):
        pltpu.make_async_remote_copy(src_ref=gg.at[yi], dst_ref=gg.at[yi], send_sem=g_sem.at[0], recv_sem=g_sem.at[1],
                                     device_id={"x": xi, "yz": lax.rem(yi + d, NY)}, device_id_type=MESH).start()

    def load_cache(src, buf, sem, l, ch):
        for grp in range(ch * gpc, (ch + 1) * gpc):
            seqs = pl.ds(grp * G, G)
            load(src.at[l, seqs], buf.at[seqs], sem.at[ch])

    def need_cache(buf, sem, ch):
        ref = buf.at[pl.ds(ch * R, R)]
        pltpu.make_async_copy(ref, ref, sem.at[ch]).wait()

    gpc = NG // nch
    for ch in range(nch):
        load_cache(kc_in, kbuf, sem_k, 0, ch)
        load_cache(vc_in, vbuf, sem_v, 0, ch)
    load_second(0)

    in_l.wait()
    in_i.wait()
    eye_b = (lax.broadcasted_iota(jnp.int32, (B, B), 0) == lax.broadcasted_iota(jnp.int32, (B, B), 1))
    lcol = jnp.sum(jnp.where(eye_b, lrow[...].astype(F32), 0.0), axis=1, keepdims=True)
    lenb[...] = jnp.broadcast_to(lcol, (B, D))
    ang = lcol * inv[...]
    cosb[...] = jnp.cos(ang)
    half = lax.broadcasted_iota(jnp.int32, (B, D), 1) < D // 2
    sn = jnp.sin(ang)
    sinb[...] = jnp.where(half, -sn, sn)

    def stage_in(l, chunks):
        span = pl.ds(chunks[0] * R, R * len(chunks))
        scales = []
        for ch in chunks:
            if l > 0 or ch == 0:
                arrived("h", ch)
                arrived("s", ch)
            row = ssb[l, 0, ch]
            for slot in range(1, NX * NY):
                row = row + ssb[l, slot, ch]
            col = jnp.sum(jnp.where(eye, row, 0.0), axis=1, keepdims=True)
            scales.append(lax.rsqrt(col / E + EPS))
        r = jnp.concatenate(scales, axis=0)
        if 0 in chunks:
            if l == 0:
                ref = gg.at[pl.ds(0, NY - 1)]
                pltpu.make_async_copy(ref, ref, g_sem.at[1]).wait()
                pltpu.make_async_copy(ref, ref, g_sem.at[0]).wait()
            need_w(l, 0)
            need_w(l, 1)
        xs = []
        for j in range(NY):
            gj = gg[j, pl.ds(l, 1), :].astype(F32)
            xs.append((hg[l, j, span, :].astype(F32) * r * gj).astype(BF16))
        x = jnp.concatenate(xs, axis=1)
        xbuf[span, :] = x
        for n in range(2):
            acc = _dot(x, wqkv[l, 0, :, pl.ds(n * 256, 256)])
            for m in range(2):
                a = acc[:, m * D:(m + 1) * D]
                qf[2 * n + m, span, :] = a
                qb[l, 2 * n + m, span, :] = a.astype(BF16)

    def send_q(l, ch):
        rows = pl.ds(ch * R, R)
        tos = [lax.rem(xi + d, NX) for d in range(NX)]
        exchange("q", l, ch, [(qb.at[l, tos[d], rows], qr.at[l, d - 1, rows], {"x": tos[d]}) for d in (2, 1, 3)],
                 qr.at[l, :, rows])

    def stage_in_rest(l, chunks):
        span = pl.ds(chunks[0] * R, R * len(chunks))
        x = xbuf[span, :]
        for t in range(2):
            for n in range(2):
                acc = _dot(x, wqkv[l, t + 1, :, pl.ds(n * 256, 256)])
                for cc in range(2):
                    a = acc[:, cc * D:(cc + 1) * D]
                    pf[cc, t, n, span, :] = a
                    pb[l, cc, t, n, span, :] = a.astype(BF16)
        for ch in chunks:
            rows = pl.ds(ch * R, R)
            exchange("kv", l, ch, [(pb.at[l, 1 - c, :, :, rows], rq.at[l, :, :, rows], {"x": partner})],
                     rq.at[l, :, :, rows])
        for n in range(8):
            acc = _dot(x, win[l, :, pl.ds(n * 256, 256)])
            cols = pl.ds((n % 4) * 256, 256)
            uf[n // 4, span, cols] = acc
            ub[l, n // 4, span, cols] = acc.astype(BF16)
        for ch in chunks:
            rows = pl.ds(ch * R, R)
            exchange("u", l, ch, [(ub.at[l, 1 - c, rows], ur.at[l, rows], {"x": partner})], ur.at[l, rows])
        if nch - 1 in chunks and l + 1 < L:
            load_first(l + 1)

    def reduce_kv(l, ch):
        rows = pl.ds(ch * R, R)
        arrived("kv", ch)
        for t in range(2):
            for n in range(2):
                s = pf[c, t, n, rows, :] + rq[l, t, n, rows, :].astype(F32)
                sf[n, t, rows, :] = s
                sb[l, n, t, rows, :] = s.astype(BF16)
        exchange("kvx", l, ch, [(sb.at[l, 1 - xc, :, rows], xr.at[l, :, rows], {"x": across})], xr.at[l, :, rows])

    u_done = {}

    def reduce_u(l, ch):
        pieces = ORDER.count(f"RU{'AB'[ch]}{l}")
        piece = u_done.get((l, ch), 0)
        u_done[l, ch] = piece + 1
        if piece == 0:
            arrived("u", ch)
        rows = pl.ds(ch * R + piece * (R // pieces), R // pieces)
        us = uf[c, rows, :] + ur[l, rows, :].astype(F32)
        usf[rows, :] = us
        usb[l, rows, :] = us.astype(BF16)
        exchange("ux", l, ch, [(usb.at[l, rows], ux.at[l, rows], {"x": across})], ux.at[l, pl.ds(ch * R, R)],
                 first=piece == 0)

    def rope(t, rows):
        tf = t.astype(F32)
        return (tf * cosb[rows, :] + pltpu.roll(tf, D // 2, 1) * sinb[rows, :]).astype(BF16)

    def stage_q(l, ch):
        rows = pl.ds(ch * R, R)
        arrived("q", ch)
        q = qf[xi, rows, :]
        for d in range(NX - 1):
            q = q + qr[l, d, rows, :].astype(F32)
        qv[rows, :] = rope(q.astype(BF16), rows)

    rowid = lax.broadcasted_iota(jnp.int32, (G, D), 0)
    pos = lax.broadcasted_iota(jnp.int32, (R, S), 1).astype(F32)
    scale = D ** -0.5

    ready, flipped, scored = set(), {}, {}

    def need_keys(l, ch):
        if (l, ch) not in ready:
            ready.add((l, ch))
            need_cache(kbuf, sem_k, ch)

    def transpose(l, ch):
        need_keys(l, ch)
        g = flipped.get((l, ch), 0)
        flipped[l, ch] = g + 1
        for b in range(ch * R + g * G, ch * R + (g + 1) * G):
            for j in range(S // D):
                kbuf[b, pl.ds(j * D, D), :] = kbuf[b, pl.ds(j * D, D), :].T

    def scores(l, ch):
        need_keys(l, ch)
        first = scored.get((l, ch), 0)
        scored[l, ch] = first + gpc // 2
        for g in range(first, first + gpc // 2):
            base = ch * R + g * G
            rows = pl.ds(base, G)
            q = qv[rows, :].astype(F32)
            s = jnp.zeros((G, S), F32)
            for i in range(0, G, 2):
                lhs = jnp.concatenate([jnp.where(rowid == i, q, 0.0), jnp.where(rowid == i + 1, q, 0.0)],
                                      axis=1).astype(BF16)
                if g < flipped.get((l, ch), 0):
                    keys = [jnp.concatenate([kbuf[base + i + e, pl.ds(j * D, D), :] for j in range(S // D)], axis=1)
                            for e in range(2)]
                    s = s + _dot(lhs, jnp.concatenate(keys, axis=0))
                else:
                    s = s + _dot_t(lhs, jnp.concatenate([kbuf[base + i], kbuf[base + i + 1]], axis=1))
            sbuf[rows, :] = s
        if scored[l, ch] == gpc and l + 1 < L:
            load_cache(kc_in, kbuf, sem_k, l + 1, ch)

    def softmax(l, ch):
        rows = pl.ds(ch * R, R)
        s = jnp.where(pos < lenb[rows, :][:, :1], sbuf[rows, :] * scale, -jnp.inf)
        m = jnp.max(s, axis=1, keepdims=True)
        p = jnp.exp(s - m)
        pbuf[rows, :] = p.astype(BF16)
        mbuf[rows, :] = jnp.broadcast_to(m, (R, D))
        dbuf[rows, :] = jnp.broadcast_to(jnp.sum(p, axis=1, keepdims=True), (R, D))

    def values(l, ch):
        need_cache(vbuf, sem_v, ch)
        for g in range(gpc):
            base = ch * R + g * G
            rows = pl.ds(base, G)
            p = pbuf[rows, :]
            o = jnp.zeros((G, D), F32)
            for i in range(0, G, 2):
                t = _dot(p, jnp.concatenate([vbuf[base + i], vbuf[base + i + 1]], axis=1))
                o = o + jnp.where(rowid == i, t[:, :D], jnp.where(rowid == i + 1, t[:, D:], 0.0))
            obuf[rows, :] = o

    def load_values(l, ch):
        load_cache(vc_in, vbuf, sem_v, l + 1, ch)

    def stage_kv(l, ch):
        rows = pl.ds(ch * R, R)
        arrived("kvx", ch)
        k = rope((sf[xc, 0, rows, :] + xr[l, 0, rows, :].astype(F32)).astype(BF16), rows)
        v = (sf[xc, 1, rows, :] + xr[l, 1, rows, :].astype(F32)).astype(BF16)
        k_out[l, rows, :] = k
        v_out[l, rows, :] = v
        s_new = jnp.sum(qv[rows, :].astype(F32) * k.astype(F32), axis=1, keepdims=True) * scale
        m_c = mbuf[rows, :]
        m = jnp.maximum(m_c, s_new)
        a = jnp.exp(m_c - m)
        p_new = jnp.exp(s_new - m)
        o = (a * obuf[rows, :] + p_new * v.astype(F32)) / (a * dbuf[rows, :] + p_new)
        og[l, xi, rows, :] = o.astype(BF16)

    def send_o(l, ch):
        rows = pl.ds(ch * R, R)
        exchange("o", l, ch, [(og.at[l, xi, rows], og.at[l, xi, rows], {"x": lax.rem(xi + d, NX)}) for d in (2, 1, 3)],
                 og.at[l, pl.ds(0, NX - 1), rows])

    def stage_f(l, ch):
        rows = pl.ds(ch * R, R)
        arrived("ux", ch)
        u = (usf[rows, :] + ux[l, rows, :].astype(F32)).astype(BF16)
        fb[l, c, rows, :] = jax.nn.gelu(u.astype(F32), approximate=True).astype(BF16)
        exchange("f", l, ch, [(fb.at[l, c, rows], fb.at[l, c, rows], {"x": partner})], fb.at[l, 0, rows])

    def stage_mlp(l, ch):
        rows = pl.ds(ch * R, R)
        arrived("f", ch)
        if ch == 0:
            need_w(l, 3)
        f = jnp.concatenate([fb[l, 0, rows, :], fb[l, 1, rows, :]], axis=1)
        for n in range(2):
            acc = _dot(f, wout[l, :, pl.ds(n * 256, 256)])
            zf[2 * n, rows, :] = acc[:, :D]
            zf[2 * n + 1, rows, :] = acc[:, D:]

    def stage_out(l, ch):
        rows = pl.ds(ch * R, R)
        arrived("o", ch)
        if ch == 0:
            need_w(l, 2)
        o = jnp.concatenate([og[l, j, rows, :] for j in range(NX)], axis=1)
        for n in range(2):
            acc = _dot(o, wo[l, :, pl.ds(n * 256, 256)])
            for m in range(2):
                a = acc[:, m * D:(m + 1) * D] + zf[2 * n + m, rows, :]
                zf[2 * n + m, rows, :] = a
                zb[l, 2 * n + m, rows, :] = a.astype(BF16)
        tos = [lax.rem(yi + d, NY) for d in range(NY)]
        exchange("y", l, ch, [(zb.at[l, tos[d], rows], zr.at[l, d - 1, rows], {"yz": tos[d]}) for d in (3, 1, 2)],
                 zr.at[l, :, rows])
        if ch == nch - 1 and l + 1 < L:
            load_second(l + 1)

    def stage_h(l, ch):
        rows = pl.ds(ch * R, R)
        arrived("y", ch)
        y = zf[yi, rows, :]
        for d in range(NY - 1):
            y = y + zr[l, d, rows, :].astype(F32)
        hn = (hg[l, yi, rows, :].astype(F32) + y.astype(BF16).astype(F32)).astype(BF16)
        if l + 1 < L:
            hg[l + 1, yi, rows, :] = hn
            stats(l + 1, ch, hn.astype(F32))
            send_h(l + 1, ch, rows, pl.ds(ch, 1))
        else:
            h_out[rows, :] = hn

    stages = dict(IN=stage_in, SQ=send_q, JN=stage_in_rest, RKV=reduce_kv, RU=reduce_u, Q=stage_q, QK=scores, X=transpose, KV=stage_kv, SM=softmax, PV=values, LV=load_values,
                  SO=send_o, F=stage_f, MLP=stage_mlp, OUT=stage_out, H=stage_h)
    for step in ORDER:
        with jax.named_scope(step):
            chunks = range(nch) if step[-2] == "*" else ("AB".index(step[-2]),)
            stages[step[:-2]](int(step[-1]), chunks if step[:2] in ("IN", "JN") else chunks[0])
    for n, ch in list(open_sends):
        drain(n, ch)


def _tail(h_in, k_in, v_in, h_out, k_out, v_out, sem):
    cps = [pltpu.make_async_copy(a, o, sem.at[n])
           for n, (a, o) in enumerate(((k_in, k_out), (v_in, v_out), (h_in, h_out)))]
    for cp in cps:
        cp.start()
    for cp in cps:
        cp.wait()


def solution(mesh):
    nch = 2
    act = P(None, ('x', 'yz'))
    w_first = P(None, 'x', 'yz')
    w_second = P(None, 'yz', 'x')
    cache = P(None, None, ('yz', 'x'), None, None)
    new = P(None, None, ('yz', 'x'), None)
    inv_half = 10000.0 ** (-np.arange(D // 2, dtype=np.float64) / (D // 2))
    inv_np = np.concatenate([inv_half, inv_half]).astype(np.float32)[None]

    def body(h, g, wq, wk, wv, w_in, wo, w_out, kc, vc, lens):
        any_spec = pl.BlockSpec(memory_space=pl.ANY)
        vm_spec = pl.BlockSpec(memory_space=pltpu.VMEM)
        shapes = ((B, D), (L, B, D), (L, B, D))
        vm = pltpu.VMEM
        dma = pltpu.SemaphoreType.DMA
        scratch = [
            vm((B, S, D), BF16), vm((B, S, D), BF16),
            vm((L, 3, 512, 512), BF16), vm((L, 512, 2048), BF16), vm((L, 512, 512), BF16), vm((L, 2048, 512), BF16),
            vm((NY, L, D), BF16), vm((1, B), jnp.int32), vm((1, D), F32),
            vm((B, D), F32), vm((B, D), F32), vm((B, D), F32),
            vm((L, NY, B, D), BF16),
            vm((L, NX * NY, nch, 1, B), F32),
            vm((NX, B, D), F32),
            vm((L, NX, B, D), BF16),
            vm((L, NX - 1, B, D), BF16),
            vm((2, 2, 2, B, D), F32),
            vm((L, 2, 2, 2, B, D), BF16),
            vm((L, 2, 2, B, D), BF16),
            vm((2, 2, B, D), F32),
            vm((L, 2, 2, B, D), BF16),
            vm((L, 2, B, D), BF16),
            vm((2, B, 1024), F32),
            vm((L, 2, B, 1024), BF16),
            vm((L, B, 1024), BF16),
            vm((B, 1024), F32),
            vm((L, B, 1024), BF16),
            vm((L, B, 1024), BF16),
            vm((L, 2, B, 1024), BF16),
            vm((L, NX, B, D), BF16),
            vm((NY, B, D), F32),
            vm((L, NY, B, D), BF16),
            vm((L, NY - 1, B, D), BF16),
            vm((B, NY * D), BF16), vm((B, D), BF16), vm((B, D), F32),
            vm((B, S), F32), vm((B, S), BF16), vm((B, D), F32), vm((B, D), F32),
            dma((4,)), dma((4,)), dma((nch,)), dma((nch,)), dma((2,)),
            dma((3, nch)), dma((len(KINDS), nch)),
        ]
        h_new, k_new, v_new = pl.pallas_call(
            functools.partial(_kernel, nch),
            out_shape=tuple(vm(n, BF16) for n in shapes),
            in_specs=[any_spec] * 12,
            out_specs=(vm_spec,) * 3,
            scratch_shapes=scratch,
            compiler_params=pltpu.CompilerParams(collective_id=0, has_side_effects=True,
                                                 vmem_limit_bytes=66_000_000),
            name="decode_step",
        )(h, g, wq, wk, wv, w_in, wo, w_out, kc.reshape(L, B, S, D), vc.reshape(L, B, S, D),
          lens.reshape(1, B), jnp.asarray(inv_np))
        h_new, k_new, v_new = pl.pallas_call(
            _tail,
            out_shape=tuple(jax.ShapeDtypeStruct(n, BF16) for n in shapes),
            in_specs=[vm_spec] * 3,
            out_specs=(any_spec,) * 3,
            scratch_shapes=[dma((3,))],
            name="results",
        )(*(pltpu.with_memory_space_constraint(a, pltpu.VMEM) for a in (h_new, k_new, v_new)))
        return h_new, k_new.reshape(L, B, 1, D), v_new.reshape(L, B, 1, D)

    return jax.shard_map(
        body, mesh=mesh,
        in_specs=(act, act, w_first, w_first, w_first, w_first, w_second, w_second, cache, cache, P(None)),
        out_specs=(act, new, new), check_vma=False)
```

```python
import functools

import jax
import jax.numpy as jnp
import numpy as np
from jax import lax
from jax.experimental import pallas as pl
from jax.experimental.pallas import tpu as pltpu
from jax.sharding import PartitionSpec as P

EPS = 1e-6
MESH = pl.DeviceIdType.MESH
F32 = jnp.float32
BF16 = jnp.bfloat16

L = 2
B = 128
D = 128
S = 512
NX = 4
NY = 4
E = 2048
G = 16
NG = B // G


KINDS = {k: n for n, k in enumerate(("s", "h", "q", "kv", "kvx", "u", "ux", "f", "o", "y"))}
SENDS = {"s": 0, "h": 1, "q": 0, "kv": 1, "kvx": 1, "u": 2, "ux": 2, "f": 1, "o": 0, "y": 0}
ORDER = ("IN*0 SQA0 SQB0 JN*0 XA0 RKVA0 XA0 RUA0 XA0 XA0 QA0 QKA0 QKA0 RKVB0 RUB0 SMA0 PVA0 KVA0 SOA0 RUB0 QB0 QKB0 QKB0 "
         "FA0 SMB0 PVB0 KVB0 SOB0 MLPA0 OUTA0 XA1 FB0 XA1 XA1 MLPB0 OUTB0 XA1 HA0 XB1 LVA0 XB1 XB1 LVB0 HB0 XB1 INA1 SQA1 JNA1 "
         "RKVA1 RUA1 INB1 SQB1 RUA1 JNB1 QA1 QKA1 QKA1 RKVB1 RUB1 SMA1 PVA1 KVA1 SOA1 QB1 QKB1 QKB1 SMB1 PVB1 KVB1 SOB1 FA1 "
         "MLPA1 FB1 OUTA1 MLPB1 OUTB1 HA1 HB1").split()


def _dot(a, b):
    return jnp.dot(a, b, preferred_element_type=F32)


def _dot_t(a, b):
    return lax.dot_general(a, b, (((1,), (1,)), ((), ())), preferred_element_type=F32)


def _kernel(nch, h_in, g_in, wq_in, wk_in, wv_in, win_in, wo_in, wout_in, kc_in, vc_in, lens_in, inv_in,
            h_out, k_out, v_out,
            kbuf, vbuf, wqkv, win, wo, wout, gg, lrow, inv, cosb, sinb, lenb,
            hg, ssb, qf, qb, qr, pf, pb, rq, sf, sb, xr, uf, ub, ur, usf, usb, ux, fb, og, zf, zb, zr,
            xbuf, qv, obuf, sbuf, pbuf, mbuf, dbuf,
            sem_in, sem_w, sem_k, sem_v, g_sem, send_sem, recv_sem):
    R = B // nch
    xi = lax.axis_index("x")
    yi = lax.axis_index("yz")
    c = lax.rem(xi, 2)
    xc = lax.div(xi, 2)
    partner = xi + 1 - 2 * c
    across = lax.rem(xi + 2, NX)
    open_sends, regions = {}, {}

    def exchange(kind, l, ch, copies, region, first=True):
        ss, rs = send_sem.at[SENDS[kind], ch], recv_sem.at[KINDS[kind], ch]
        if first:
            drain(SENDS[kind], ch)
        for src, dst, dev in copies:
            pltpu.make_async_remote_copy(src_ref=src, dst_ref=dst, send_sem=ss, recv_sem=rs,
                                         device_id={"x": xi, "yz": yi, **dev}, device_id_type=MESH).start()
        open_sends[SENDS[kind], ch] = regions[kind, ch] = region

    def drain(n, ch):
        region = open_sends.pop((n, ch), None)
        if region is not None:
            pltpu.make_async_copy(region, region, send_sem.at[n, ch]).wait()

    def arrived(kind, ch):
        region = regions[kind, ch]
        with jax.named_scope(f"w_{kind}_{ch}"):
            pltpu.make_async_copy(region, region, recv_sem.at[KINDS[kind], ch]).wait()

    def load(src, dst, sem):
        cp = pltpu.make_async_copy(src, dst, sem)
        cp.start()
        return cp

    in_h = load(h_in, hg.at[0, yi], sem_in.at[0])
    in_g = load(g_in, gg.at[yi], sem_in.at[1])
    in_l = load(lens_in, lrow, sem_in.at[2])
    in_i = load(inv_in, inv, sem_in.at[3])

    def load_first(l):
        for n, w in enumerate((wq_in, wk_in, wv_in)):
            load(w.at[l], wqkv.at[l, n], sem_w.at[0])
        load(win_in.at[l], win.at[l], sem_w.at[1])

    def load_second(l):
        load(wo_in.at[l], wo.at[l], sem_w.at[2])
        load(wout_in.at[l], wout.at[l], sem_w.at[3])

    def need_w(l, n):
        ref = (wqkv, win, wo, wout)[n].at[l]
        pltpu.make_async_copy(ref, ref, sem_w.at[n]).wait()

    load_first(0)

    barrier = pltpu.get_barrier_semaphore()
    for dx in range(NX):
        for dy in range(NY):
            if dx or dy:
                pl.semaphore_signal(barrier, inc=1, device_id={"yz": lax.rem(yi + dy, NY), "x": lax.rem(xi + dx, NX)},
                                    device_id_type=MESH)

    eye = (lax.broadcasted_iota(jnp.int32, (R, B), 0) == lax.broadcasted_iota(jnp.int32, (R, B), 1))

    def stats(l, ch, hb):
        col = jnp.sum(hb * hb, axis=1, keepdims=True)
        ssb[l, 0, ch] = jnp.sum(jnp.where(eye, col, 0.0), axis=0, keepdims=True)

    def send_h(l, ch, rows, chs):
        exchange("s", l, ch,
                 [(ssb.at[l, 0, chs], ssb.at[l, dx * NY + dy, chs],
                   {"x": lax.rem(xi + dx, NX), "yz": lax.rem(yi + dy, NY)})
                  for dx in (2, 1, 3, 0) for dy in (3, 1, 2, 0) if dx or dy],
                 ssb.at[l, pl.ds(1, NX * NY - 1), chs])
        exchange("h", l, ch,
                 [(hg.at[l, yi, rows], hg.at[l, yi, rows], {"yz": lax.rem(yi + d, NY)}) for d in (3, 1, 2)],
                 hg.at[l, pl.ds(0, NY - 1), rows])

    in_h.wait()
    in_g.wait()
    for ch in range(nch):
        stats(0, ch, hg[0, yi, pl.ds(ch * R, R), :].astype(F32))
    with jax.named_scope('barrier_wait'):
        pl.semaphore_wait(barrier, NX * NY - 1)
    send_h(0, 0, pl.ds(0, B), pl.ds(0, nch))
    for d in (1, 2, 3):
        pltpu.make_async_remote_copy(src_ref=gg.at[yi], dst_ref=gg.at[yi], send_sem=g_sem.at[0], recv_sem=g_sem.at[1],
                                     device_id={"x": xi, "yz": lax.rem(yi + d, NY)}, device_id_type=MESH).start()

    def load_cache(src, buf, sem, l, ch):
        for grp in range(ch * gpc, (ch + 1) * gpc):
            seqs = pl.ds(grp * G, G)
            load(src.at[l, seqs], buf.at[seqs], sem.at[ch])

    def need_cache(buf, sem, ch):
        ref = buf.at[pl.ds(ch * R, R)]
        pltpu.make_async_copy(ref, ref, sem.at[ch]).wait()

    gpc = NG // nch
    for ch in range(nch):
        load_cache(kc_in, kbuf, sem_k, 0, ch)
        load_cache(vc_in, vbuf, sem_v, 0, ch)
    load_second(0)

    in_l.wait()
    in_i.wait()
    eye_b = (lax.broadcasted_iota(jnp.int32, (B, B), 0) == lax.broadcasted_iota(jnp.int32, (B, B), 1))
    lcol = jnp.sum(jnp.where(eye_b, lrow[...].astype(F32), 0.0), axis=1, keepdims=True)
    lenb[...] = jnp.broadcast_to(lcol, (B, D))
    ang = lcol * inv[...]
    cosb[...] = jnp.cos(ang)
    half = lax.broadcasted_iota(jnp.int32, (B, D), 1) < D // 2
    sn = jnp.sin(ang)
    sinb[...] = jnp.where(half, -sn, sn)

    def stage_in(l, chunks):
        span = pl.ds(chunks[0] * R, R * len(chunks))
        scales = []
        for ch in chunks:
            if l > 0 or ch == 0:
                arrived("h", ch)
                arrived("s", ch)
            row = ssb[l, 0, ch]
            for slot in range(1, NX * NY):
                row = row + ssb[l, slot, ch]
            col = jnp.sum(jnp.where(eye, row, 0.0), axis=1, keepdims=True)
            scales.append(lax.rsqrt(col / E + EPS))
        r = jnp.concatenate(scales, axis=0)
        if 0 in chunks:
            if l == 0:
                ref = gg.at[pl.ds(0, NY - 1)]
                pltpu.make_async_copy(ref, ref, g_sem.at[1]).wait()
                pltpu.make_async_copy(ref, ref, g_sem.at[0]).wait()
            need_w(l, 0)
            need_w(l, 1)
        xs = []
        for j in range(NY):
            gj = gg[j, pl.ds(l, 1), :].astype(F32)
            xs.append((hg[l, j, span, :].astype(F32) * r * gj).astype(BF16))
        x = jnp.concatenate(xs, axis=1)
        xbuf[span, :] = x
        for n in range(2):
            acc = _dot(x, wqkv[l, 0, :, pl.ds(n * 256, 256)])
            for m in range(2):
                a = acc[:, m * D:(m + 1) * D]
                qf[2 * n + m, span, :] = a
                qb[l, 2 * n + m, span, :] = a.astype(BF16)

    def send_q(l, ch):
        rows = pl.ds(ch * R, R)
        tos = [lax.rem(xi + d, NX) for d in range(NX)]
        exchange("q", l, ch, [(qb.at[l, tos[d], rows], qr.at[l, d - 1, rows], {"x": tos[d]}) for d in (2, 1, 3)],
                 qr.at[l, :, rows])

    def stage_in_rest(l, chunks):
        span = pl.ds(chunks[0] * R, R * len(chunks))
        x = xbuf[span, :]
        for t in range(2):
            for n in range(2):
                acc = _dot(x, wqkv[l, t + 1, :, pl.ds(n * 256, 256)])
                for cc in range(2):
                    a = acc[:, cc * D:(cc + 1) * D]
                    pf[cc, t, n, span, :] = a
                    pb[l, cc, t, n, span, :] = a.astype(BF16)
        for ch in chunks:
            rows = pl.ds(ch * R, R)
            exchange("kv", l, ch, [(pb.at[l, 1 - c, :, :, rows], rq.at[l, :, :, rows], {"x": partner})],
                     rq.at[l, :, :, rows])
        for n in range(8):
            acc = _dot(x, win[l, :, pl.ds(n * 256, 256)])
            cols = pl.ds((n % 4) * 256, 256)
            uf[n // 4, span, cols] = acc
            ub[l, n // 4, span, cols] = acc.astype(BF16)
        for ch in chunks:
            rows = pl.ds(ch * R, R)
            exchange("u", l, ch, [(ub.at[l, 1 - c, rows], ur.at[l, rows], {"x": partner})], ur.at[l, rows])
        if nch - 1 in chunks and l + 1 < L:
            load_first(l + 1)

    def reduce_kv(l, ch):
        rows = pl.ds(ch * R, R)
        arrived("kv", ch)
        for t in range(2):
            for n in range(2):
                s = pf[c, t, n, rows, :] + rq[l, t, n, rows, :].astype(F32)
                sf[n, t, rows, :] = s
                sb[l, n, t, rows, :] = s.astype(BF16)
        exchange("kvx", l, ch, [(sb.at[l, 1 - xc, :, rows], xr.at[l, :, rows], {"x": across})], xr.at[l, :, rows])

    u_done = {}

    def reduce_u(l, ch):
        pieces = ORDER.count(f"RU{'AB'[ch]}{l}")
        piece = u_done.get((l, ch), 0)
        u_done[l, ch] = piece + 1
        if piece == 0:
            arrived("u", ch)
        rows = pl.ds(ch * R + piece * (R // pieces), R // pieces)
        us = uf[c, rows, :] + ur[l, rows, :].astype(F32)
        usf[rows, :] = us
        usb[l, rows, :] = us.astype(BF16)
        exchange("ux", l, ch, [(usb.at[l, rows], ux.at[l, rows], {"x": across})], ux.at[l, pl.ds(ch * R, R)],
                 first=piece == 0)

    def rope(t, rows):
        tf = t.astype(F32)
        return (tf * cosb[rows, :] + pltpu.roll(tf, D // 2, 1) * sinb[rows, :]).astype(BF16)

    def stage_q(l, ch):
        rows = pl.ds(ch * R, R)
        arrived("q", ch)
        q = qf[xi, rows, :]
        for d in range(NX - 1):
            q = q + qr[l, d, rows, :].astype(F32)
        qv[rows, :] = rope(q.astype(BF16), rows)

    rowid = lax.broadcasted_iota(jnp.int32, (G, D), 0)
    pos = lax.broadcasted_iota(jnp.int32, (R, S), 1).astype(F32)
    scale = D ** -0.5

    ready, flipped, scored = set(), {}, {}

    def need_keys(l, ch):
        if (l, ch) not in ready:
            ready.add((l, ch))
            need_cache(kbuf, sem_k, ch)

    def transpose(l, ch):
        need_keys(l, ch)
        g = flipped.get((l, ch), 0)
        flipped[l, ch] = g + 1
        for b in range(ch * R + g * G, ch * R + (g + 1) * G):
            for j in range(S // D):
                kbuf[b, pl.ds(j * D, D), :] = kbuf[b, pl.ds(j * D, D), :].T

    def scores(l, ch):
        need_keys(l, ch)
        first = scored.get((l, ch), 0)
        scored[l, ch] = first + gpc // 2
        for g in range(first, first + gpc // 2):
            base = ch * R + g * G
            rows = pl.ds(base, G)
            q = qv[rows, :].astype(F32)
            s = jnp.zeros((G, S), F32)
            for i in range(0, G, 2):
                lhs = jnp.concatenate([jnp.where(rowid == i, q, 0.0), jnp.where(rowid == i + 1, q, 0.0)],
                                      axis=1).astype(BF16)
                if g < flipped.get((l, ch), 0):
                    keys = [jnp.concatenate([kbuf[base + i + e, pl.ds(j * D, D), :] for j in range(S // D)], axis=1)
                            for e in range(2)]
                    s = s + _dot(lhs, jnp.concatenate(keys, axis=0))
                else:
                    s = s + _dot_t(lhs, jnp.concatenate([kbuf[base + i], kbuf[base + i + 1]], axis=1))
            sbuf[rows, :] = s
        if scored[l, ch] == gpc and l + 1 < L:
            load_cache(kc_in, kbuf, sem_k, l + 1, ch)

    def softmax(l, ch):
        rows = pl.ds(ch * R, R)
        s = jnp.where(pos < lenb[rows, :][:, :1], sbuf[rows, :] * scale, -jnp.inf)
        m = jnp.max(s, axis=1, keepdims=True)
        p = jnp.exp(s - m)
        pbuf[rows, :] = p.astype(BF16)
        mbuf[rows, :] = jnp.broadcast_to(m, (R, D))
        dbuf[rows, :] = jnp.broadcast_to(jnp.sum(p, axis=1, keepdims=True), (R, D))

    def values(l, ch):
        need_cache(vbuf, sem_v, ch)
        for g in range(gpc):
            base = ch * R + g * G
            rows = pl.ds(base, G)
            p = pbuf[rows, :]
            o = jnp.zeros((G, D), F32)
            for i in range(0, G, 2):
                t = _dot(p, jnp.concatenate([vbuf[base + i], vbuf[base + i + 1]], axis=1))
                o = o + jnp.where(rowid == i, t[:, :D], jnp.where(rowid == i + 1, t[:, D:], 0.0))
            obuf[rows, :] = o

    def load_values(l, ch):
        load_cache(vc_in, vbuf, sem_v, l + 1, ch)

    def stage_kv(l, ch):
        rows = pl.ds(ch * R, R)
        arrived("kvx", ch)
        k = rope((sf[xc, 0, rows, :] + xr[l, 0, rows, :].astype(F32)).astype(BF16), rows)
        v = (sf[xc, 1, rows, :] + xr[l, 1, rows, :].astype(F32)).astype(BF16)
        k_out[l, rows, :] = k
        v_out[l, rows, :] = v
        s_new = jnp.sum(qv[rows, :].astype(F32) * k.astype(F32), axis=1, keepdims=True) * scale
        m_c = mbuf[rows, :]
        m = jnp.maximum(m_c, s_new)
        a = jnp.exp(m_c - m)
        p_new = jnp.exp(s_new - m)
        o = (a * obuf[rows, :] + p_new * v.astype(F32)) / (a * dbuf[rows, :] + p_new)
        og[l, xi, rows, :] = o.astype(BF16)

    def send_o(l, ch):
        rows = pl.ds(ch * R, R)
        exchange("o", l, ch, [(og.at[l, xi, rows], og.at[l, xi, rows], {"x": lax.rem(xi + d, NX)}) for d in (2, 1, 3)],
                 og.at[l, pl.ds(0, NX - 1), rows])

    def stage_f(l, ch):
        rows = pl.ds(ch * R, R)
        arrived("ux", ch)
        u = (usf[rows, :] + ux[l, rows, :].astype(F32)).astype(BF16)
        fb[l, c, rows, :] = jax.nn.gelu(u.astype(F32), approximate=True).astype(BF16)
        exchange("f", l, ch, [(fb.at[l, c, rows], fb.at[l, c, rows], {"x": partner})], fb.at[l, 0, rows])

    def stage_mlp(l, ch):
        rows = pl.ds(ch * R, R)
        arrived("f", ch)
        if ch == 0:
            need_w(l, 3)
        f = jnp.concatenate([fb[l, 0, rows, :], fb[l, 1, rows, :]], axis=1)
        for n in range(2):
            acc = _dot(f, wout[l, :, pl.ds(n * 256, 256)])
            zf[2 * n, rows, :] = acc[:, :D]
            zf[2 * n + 1, rows, :] = acc[:, D:]

    def stage_out(l, ch):
        rows = pl.ds(ch * R, R)
        arrived("o", ch)
        if ch == 0:
            need_w(l, 2)
        o = jnp.concatenate([og[l, j, rows, :] for j in range(NX)], axis=1)
        for n in range(2):
            acc = _dot(o, wo[l, :, pl.ds(n * 256, 256)])
            for m in range(2):
                a = acc[:, m * D:(m + 1) * D] + zf[2 * n + m, rows, :]
                zf[2 * n + m, rows, :] = a
                zb[l, 2 * n + m, rows, :] = a.astype(BF16)
        tos = [lax.rem(yi + d, NY) for d in range(NY)]
        exchange("y", l, ch, [(zb.at[l, tos[d], rows], zr.at[l, d - 1, rows], {"yz": tos[d]}) for d in (3, 1, 2)],
                 zr.at[l, :, rows])
        if ch == nch - 1 and l + 1 < L:
            load_second(l + 1)

    def stage_h(l, ch):
        rows = pl.ds(ch * R, R)
        arrived("y", ch)
        y = zf[yi, rows, :]
        for d in range(NY - 1):
            y = y + zr[l, d, rows, :].astype(F32)
        hn = (hg[l, yi, rows, :].astype(F32) + y.astype(BF16).astype(F32)).astype(BF16)
        if l + 1 < L:
            hg[l + 1, yi, rows, :] = hn
            stats(l + 1, ch, hn.astype(F32))
            send_h(l + 1, ch, rows, pl.ds(ch, 1))
        else:
            h_out[rows, :] = hn

    stages = dict(IN=stage_in, SQ=send_q, JN=stage_in_rest, RKV=reduce_kv, RU=reduce_u, Q=stage_q, QK=scores, X=transpose, KV=stage_kv, SM=softmax, PV=values, LV=load_values,
                  SO=send_o, F=stage_f, MLP=stage_mlp, OUT=stage_out, H=stage_h)
    for step in ORDER:
        with jax.named_scope(step):
            chunks = range(nch) if step[-2] == "*" else ("AB".index(step[-2]),)
            stages[step[:-2]](int(step[-1]), chunks if step[:2] in ("IN", "JN") else chunks[0])
    for n, ch in list(open_sends):
        drain(n, ch)


def _tail(h_in, k_in, v_in, h_out, k_out, v_out, sem):
    cps = [pltpu.make_async_copy(a, o, sem.at[n])
           for n, (a, o) in enumerate(((k_in, k_out), (v_in, v_out), (h_in, h_out)))]
    for cp in cps:
        cp.start()
    for cp in cps:
        cp.wait()


def solution(mesh):
    nch = 2
    act = P(None, ('x', 'yz'))
    w_first = P(None, 'x', 'yz')
    w_second = P(None, 'yz', 'x')
    cache = P(None, None, ('yz', 'x'), None, None)
    new = P(None, None, ('yz', 'x'), None)
    inv_half = 10000.0 ** (-np.arange(D // 2, dtype=np.float64) / (D // 2))
    inv_np = np.concatenate([inv_half, inv_half]).astype(np.float32)[None]

    def body(h, g, wq, wk, wv, w_in, wo, w_out, kc, vc, lens):
        any_spec = pl.BlockSpec(memory_space=pl.ANY)
        vm_spec = pl.BlockSpec(memory_space=pltpu.VMEM)
        shapes = ((B, D), (L, B, D), (L, B, D))
        vm = pltpu.VMEM
        dma = pltpu.SemaphoreType.DMA
        scratch = [
            vm((B, S, D), BF16), vm((B, S, D), BF16),
            vm((L, 3, 512, 512), BF16), vm((L, 512, 2048), BF16), vm((L, 512, 512), BF16), vm((L, 2048, 512), BF16),
            vm((NY, L, D), BF16), vm((1, B), jnp.int32), vm((1, D), F32),
            vm((B, D), F32), vm((B, D), F32), vm((B, D), F32),
            vm((L, NY, B, D), BF16),
            vm((L, NX * NY, nch, 1, B), F32),
            vm((NX, B, D), F32),
            vm((L, NX, B, D), BF16),
            vm((L, NX - 1, B, D), BF16),
            vm((2, 2, 2, B, D), F32),
            vm((L, 2, 2, 2, B, D), BF16),
            vm((L, 2, 2, B, D), BF16),
            vm((2, 2, B, D), F32),
            vm((L, 2, 2, B, D), BF16),
            vm((L, 2, B, D), BF16),
            vm((2, B, 1024), F32),
            vm((L, 2, B, 1024), BF16),
            vm((L, B, 1024), BF16),
            vm((B, 1024), F32),
            vm((L, B, 1024), BF16),
            vm((L, B, 1024), BF16),
            vm((L, 2, B, 1024), BF16),
            vm((L, NX, B, D), BF16),
            vm((NY, B, D), F32),
            vm((L, NY, B, D), BF16),
            vm((L, NY - 1, B, D), BF16),
            vm((B, NY * D), BF16), vm((B, D), BF16), vm((B, D), F32),
            vm((B, S), F32), vm((B, S), BF16), vm((B, D), F32), vm((B, D), F32),
            dma((4,)), dma((4,)), dma((nch,)), dma((nch,)), dma((2,)),
            dma((3, nch)), dma((len(KINDS), nch)),
        ]
        h_new, k_new, v_new = pl.pallas_call(
            functools.partial(_kernel, nch),
            out_shape=tuple(vm(n, BF16) for n in shapes),
            in_specs=[any_spec] * 12,
            out_specs=(vm_spec,) * 3,
            scratch_shapes=scratch,
            compiler_params=pltpu.CompilerParams(collective_id=0, has_side_effects=True,
                                                 vmem_limit_bytes=66_000_000),
            name="decode_step",
        )(h, g, wq, wk, wv, w_in, wo, w_out, kc.reshape(L, B, S, D), vc.reshape(L, B, S, D),
          lens.reshape(1, B), jnp.asarray(inv_np))
        h_new, k_new, v_new = pl.pallas_call(
            _tail,
            out_shape=tuple(jax.ShapeDtypeStruct(n, BF16) for n in shapes),
            in_specs=[vm_spec] * 3,
            out_specs=(any_spec,) * 3,
            scratch_shapes=[dma((3,))],
            name="results",
        )(*(pltpu.with_memory_space_constraint(a, pltpu.VMEM) for a in (h_new, k_new, v_new)))
        return h_new, k_new.reshape(L, B, 1, D), v_new.reshape(L, B, 1, D)

    return jax.shard_map(
        body, mesh=mesh,
        in_specs=(act, act, w_first, w_first, w_first, w_first, w_second, w_second, cache, cache, P(None)),
        out_specs=(act, new, new), check_vma=False)
```
